32 devices in a mesh: rep: 2 (over x), shard: 16 (over z, y, core).
Axes of the slice: x: 2, y: 2, z: 4, core: 2. Of those that a mesh axis runs over, the one named last changes fastest.
Arguments:
- dense: bfloat16 [8192, 128], P(('rep', 'shard')), may hold values from -6 to 6
- small_ids: int32 [8192, 32], P(('rep', 'shard')), may hold values from 0 to 511
- labels: int32 [8192], P(('rep', 'shard')), may hold values 0 or 1
- small_tables: bfloat16 [32, 512, 128], replicated, may hold values from -6 to 6
- large_tables: bfloat16 [16, 8192, 128], P('shard'), may hold values from -6 to 6
- batch_sizes: int32 [16, 32], replicated, may hold values from 1 to 128, as said below
- bag_ends: int32 [16, 32, 128], P('shard'), may hold values from 0 to 256, as said below
- owner_row_index: int32 [16, 32, 256], P('shard'), may hold values from 0 to 8191
- w_first: bfloat16 [1304, 1024], replicated, may hold values from -0.15625 to 0.15625
- b_first: float32 [1024], replicated, may hold values from -3 to 3
- w_out: float32 [1024], replicated, may hold values from -0.1875 to 0.1875
Outputs:
- small_new: bfloat16 [32, 512, 128], replicated
- large_new: bfloat16 [16, 8192, 128], P('shard')
The draws below stay inside these ranges and needn't reach their ends.
Inputs may be any that keep to these rules, and one draw needn't show every extreme that they name: `batch_sizes`: every feature has some owner, and every owner some feature, with exactly 128. `bag_ends`: nondecreasing along the last dimension; bags j >= batch_sizes[f, d] are empty; some bag list reaches 256.
All inputs are finite; a program needn't handle non-finite values. No bound on the sum of `labels` on one device may be relied on, other than what follows from the above.
Results may differ from the reference program's by a relative error of at most 0.0095.
Values may be sent and summed in bfloat16 or wider, within the bound.
A program may use at most 192 MiB of HBM per device.

```python
import math
import jax
import jax.numpy as jnp
import numpy as np
from jax import lax

E = 128
SROWS = 512
NSMALL = 32
LROWS = 8192
HID1 = 1024
PMAX = 3
BATCH = 256
BSMAX = 128
SLOTS = 256
FEAT = 16
DEST = 32
ROWS = 8192
PAIRS = 1176


def batch_table(key):
    folded = jax.random.fold_in(key, 7301)
    first_key, second_key, third_key = jax.random.split(folded, 3)
    size_table = jax.random.randint(first_key, (FEAT, DEST), 1, BSMAX + 1)
    pick_feature = jax.random.randint(second_key, (DEST,), 0, FEAT)
    pick_owner = jax.random.randint(third_key, (FEAT,), 0, DEST)
    forced = (jnp.arange(FEAT)[:, None] == pick_feature[None, :]) | (jnp.arange(DEST)[None, :] == pick_owner[:, None])
    return jnp.where(forced, BSMAX, size_table).astype(jnp.int32)


def draw_batch_sizes(key, part):
    return batch_table(key)


def draw_bag_ends(key, part):
    size_table = batch_table(key)
    lengths = jax.random.randint(jax.random.fold_in(key, 7302), (FEAT, DEST, BSMAX), 1, PMAX + 1)
    lengths = jnp.where(size_table[:, :, None] == BSMAX, PMAX, lengths)
    active = jnp.arange(BSMAX)[None, None, :] < size_table[:, :, None]
    limits = jnp.cumsum(jnp.where(active, lengths, 0), axis=2)
    return jnp.minimum(limits, SLOTS).astype(jnp.int32)


def touch_ends(result, stream_key, smallest, top_value):
    place = [jax.random.randint(jax.random.fold_in(stream_key, axis), (), 0, length) for axis, length in enumerate(result.shape)]
    widest = result.shape.index(max(result.shape))
    neighbour = place[:widest] + [(place[widest] + 1) % result.shape[widest]] + place[widest + 1:]
    return result.at[tuple(place)].set(smallest).at[tuple(neighbour)].set(top_value)


def block_levels(own_key, dims, cuts, least, largest):
    gain, own = 1.0, jax.random.fold_in(own_key, 6)
    for position, blocks in cuts:
        heights = jnp.exp(jax.random.uniform(jax.random.fold_in(own, position), (blocks,), jnp.float32, least / len(cuts), largest / len(cuts)))
        gain = gain * jnp.repeat(heights, dims[position] // blocks).reshape([-1 if axis == position else 1 for axis in range(len(dims))])
    return gain


def rank_table(amount, lean):
    weights = [(1 << 20) // math.isqrt(standing ** lean) + 1 for standing in range(1, amount + 1)]
    deviation = 1 + sum(weights) // (1 << 30)
    return np.cumsum(np.array([max(1, weight // deviation) for weight in weights]))


def skewed_ids(own_key, shape, amount, lean):
    grid = rank_table(amount, lean)
    ticket = jax.random.randint(jax.random.fold_in(own_key, 1), shape, 0, int(grid[amount - 1]))
    grade = jnp.searchsorted(jnp.asarray(grid, jnp.int32), ticket, side="right")
    return jax.random.permutation(jax.random.fold_in(own_key, 2), amount)[grade].astype(jnp.int32)


def normal_values(rng, shape, spread, bound, shards=(), held_as=jnp.bfloat16):
    entries = jax.random.normal(rng, shape, jnp.float32) * spread
    if len(shards) > 0:
        entries = block_levels(rng, shape, shards, -0.22, 0.18) * entries
    return jnp.clip(entries, min=-bound, max=bound).astype(held_as)


def setup_inputs(seed: int = 0) -> dict:
    splits = jax.random.split(jax.random.key(seed), 12)
    return {
        "dense": normal_values(splits[0], (ROWS, E), 1.0, 6.0, ((0, 32),)),
        "small_ids": touch_ends(jax.random.randint(splits[1], (ROWS, NSMALL), 0, SROWS), jax.random.fold_in(splits[1], 1), 0, SROWS - 1).astype(jnp.int32),
        "labels": touch_ends((jax.random.randint(splits[2], (ROWS,), 0, 4) < 1).astype(jnp.int32), jax.random.fold_in(splits[2], 1), 0, 1),
        "small_tables": normal_values(splits[3], (NSMALL, SROWS, E), 1.0, 6.0),
        "large_tables": normal_values(splits[4], (FEAT, LROWS, E), 1.0, 6.0, ((0, 16),)),
        "batch_sizes": draw_batch_sizes(jax.random.fold_in(splits[11], 71), 0),
        "bag_ends": draw_bag_ends(jax.random.fold_in(splits[11], 71), 0),
        "owner_row_index": touch_ends(skewed_ids(splits[7], (FEAT, DEST, SLOTS), LROWS, 2), jax.random.fold_in(splits[7], 3), 0, LROWS - 1).astype(jnp.int32),
        "w_first": normal_values(splits[8], (PAIRS + E, HID1), (PAIRS + E) ** -0.5, 0.15625),
        "b_first": normal_values(splits[9], (HID1,), 0.5, 3.0, (), jnp.float32),
        "w_out": normal_values(splits[10], (HID1,), HID1 ** -0.5, 0.1875, (), jnp.float32),
    }


step_size = 32.0

def bag_members(limits):
    starts = jnp.concatenate([jnp.zeros(limits.shape[:-1] + (1,), jnp.int32), limits[..., :-1]], axis=-1)
    positions = jnp.arange(SLOTS, dtype=jnp.int32)
    inside = (positions >= starts[..., None]) & (positions < limits[..., None])
    return inside.astype(jnp.float32)

def silu_slope(preacts):
    squash = jax.nn.sigmoid(preacts)
    return squash * (1.0 + preacts * (1.0 - squash))

def reference(dense, small_ids, labels, small_tables, large_tables, batch_sizes, bag_ends, owner_row_index, w_first, b_first, w_out):
    vec_count = 1 + NSMALL + FEAT
    lower_rows, lower_cols = np.tril_indices(vec_count, -1)

    def pool_one(packed):
        table_one, row_list, limits = packed
        bag_entry = bag_members(limits)
        collected_rows = table_one[row_list].astype(jnp.float32)
        return jnp.einsum('hxt,htv->hxv', bag_entry, collected_rows).astype(jnp.bfloat16)
    pooled = lax.map(pool_one, (large_tables, owner_row_index, bag_ends))
    pooled_dev = jnp.moveaxis(pooled, 1, 0)
    dense_blocks = dense.reshape(DEST, BATCH, E)
    id_blocks = small_ids.reshape(DEST, BATCH, NSMALL)
    label_blocks = labels.reshape(DEST, BATCH).astype(jnp.float32)
    size_blocks = jnp.transpose(batch_sizes)
    samples = jnp.arange(BATCH, dtype=jnp.int32)
    table_offsets = jnp.arange(NSMALL, dtype=jnp.int32) * SROWS
    feat_offsets = jnp.arange(FEAT, dtype=jnp.int32) * BSMAX

    def device_step(totals, inputs):
        dense_b, ids_b, label_b, pooled_b, size_row = inputs
        chosen = samples[None, :] * size_row[:, None] // BATCH
        large_feat = jnp.take_along_axis(pooled_b, chosen[:, :, None].astype(jnp.int32), axis=1)
        large_feat = jnp.transpose(large_feat, (1, 0, 2))
        minor_feature = small_tables[jnp.arange(NSMALL)[None, :], ids_b]
        vectors = jnp.concatenate([dense_b[:, None, :], minor_feature, large_feat], axis=1)
        vec_float = vectors.astype(jnp.float32)
        gram_matrix = jnp.einsum('bie,bje->bij', vec_float, vec_float)
        pair_values = (gram_matrix[:, lower_rows, lower_cols] * E ** (-0.5)).astype(jnp.bfloat16)
        features = jnp.concatenate([pair_values, dense_b], axis=1)
        preact = jnp.dot(features, w_first, preferred_element_type=jnp.float32) + b_first
        hidden = jax.nn.silu(preact)
        logits = lax.optimization_barrier(jnp.sum(hidden * w_out[None, :], axis=1))
        logit_grad = jax.nn.sigmoid(logits) - label_b
        pre_grad = (logit_grad[:, None] * w_out[None, :] * silu_slope(preact)).astype(jnp.bfloat16)
        pair_grad = jnp.dot(pre_grad, jnp.transpose(w_first[:PAIRS]), preferred_element_type=jnp.float32) * E ** (-0.5)
        lower_part = jnp.zeros((BATCH, vec_count, vec_count), jnp.float32).at[:, lower_rows, lower_cols].set(pair_grad)
        vec_grad = jnp.einsum('bij,bje->bie', lower_part + jnp.swapaxes(lower_part, 1, 2), vec_float).astype(jnp.bfloat16)
        small_part = vec_grad[:, 1:1 + NSMALL].astype(jnp.float32).reshape(-1, E)
        small_index = (table_offsets[None, :] + ids_b).reshape(-1).astype(jnp.int32)
        totals = totals + jax.ops.segment_sum(small_part, small_index, NSMALL * SROWS)
        large_part = jnp.transpose(vec_grad[:, 1 + NSMALL:], (1, 0, 2)).astype(jnp.float32).reshape(-1, E)
        large_index = (feat_offsets[:, None] + chosen).reshape(-1).astype(jnp.int32)
        accumulate_gradient = jax.ops.segment_sum(large_part, large_index, FEAT * BSMAX).reshape(FEAT, BSMAX, E).astype(jnp.bfloat16)
        return (totals, accumulate_gradient)
    start_totals = jnp.zeros((NSMALL * SROWS, E), jnp.float32)
    small_grad, fold_all = lax.scan(device_step, start_totals, (dense_blocks, id_blocks, label_blocks, pooled_dev, size_blocks))
    fold_feat = jnp.moveaxis(fold_all, 0, 1)

    def table_grad(packed):
        row_list, limits, gradient_list = packed
        bag_entry = bag_members(limits)
        slot_vectors = jnp.einsum('bni,bnv->biv', bag_entry, gradient_list.astype(jnp.float32))
        return jax.ops.segment_sum(slot_vectors.reshape(-1, E), row_list.reshape(-1).astype(jnp.int32), LROWS)
    large_grad = lax.map(table_grad, (owner_row_index, bag_ends, fold_feat))
    small_new = (small_tables.astype(jnp.float32) - step_size * small_grad.reshape(NSMALL, SROWS, E)).astype(jnp.bfloat16)
    large_new = (large_tables.astype(jnp.float32) - step_size * large_grad).astype(jnp.bfloat16)
    return (small_new, large_new)
```

```python
import functools

import jax
import jax.numpy as jnp
from jax import lax
from jax.experimental import pallas as pl
from jax.experimental.pallas import tpu as pltpu
from jax.sharding import PartitionSpec as P

step_size = 32.0
LANES = 128
VMEM_LIMIT = 60 * 1024 * 1024
f32 = jnp.float32
bf16 = jnp.bfloat16


def whole(space):
    return pl.BlockSpec(memory_space=space)


def iota(shape, axis):
    return lax.broadcasted_iota(jnp.int32, shape, axis)


def members_of(ends, slots):
    span = ends.shape[-1]
    starts = jnp.where(iota((1, span), 1) == 0, 0, pltpu.roll(ends, 1, 1))
    places = iota((slots, span), 0)
    return ((places >= starts) & (places < ends)).astype(f32).astype(bf16)


def pool_kernel(
    first_ref, rows_ref, count_ref, ends_ref, table_ref, ids_ref, out_ref, by_sample, wide, picked,
):
    by_sample[...] = jnp.transpose(ids_ref[...])
    slots = rows_ref.shape[1]
    owners = out_ref.shape[0]
    last = count_ref.shape[1] - 1
    first = first_ref[0]
    wide[...] = table_ref[...].astype(f32)
    picked[...] = jnp.zeros_like(picked)

    def owner(o, carry):
        d = o + first

        def group(g, c):
            base = pl.multiple_of(g * 8, 8)
            parts = [wide[pl.ds(rows_ref[d, base + u], 1), :] for u in range(8)]
            picked[pl.ds(pl.multiple_of(o * slots + base, 8), 8), :] = jnp.concatenate(parts, axis=0)
            return c

        return lax.fori_loop(0, (count_ref[d, last] + 7) // 8, group, carry)

    lax.fori_loop(0, owners, owner, 0)

    def sums(o, carry):
        members = members_of(ends_ref[pl.ds(o + first, 1), :], slots)
        block = picked[pl.ds(pl.multiple_of(o * slots, 8), slots), :].astype(bf16)
        pooled = lax.dot_general(
            members, block, (((0,), (0,)), ((), ())), preferred_element_type=f32
        )
        out_ref[o] = pooled.astype(bf16)
        return carry

    lax.fori_loop(0, owners, sums, 0, unroll=4)


def pool(first, owners, rows, ends, table, ids):
    slots = rows.shape[1]
    width = table.shape[1]
    return pl.pallas_call(
        pool_kernel,
        out_shape=(
            jax.ShapeDtypeStruct((owners, ends.shape[1], width), bf16),
            jax.ShapeDtypeStruct((ids.shape[1], ids.shape[0]), ids.dtype),
        ),
        in_specs=[whole(pltpu.SMEM)] * 3 + [whole(pltpu.VMEM)] * 3,
        out_specs=(whole(pltpu.VMEM),) * 2,
        scratch_shapes=[
            pltpu.VMEM(table.shape, f32),
            pltpu.VMEM((owners * slots, width), f32),
        ],
        compiler_params=pltpu.CompilerParams(vmem_limit_bytes=VMEM_LIMIT),
        name="pool",
    )(first, rows, ends, ends, table, ids)


def spans_of(vec_count):
    return [(i, i * (i - 1) // 2) for i in range(1, vec_count)]


def top_kernel(
    vec_count, pad, index_ref, sizes_ref, dense_ref, labels_ref, small_ref, large_ref,
    w_ref, bias_ref, wout_ref, small_out, fold_out, vecs, gram, pairs, spread,
):
    batch, width = dense_ref.shape
    small_count = small_ref.shape[0]
    feats, bag_span = large_ref.shape[0], large_ref.shape[1]
    pair_pad = pairs.shape[1]
    pair_count = vec_count * (vec_count - 1) // 2
    scale = width ** (-0.5)
    spans = spans_of(vec_count)

    def rows_of(i):
        return pl.ds(i, batch, stride=pad)

    vecs[rows_of(0), :] = dense_ref[...].astype(f32)
    for t in range(small_count):
        vecs[rows_of(1 + t), :] = small_ref[t].astype(f32)
    sample = iota((batch, bag_span), 0)
    bag = iota((batch, bag_span), 1) * batch
    for f in range(feats):
        reach = sample * sizes_ref[f, index_ref[0]]
        hot = ((reach >= bag) & (reach < bag + batch)).astype(f32).astype(bf16)
        vecs[rows_of(1 + small_count + f), :] = jnp.dot(
            hot, large_ref[f], preferred_element_type=f32
        )
    for i in range(vec_count, pad):
        vecs[rows_of(i), :] = jnp.zeros((batch, width), f32)

    unroll = 8

    def gram_step(g, c):
        for u in range(unroll):
            at = pl.ds(pl.multiple_of((g * unroll + u) * pad, 8), pad)
            own = vecs[at, :].astype(bf16)
            gram[at, 0:pad] = lax.dot_general(
                own, own, (((1,), (1,)), ((), ())), preferred_element_type=f32
            )
        return c

    lax.fori_loop(0, batch // unroll, gram_step, 0)

    lane = iota((1, LANES), 1)
    chunk = 64
    for start in range(0, batch, chunk):
        tile = jnp.zeros((chunk, LANES), f32)
        at_tile = 0
        for i, off in spans:
            piece = gram[pl.ds(start * pad + i, chunk, stride=pad), :]
            turn = off % LANES
            if turn:
                piece = pltpu.roll(piece, turn, 1)
            low = off - at_tile * LANES
            tile = jnp.where((lane >= low) & (lane < low + i), piece, tile)
            if low + i >= LANES:
                pairs[start : start + chunk, at_tile * LANES : (at_tile + 1) * LANES] = (
                    tile * scale
                ).astype(bf16)
                at_tile += 1
                rest = low + i - LANES
                tile = jnp.where(lane < rest, piece, jnp.zeros_like(piece))
        if at_tile * LANES < pair_pad:
            pairs[start : start + chunk, at_tile * LANES : pair_pad] = (tile * scale).astype(bf16)

    block = 128
    labels_col = jnp.transpose(
        jnp.broadcast_to(labels_ref[...].astype(f32), (LANES, batch))
    )[:, 0:1]
    for start in range(0, batch, block):
        at = slice(start, start + block)
        preact = (
            jnp.dot(pairs[at, :], w_ref[0:pair_pad, :], preferred_element_type=f32)
            + jnp.dot(dense_ref[at, :], w_ref[pair_count : pair_count + width, :], preferred_element_type=f32)
            + bias_ref[...]
        )
        squash = jax.nn.sigmoid(preact)
        logits = jnp.sum(preact * squash * wout_ref[...], axis=1, keepdims=True)
        grad = jax.nn.sigmoid(logits) - labels_col[at, :]
        pre_grad = (
            grad * wout_ref[...] * (squash * (1.0 + preact * (1.0 - squash)))
        ).astype(bf16)
        for q in range(0, pair_pad, LANES):
            spread[at, q : q + LANES] = lax.dot_general(
                pre_grad, w_ref[q : q + LANES, :], (((1,), (1,)), ((), ())),
                preferred_element_type=f32,
            ) * scale

    gram[rows_of(0), :] = jnp.zeros((batch, LANES), f32)
    for i in range(vec_count, pad):
        gram[rows_of(i), :] = jnp.zeros((batch, LANES), f32)
    for start in range(0, batch, chunk):
        for i, off in spans:
            first = off // LANES
            low = off - first * LANES
            here = spread[start : start + chunk, first * LANES : (first + 1) * LANES]
            if low + i > LANES:
                after = spread[start : start + chunk, (first + 1) * LANES : (first + 2) * LANES]
                here = jnp.where(lane >= low, here, after)
            if low:
                here = pltpu.roll(here, LANES - low, 1)
            gram[pl.ds(start * pad + i, chunk, stride=pad), :] = jnp.where(lane < i, here, 0.0)

    def back_step(g, c):
        for u in range(unroll):
            at = pl.ds(pl.multiple_of((g * unroll + u) * pad, 8), pad)
            lower = gram[at, :]
            both = lower[:, 0:pad] + jnp.transpose(lower)[0:pad, :]
            vecs[at, :] = jnp.dot(
                both.astype(bf16), vecs[at, :].astype(bf16), preferred_element_type=f32
            )
        return c

    lax.fori_loop(0, batch // unroll, back_step, 0)

    for t in range(small_count):
        small_out[t] = vecs[rows_of(1 + t), :].astype(bf16)
    sample_lane = iota((bag_span, batch), 1)
    bag_row = iota((bag_span, batch), 0) * batch
    for f in range(feats):
        reach = sample_lane * sizes_ref[f, index_ref[0]]
        hot = ((reach >= bag_row) & (reach < bag_row + batch)).astype(f32).astype(bf16)
        fold_out[f] = jnp.dot(
            hot, vecs[rows_of(1 + small_count + f), :].astype(bf16), preferred_element_type=f32
        ).astype(bf16)


def top(index, sizes, dense, labels, small, large, w_first, bias, wout):
    batch, width = dense.shape
    small_count, feats, bag_span = small.shape[0], large.shape[0], large.shape[1]
    vec_count = 1 + small_count + feats
    pad = -(-vec_count // 8) * 8
    pair_count = vec_count * (vec_count - 1) // 2
    pair_pad = -(-pair_count // LANES) * LANES
    return pl.pallas_call(
        functools.partial(top_kernel, vec_count, pad),
        out_shape=(
            jax.ShapeDtypeStruct((small_count, batch, width), bf16),
            jax.ShapeDtypeStruct((feats, bag_span, width), bf16),
        ),
        in_specs=[whole(pltpu.SMEM)] * 2 + [whole(pltpu.VMEM)] * 7,
        out_specs=(whole(pltpu.VMEM), whole(pltpu.VMEM)),
        scratch_shapes=[
            pltpu.VMEM((batch * pad, width), f32),
            pltpu.VMEM((batch * pad, LANES), f32),
            pltpu.VMEM((batch, pair_pad), bf16),
            pltpu.VMEM((batch, pair_pad), f32),
        ],
        compiler_params=pltpu.CompilerParams(vmem_limit_bytes=VMEM_LIMIT),
        name="top",
    )(
        index, sizes, dense, labels[None, :], small, large, w_first,
        bias[None, :], wout[None, :],
    )


def greet_all():
    copies, groups = lax.axis_size("rep"), lax.axis_size("shard")
    devices = copies * groups
    index = lax.axis_index("rep") * groups + lax.axis_index("shard")
    barrier = pltpu.get_barrier_semaphore()

    def greet(k, c):
        other = lax.rem(index + k, devices)
        pl.semaphore_signal(
            barrier, inc=1, device_id={"rep": other // groups, "shard": lax.rem(other, groups)},
            device_id_type=pl.DeviceIdType.MESH,
        )
        return c

    lax.fori_loop(1, devices, greet, 0)
    pl.semaphore_wait(barrier, devices - 1)


def remote(src, dst, send, recv, rep, shard):
    return pltpu.make_async_remote_copy(
        src_ref=src, dst_ref=dst, send_sem=send, recv_sem=recv,
        device_id={"rep": rep, "shard": shard}, device_id_type=pl.DeviceIdType.MESH,
    )


def forward_kernel(pooled_ref, own_ids_ref, tables_ref, large_out, small_out, send, recv, own, tables):
    groups = lax.axis_size("shard")
    rep, me = lax.axis_index("rep"), lax.axis_index("shard")

    def block(k):
        to = lax.rem(me + k, groups)
        return remote(pooled_ref.at[to], large_out.at[me], send.at[k], recv.at[k], rep, to)

    def block_in(k):
        at = lax.rem(me + groups - k, groups)
        return remote(pooled_ref.at[at], large_out.at[at], send.at[k], recv.at[k], rep, at)

    def run(low, high, act):
        def body(k, c):
            act(k)
            return c

        lax.fori_loop(low, high, body, 0)

    fetch = pltpu.make_async_copy(tables_ref, tables, own.at[1])
    fetch.start()
    greet_all()
    run(1, groups, lambda k: block(k).start())
    mine = pltpu.make_async_copy(pooled_ref.at[me], large_out.at[me], own.at[0])
    mine.start()
    batch, small_count = own_ids_ref.shape
    rows = iota((batch, tables_ref.shape[1]), 1)
    fetch.wait()
    for t in range(small_count):
        hot = (own_ids_ref[:, t : t + 1] == rows).astype(f32).astype(bf16)
        small_out[t] = jnp.dot(hot, tables[t], preferred_element_type=f32).astype(bf16)
    mine.wait()
    run(1, groups, lambda k: block_in(k).wait_recv())
    run(1, groups, lambda k: block(k).wait_send())


def forward(pooled, own_ids, tables):
    groups = pooled.shape[0]
    return pl.pallas_call(
        forward_kernel,
        out_shape=(
            jax.ShapeDtypeStruct(pooled.shape, pooled.dtype),
            jax.ShapeDtypeStruct(
                (tables.shape[0], own_ids.shape[0], tables.shape[2]), tables.dtype
            ),
        ),
        in_specs=[whole(pltpu.VMEM)] * 2 + [whole(pl.ANY)],
        out_specs=(whole(pltpu.VMEM),) * 2,
        scratch_shapes=[pltpu.SemaphoreType.DMA((groups,))] * 2
        + [pltpu.SemaphoreType.DMA((2,)), pltpu.VMEM(tables.shape, tables.dtype)],
        compiler_params=pltpu.CompilerParams(
            collective_id=0, has_side_effects=True, vmem_limit_bytes=VMEM_LIMIT
        ),
        name="forward",
    )(pooled, own_ids, tables)


def tail_kernel(
    ids_ref, grads_ref, fold_ref, rows_ref, ends_ref, table_ref, tables_ref, small_out, large_out,
    peer_ids, peer_grads, folds, acc, lhs, rhs, keep, sent, came, sent_2, came_2, sent_3, came_3,
    prior, local, peer_s, peer_r, fold_s, fold_r, far_s, far_r, rs1_s, rs1_r, rs2_s, rs2_r,
    rs3_s, rs3_r, ag_z, ag_1, ag_2, ag_core, ag_r,
):
    groups = lax.axis_size("shard")
    ring = groups // 4
    rep, me = lax.axis_index("rep"), lax.axis_index("shard")
    z, y, core = me // 4, lax.rem(me, 4) // 2, lax.rem(me, 2)
    other = 1 - rep
    small_count, batch = ids_ref.shape
    half_count = small_count // 2
    per_unit = small_count // 16
    small_rows = keep.shape[2] // per_unit
    part = small_out.shape[5]
    slots = rows_ref.shape[1]
    spots = acc.shape[0]
    width = table_ref.shape[1]
    blocks = acc.shape[1] // width

    def shard_of(z_at, y_at, core_at):
        return z_at * 4 + y_at * 2 + core_at

    def loop(low, high, act):
        def body(k, c):
            act(k)
            return c

        lax.fori_loop(low, high, body, 0)

    peer = shard_of(z, y, 1 - core)
    away = (1 - core) * half_count
    swap = [
        remote(ids_ref.at[pl.ds(pl.multiple_of(away, 8), half_count)], peer_ids, peer_s.at[0], peer_r.at[0], rep, peer),
        remote(grads_ref.at[pl.ds(away, half_count)], peer_grads, peer_s.at[1], peer_r.at[1], rep, peer),
    ]

    def out_block(k):
        to = lax.rem(me + k, groups)
        return remote(fold_ref.at[to], folds.at[rep * groups + me], fold_s.at[k], fold_r.at[k], rep, to)

    def in_block(k):
        at = lax.rem(me + groups - k, groups)
        return remote(fold_ref.at[at], folds.at[rep * groups + at], fold_s.at[k], fold_r.at[k], rep, at)

    def far_out(k):
        slot = folds.at[rep * groups + lax.rem(me + groups - k, groups)]
        return remote(slot, slot, far_s.at[k], far_r.at[k], other, me)

    def far_in(k):
        slot = folds.at[other * groups + lax.rem(me + groups - k, groups)]
        return remote(slot, slot, far_s.at[k], far_r.at[k], other, me)

    own_far = remote(fold_ref.at[me], folds.at[rep * groups + me], far_s.at[0], far_r.at[0], other, me)

    greet_all()
    for copy in swap:
        copy.start()
    loop(1, groups, lambda k: out_block(k).start())
    own_far.start()
    fetch = [
        pltpu.make_async_copy(tables_ref.at[core, h, rep, y, z], prior.at[h], local.at[h])
        for h in range(2)
    ]
    for copy in fetch:
        copy.start()
    folds[rep * groups + me] = fold_ref[me]
    acc[...] = jnp.zeros_like(acc)
    for copy in swap:
        copy.wait_recv()

    row = iota((small_rows, batch), 0)

    def dense(t):
        own = (row == ids_ref[pl.ds(core * half_count + t, 1), :]).astype(f32).astype(bf16)
        far = (row == peer_ids[pl.ds(t, 1), :]).astype(f32).astype(bf16)
        return jnp.dot(
            own, grads_ref[core * half_count + t], preferred_element_type=f32
        ) + jnp.dot(far, peer_grads[t], preferred_element_type=f32)

    def first_hop(h, s):
        to_rep = rep + (1 - h) * (1 - 2 * rep)
        to_y = y + h * (1 - 2 * y)
        return remote(
            sent.at[h, s], came.at[h, s], rs1_s.at[h, s], rs1_r.at[h, s], to_rep, shard_of(z, to_y, core)
        )

    def second_hop(h):
        to_rep = rep + h * (1 - 2 * rep)
        to_y = y + (1 - h) * (1 - 2 * y)
        return remote(
            sent_2.at[h], came_2.at[h], rs2_s.at[h], rs2_r.at[h], to_rep, shard_of(z, to_y, core)
        )

    def third_hop(h, k):
        to = lax.rem(z + k, ring)
        return remote(
            sent_3.at[h, to], came_3.at[h, z], rs3_s.at[h, k], rs3_r.at[h, k], rep, shard_of(to, y, core)
        )

    def third_in(h, k):
        at = lax.rem(z + ring - k, ring)
        return remote(
            sent_3.at[h, at], came_3.at[h, at], rs3_s.at[h, k], rs3_r.at[h, k], rep, shard_of(at, y, core)
        )

    def give(i):
        s, h = i // 2, lax.rem(i, 2)
        r_at = other + h * s * (2 * rep - 1)
        y_at = (1 - y) + (1 - h) * s * (2 * y - 1)
        first = ((h * 2 + r_at) * 2 + y_at) * per_unit
        for j in range(per_unit):
            sent[h, s, j * small_rows : (j + 1) * small_rows, :] = dense(first + j).astype(bf16)
        first_hop(h, s).start()

    def hold(i):
        s, h = i // 2, lax.rem(i, 2)
        r_at = rep + h * (1 - s) * (1 - 2 * rep)
        y_at = y + (1 - h) * (1 - s) * (1 - 2 * y)
        first = ((h * 2 + r_at) * 2 + y_at) * per_unit
        for j in range(per_unit):
            keep[h, s, j * small_rows : (j + 1) * small_rows, :] = dense(first + j)

    loop(0, 4, give)
    loop(0, 4, hold)

    spot = iota((spots, slots), 0)

    def spread_one(d, v):
        members = members_of(ends_ref[pl.ds(d, 1), :], slots)
        moved = jnp.dot(members, folds[d], preferred_element_type=f32)
        at = rows_ref[pl.ds(d, 1), :]
        block = at // spots
        wide = jnp.transpose(jnp.broadcast_to(block.astype(f32), (width, slots)))
        for q in range(blocks):
            rhs[v * slots : (v + 1) * slots, q * width : (q + 1) * width] = jnp.where(
                wide == q, moved, 0.0
            ).astype(bf16)
        lhs[:, v * slots : (v + 1) * slots] = (spot == at - block * spots).astype(f32).astype(bf16)

    step = 2 * width

    def spread_pair(d, e):
        spread_one(d, 0)
        spread_one(e, 1)

        def add(n):
            at = pl.ds(pl.multiple_of(n * step, step), step)
            acc[:, at] += jnp.dot(lhs[...], rhs[:, at], preferred_element_type=f32)

        loop(0, acc.shape[1] // step, add)

    def take(k):
        in_block(k).wait_recv()
        far_out(k).start()

    def near(k):
        return rep * groups + lax.rem(me + groups - k, groups)

    def near_pair(p):
        @pl.when(p > 0)
        def _():
            take(2 * p)

        take(2 * p + 1)
        spread_pair(near(2 * p), near(2 * p + 1))

    def far_pair(p):
        far_in(2 * p).wait_recv()
        far_in(2 * p + 1).wait_recv()
        spread_pair(
            other * groups + lax.rem(me + groups - 2 * p, groups),
            other * groups + lax.rem(me + groups - 2 * p - 1, groups),
        )

    pairs = groups // 2
    cut_1, cut_2 = pairs * 3 // 8, pairs // 2
    loop(0, cut_1, near_pair)

    def turn(h):
        first_hop(h, 0).wait_recv()
        sent_2[h] = (keep[h, 0] + came[h, 0].astype(f32)).astype(bf16)
        second_hop(h).start()

    loop(0, 2, turn)
    loop(cut_1, pairs, near_pair)

    def along(h):
        first_hop(h, 1).wait_recv()
        second_hop(h).wait_recv()
        total = keep[h, 1] + came[h, 1].astype(f32) + came_2[h].astype(f32)
        keep[h, 1] = total
        sent_3[h] = total.astype(bf16).reshape(ring, part, width)
        loop(1, ring, lambda k: third_hop(h, k).start())

    loop(0, 2, along)
    loop(0, cut_2, far_pair)

    for copy in fetch:
        copy.wait()

    def own_part(h):
        total = keep[h, 1, pl.ds(pl.multiple_of(z * part, part), part), :]
        for k in range(1, ring):
            third_in(h, k).wait_recv()
            total = total + came_3[h, lax.rem(z + ring - k, ring)].astype(f32)
        small_out[core, h, rep, y, z] = (prior[h].astype(f32) - step_size * total).astype(bf16)

    loop(0, 2, own_part)

    pending = []

    def place(h, rep_at, z_at, y_at, core_at):
        return small_out.at[core_at, h, rep_at, y_at, z_at]

    def slot_of(rep_at, z_at, y_at, core_at):
        return rep_at * groups + shard_of(z_at, y_at, core_at)

    def send(h, rep_at, z_at, y_at, sem, to_rep, to_z, to_y, to_core):
        block = place(h, rep_at, z_at, y_at, core)
        copy = remote(
            block, block, sem, ag_r.at[h, slot_of(rep_at, z_at, y_at, core)],
            to_rep, shard_of(to_z, to_y, to_core),
        )
        copy.start()
        pending.append(copy)

    def arrived(h, rep_at, z_at, y_at, core_at):
        block = place(h, rep_at, z_at, y_at, core_at)
        remote(
            block, block, local.at[2], ag_r.at[h, slot_of(rep_at, z_at, y_at, core_at)], rep, peer
        ).wait_recv()

    def second(h, k, rep_at, z_at, y_at):
        hop = (rep, z, 1 - y, core) if h == 0 else (other, z, y, core)
        send(h, rep_at, z_at, y_at, ag_1.at[h, k], *hop)

    def third(h, k, rep_at, z_at, y_at):
        hop = (other, z, y, core) if h == 0 else (rep, z, 1 - y, core)
        send(h, rep_at, z_at, y_at, ag_2.at[h, k], *hop)

    def last(h, k, rep_at, z_at, y_at):
        send(h, rep_at, z_at, y_at, ag_core.at[h, k], rep, z, y, 1 - core)

    for k in range(1, ring):
        for h in range(2):
            send(h, rep, z, y, ag_z.at[h, k], rep, lax.rem(z + k, ring), y, core)
    for h in range(2):
        second(h, 0, rep, z, y)
        third(h, 0, rep, z, y)
        last(h, 0, rep, z, y)

    loop(cut_2, pairs, far_pair)
    for q in range(blocks):
        at = slice(q * spots, (q + 1) * spots)
        large_out[at, :] = (
            table_ref[at, :].astype(f32) - step_size * acc[:, q * width : (q + 1) * width]
        ).astype(bf16)

    for k in range(1, ring):
        z_at = lax.rem(z + ring - k, ring)
        for h in range(2):
            arrived(h, rep, z_at, y, core)
            second(h, k, rep, z_at, y)
            third(h, k, rep, z_at, y)
            last(h, k, rep, z_at, y)
    for k in range(ring):
        z_at = lax.rem(z + ring - k, ring)
        for h in range(2):
            where = (rep, z_at, 1 - y) if h == 0 else (other, z_at, y)
            arrived(h, *where, core)
            third(h, ring + k, *where)
            last(h, ring + k, *where)
    for k in range(2 * ring):
        z_at = lax.rem(z + ring - k % ring, ring)
        for h in range(2):
            if h == 0:
                where = (other, z_at, y if k < ring else 1 - y)
            else:
                where = (rep if k < ring else other, z_at, 1 - y)
            arrived(h, *where, core)
            last(h, 2 * ring + k, *where)
    for r in range(2):
        for k in range(ring):
            for y_at in range(2):
                for h in range(2):
                    arrived(h, r, k, y_at, 1 - core)

    for copy in pending + swap:
        copy.wait_send()
    own_far.wait_send()
    loop(1, groups, lambda k: out_block(k).wait_send())
    loop(1, groups, lambda k: far_out(k).wait_send())
    loop(0, 4, lambda i: first_hop(lax.rem(i, 2), i // 2).wait_send())
    loop(0, 2, lambda h: second_hop(h).wait_send())
    for h in range(2):
        loop(1, ring, lambda k: third_hop(h, k).wait_send())


def tail(ids, grads, fold, rows, ends, table, tables):
    groups = fold.shape[0]
    devices, slots = rows.shape
    ring = groups // 4
    small_count, small_rows, width = tables.shape
    part = small_count * small_rows // devices // 2
    unit = small_count * small_rows // 16
    blocks = 8
    split = (2, 2, 2, 2, ring, part, width)
    dma = pltpu.SemaphoreType.DMA
    small, large = pl.pallas_call(
        tail_kernel,
        out_shape=(
            jax.ShapeDtypeStruct(split, bf16),
            jax.ShapeDtypeStruct(table.shape, bf16),
        ),
        in_specs=[whole(pltpu.VMEM)] * 6 + [whole(pl.ANY)],
        out_specs=(whole(pltpu.VMEM),) * 2,
        scratch_shapes=[
            pltpu.VMEM((small_count // 2, ids.shape[1]), ids.dtype),
            pltpu.VMEM((small_count // 2,) + grads.shape[1:], bf16),
            pltpu.VMEM((devices,) + fold.shape[1:], bf16),
            pltpu.VMEM((table.shape[0] // blocks, blocks * width), f32),
            pltpu.VMEM((table.shape[0] // blocks, 2 * slots), bf16),
            pltpu.VMEM((2 * slots, blocks * width), bf16),
            pltpu.VMEM((2, 2, unit, width), f32),
            pltpu.VMEM((2, 2, unit, width), bf16),
            pltpu.VMEM((2, 2, unit, width), bf16),
            pltpu.VMEM((2, unit, width), bf16),
            pltpu.VMEM((2, unit, width), bf16),
            pltpu.VMEM((2, ring, part, width), bf16),
            pltpu.VMEM((2, ring, part, width), bf16),
            pltpu.VMEM((2, part, width), bf16),
            dma((3,)), dma((2,)), dma((2,)),
            dma((groups,)), dma((groups,)), dma((groups,)), dma((groups,)),
            dma((2, 2)), dma((2, 2)), dma((2,)), dma((2,)), dma((2, ring)), dma((2, ring)),
            dma((2, ring)), dma((2, ring)), dma((2, 2 * ring)), dma((2, 4 * ring)), dma((2, devices)),
        ],
        compiler_params=pltpu.CompilerParams(
            collective_id=1, has_side_effects=True, vmem_limit_bytes=VMEM_LIMIT
        ),
        name="tail",
    )(ids, grads, fold, rows, ends, table, tables.reshape(split))
    return small.reshape(tables.shape), large


def store_kernel(small_ref, large_ref, small_out, large_out, sems):
    pieces = 4
    copies = []
    for n, (src, dst) in enumerate(((small_ref, small_out), (large_ref, large_out))):
        size = src.shape[0] // pieces
        for p in range(pieces):
            at = pl.ds(p * size, size)
            copies.append(pltpu.make_async_copy(src.at[at], dst.at[at], sems.at[n, p]))
    for copy in copies:
        copy.start()
    for copy in copies:
        copy.wait()


def store(small, large):
    return pl.pallas_call(
        store_kernel,
        out_shape=(
            jax.ShapeDtypeStruct(small.shape, small.dtype),
            jax.ShapeDtypeStruct(large.shape, large.dtype),
        ),
        in_specs=[whole(pltpu.VMEM)] * 2,
        out_specs=(whole(pl.ANY),) * 2,
        scratch_shapes=[pltpu.SemaphoreType.DMA((2, 4))],
        compiler_params=pltpu.CompilerParams(vmem_limit_bytes=16 * 1024 * 1024),
        name="store",
    )(small, large)


def shards(
    dense, small_ids, labels, small_tables, large_tables, batch_sizes, bag_ends,
    owner_row_index, w_first, b_first, w_out,
):
    groups = lax.axis_size("shard")
    first = lax.axis_index("rep") * groups
    index = first + lax.axis_index("shard")
    ends, rows, table = bag_ends[0], owner_row_index[0], large_tables[0]
    ids = jnp.transpose(small_ids)

    pooled, own_ids = pool(first[None], groups, rows, ends, table, ids)
    large, small = forward(pooled, own_ids, small_tables)
    small_grads, fold = top(
        index[None], batch_sizes, dense, labels, small, large, w_first, b_first, w_out
    )
    small_new, large_new = tail(ids, small_grads, fold, rows, ends, table, small_tables)
    small_new, large_new = store(small_new, large_new)
    return small_new, large_new[None]


def solution(mesh):
    both = ("rep", "shard")
    placed = (
        P(both, None), P(both, None), P(both), P(), P("shard", None, None), P(),
        P("shard", None, None), P("shard", None, None), P(), P(), P(),
    )
    return jax.shard_map(
        shards, mesh=mesh, in_specs=placed, out_specs=(P(), P("shard", None, None)), check_vma=False
    )
```

```python
import functools
import math

import jax
import jax.numpy as jnp
from jax import lax
from jax.experimental import pallas as pl
from jax.experimental.pallas import tpu as pltpu
from jax.sharding import PartitionSpec as P

step_size = 32.0
LANES = 128
VMEM_LIMIT = 60 * 1024 * 1024
MIB = 1024 * 1024
f32 = jnp.float32
bf16 = jnp.bfloat16


def whole(space):
    return pl.BlockSpec(memory_space=space)


def grant(*arrays):
    total = sum(math.prod(a.shape) * jnp.dtype(a.dtype).itemsize for a in arrays)
    return min(VMEM_LIMIT, total + 6 * MIB)


def iota(shape, axis):
    return lax.broadcasted_iota(jnp.int32, shape, axis)


def members_of(ends, slots):
    span = ends.shape[-1]
    starts = jnp.where(iota((1, span), 1) == 0, 0, pltpu.roll(ends, 1, 1))
    places = iota((slots, span), 0)
    return ((places >= starts) & (places < ends)).astype(f32).astype(bf16)


def pool_kernel(
    first_ref, rows_ref, count_ref, ends_ref, table_ref, ids_ref, out_ref, by_sample, wide, picked,
):
    by_sample[...] = jnp.transpose(ids_ref[...])
    slots = rows_ref.shape[1]
    owners = out_ref.shape[0]
    last = count_ref.shape[1] - 1
    first = first_ref[0]
    wide[...] = table_ref[...].astype(f32)
    picked[...] = jnp.zeros_like(picked)

    def owner(o, carry):
        d = o + first

        def group(g, c):
            base = pl.multiple_of(g * 8, 8)
            parts = [wide[pl.ds(rows_ref[d, base + u], 1), :] for u in range(8)]
            picked[pl.ds(pl.multiple_of(o * slots + base, 8), 8), :] = jnp.concatenate(parts, axis=0)
            return c

        return lax.fori_loop(0, (count_ref[d, last] + 7) // 8, group, carry)

    lax.fori_loop(0, owners, owner, 0)

    def sums(o, carry):
        members = members_of(ends_ref[pl.ds(o + first, 1), :], slots)
        block = picked[pl.ds(pl.multiple_of(o * slots, 8), slots), :].astype(bf16)
        pooled = lax.dot_general(
            members, block, (((0,), (0,)), ((), ())), preferred_element_type=f32
        )
        out_ref[o] = pooled.astype(bf16)
        return carry

    lax.fori_loop(0, owners, sums, 0, unroll=4)


def pool(first, owners, rows, ends, table, ids):
    slots = rows.shape[1]
    width = table.shape[1]
    scratch = [pltpu.VMEM(table.shape, f32), pltpu.VMEM((owners * slots, width), f32)]
    return pl.pallas_call(
        pool_kernel,
        out_shape=(
            jax.ShapeDtypeStruct((owners, ends.shape[1], width), bf16),
            jax.ShapeDtypeStruct((ids.shape[1], ids.shape[0]), ids.dtype),
        ),
        in_specs=[whole(pltpu.SMEM)] * 3 + [whole(pltpu.VMEM)] * 3,
        out_specs=(whole(pltpu.VMEM),) * 2,
        scratch_shapes=scratch,
        compiler_params=pltpu.CompilerParams(vmem_limit_bytes=grant(table, ids, ids, ends, *scratch)),
        name="pool",
    )(first, rows, ends, ends, table, ids)


def spans_of(vec_count):
    return [(i, i * (i - 1) // 2) for i in range(1, vec_count)]


def top_kernel(
    vec_count, pad, index_ref, sizes_ref, dense_ref, labels_ref, small_ref, large_ref,
    w_ref, bias_ref, wout_ref, small_out, fold_out, vecs, gram, pairs, spread,
):
    batch, width = dense_ref.shape
    small_count = small_ref.shape[0]
    feats, bag_span = large_ref.shape[0], large_ref.shape[1]
    pair_pad = pairs.shape[1]
    pair_count = vec_count * (vec_count - 1) // 2
    scale = width ** (-0.5)
    spans = spans_of(vec_count)

    def rows_of(i):
        return pl.ds(i, batch, stride=pad)

    vecs[rows_of(0), :] = dense_ref[...].astype(f32)
    for t in range(small_count):
        vecs[rows_of(1 + t), :] = small_ref[t].astype(f32)
    sample = iota((batch, bag_span), 0)
    bag = iota((batch, bag_span), 1) * batch
    for f in range(feats):
        reach = sample * sizes_ref[f, index_ref[0]]
        hot = ((reach >= bag) & (reach < bag + batch)).astype(f32).astype(bf16)
        vecs[rows_of(1 + small_count + f), :] = jnp.dot(
            hot, large_ref[f], preferred_element_type=f32
        )
    for i in range(vec_count, pad):
        vecs[rows_of(i), :] = jnp.zeros((batch, width), f32)

    unroll = 8

    def gram_step(g, c):
        for u in range(unroll):
            at = pl.ds(pl.multiple_of((g * unroll + u) * pad, 8), pad)
            own = vecs[at, :].astype(bf16)
            gram[at, 0:pad] = lax.dot_general(
                own, own, (((1,), (1,)), ((), ())), preferred_element_type=f32
            )
        return c

    lax.fori_loop(0, batch // unroll, gram_step, 0)

    lane = iota((1, LANES), 1)
    chunk = 64
    for start in range(0, batch, chunk):
        tile = jnp.zeros((chunk, LANES), f32)
        at_tile = 0
        for i, off in spans:
            piece = gram[pl.ds(start * pad + i, chunk, stride=pad), :]
            turn = off % LANES
            if turn:
                piece = pltpu.roll(piece, turn, 1)
            low = off - at_tile * LANES
            tile = jnp.where((lane >= low) & (lane < low + i), piece, tile)
            if low + i >= LANES:
                pairs[start : start + chunk, at_tile * LANES : (at_tile + 1) * LANES] = (
                    tile * scale
                ).astype(bf16)
                at_tile += 1
                rest = low + i - LANES
                tile = jnp.where(lane < rest, piece, jnp.zeros_like(piece))
        if at_tile * LANES < pair_pad:
            pairs[start : start + chunk, at_tile * LANES : pair_pad] = (tile * scale).astype(bf16)

    block = 128
    labels_col = jnp.transpose(
        jnp.broadcast_to(labels_ref[...].astype(f32), (LANES, batch))
    )[:, 0:1]
    for start in range(0, batch, block):
        at = slice(start, start + block)
        preact = (
            jnp.dot(pairs[at, :], w_ref[0:pair_pad, :], preferred_element_type=f32)
            + jnp.dot(dense_ref[at, :], w_ref[pair_count : pair_count + width, :], preferred_element_type=f32)
            + bias_ref[...]
        )
        squash = jax.nn.sigmoid(preact)
        logits = jnp.sum(preact * squash * wout_ref[...], axis=1, keepdims=True)
        grad = jax.nn.sigmoid(logits) - labels_col[at, :]
        pre_grad = (
            grad * wout_ref[...] * (squash * (1.0 + preact * (1.0 - squash)))
        ).astype(bf16)
        for q in range(0, pair_pad, LANES):
            spread[at, q : q + LANES] = lax.dot_general(
                pre_grad, w_ref[q : q + LANES, :], (((1,), (1,)), ((), ())),
                preferred_element_type=f32,
            ) * scale

    gram[rows_of(0), :] = jnp.zeros((batch, LANES), f32)
    for i in range(vec_count, pad):
        gram[rows_of(i), :] = jnp.zeros((batch, LANES), f32)
    for start in range(0, batch, chunk):
        for i, off in spans:
            first = off // LANES
            low = off - first * LANES
            here = spread[start : start + chunk, first * LANES : (first + 1) * LANES]
            if low + i > LANES:
                after = spread[start : start + chunk, (first + 1) * LANES : (first + 2) * LANES]
                here = jnp.where(lane >= low, here, after)
            if low:
                here = pltpu.roll(here, LANES - low, 1)
            gram[pl.ds(start * pad + i, chunk, stride=pad), :] = jnp.where(lane < i, here, 0.0)

    def back_step(g, c):
        for u in range(unroll):
            at = pl.ds(pl.multiple_of((g * unroll + u) * pad, 8), pad)
            lower = gram[at, :]
            both = lower[:, 0:pad] + jnp.transpose(lower)[0:pad, :]
            vecs[at, :] = jnp.dot(
                both.astype(bf16), vecs[at, :].astype(bf16), preferred_element_type=f32
            )
        return c

    lax.fori_loop(0, batch // unroll, back_step, 0)

    for t in range(small_count):
        small_out[t] = vecs[rows_of(1 + t), :].astype(bf16)
    sample_lane = iota((bag_span, batch), 1)
    bag_row = iota((bag_span, batch), 0) * batch
    for f in range(feats):
        reach = sample_lane * sizes_ref[f, index_ref[0]]
        hot = ((reach >= bag_row) & (reach < bag_row + batch)).astype(f32).astype(bf16)
        fold_out[f] = jnp.dot(
            hot, vecs[rows_of(1 + small_count + f), :].astype(bf16), preferred_element_type=f32
        ).astype(bf16)


def top(index, sizes, dense, labels, small, large, w_first, bias, wout):
    batch, width = dense.shape
    small_count, feats, bag_span = small.shape[0], large.shape[0], large.shape[1]
    vec_count = 1 + small_count + feats
    pad = -(-vec_count // 8) * 8
    pair_count = vec_count * (vec_count - 1) // 2
    pair_pad = -(-pair_count // LANES) * LANES
    scratch = [
        pltpu.VMEM((batch * pad, width), f32),
        pltpu.VMEM((batch * pad, LANES), f32),
        pltpu.VMEM((batch, pair_pad), bf16),
        pltpu.VMEM((batch, pair_pad), f32),
    ]
    return pl.pallas_call(
        functools.partial(top_kernel, vec_count, pad),
        out_shape=(
            jax.ShapeDtypeStruct((small_count, batch, width), bf16),
            jax.ShapeDtypeStruct((feats, bag_span, width), bf16),
        ),
        in_specs=[whole(pltpu.SMEM)] * 2 + [whole(pltpu.VMEM)] * 7,
        out_specs=(whole(pltpu.VMEM), whole(pltpu.VMEM)),
        scratch_shapes=scratch,
        compiler_params=pltpu.CompilerParams(
            vmem_limit_bytes=grant(dense, small, large, small, large, w_first, *scratch)
        ),
        name="top",
    )(
        index, sizes, dense, labels[None, :], small, large, w_first,
        bias[None, :], wout[None, :],
    )


def greet_all():
    copies, groups = lax.axis_size("rep"), lax.axis_size("shard")
    devices = copies * groups
    index = lax.axis_index("rep") * groups + lax.axis_index("shard")
    barrier = pltpu.get_barrier_semaphore()

    def greet(k, c):
        other = lax.rem(index + k, devices)
        pl.semaphore_signal(
            barrier, inc=1, device_id={"rep": other // groups, "shard": lax.rem(other, groups)},
            device_id_type=pl.DeviceIdType.MESH,
        )
        return c

    lax.fori_loop(1, devices, greet, 0)
    pl.semaphore_wait(barrier, devices - 1)


def remote(src, dst, send, recv, rep, shard):
    return pltpu.make_async_remote_copy(
        src_ref=src, dst_ref=dst, send_sem=send, recv_sem=recv,
        device_id={"rep": rep, "shard": shard}, device_id_type=pl.DeviceIdType.MESH,
    )


def forward_kernel(pooled_ref, own_ids_ref, tables_ref, large_out, small_out, send, recv, own, tables):
    groups = lax.axis_size("shard")
    rep, me = lax.axis_index("rep"), lax.axis_index("shard")

    def block(k):
        to = lax.rem(me + k, groups)
        return remote(pooled_ref.at[to], large_out.at[me], send.at[k], recv.at[k], rep, to)

    def block_in(k):
        at = lax.rem(me + groups - k, groups)
        return remote(pooled_ref.at[at], large_out.at[at], send.at[k], recv.at[k], rep, at)

    def run(low, high, act):
        def body(k, c):
            act(k)
            return c

        lax.fori_loop(low, high, body, 0)

    fetch = pltpu.make_async_copy(tables_ref, tables, own.at[1])
    fetch.start()
    greet_all()
    run(1, groups, lambda k: block(k).start())
    mine = pltpu.make_async_copy(pooled_ref.at[me], large_out.at[me], own.at[0])
    mine.start()
    batch, small_count = own_ids_ref.shape
    rows = iota((batch, tables_ref.shape[1]), 1)
    fetch.wait()
    for t in range(small_count):
        hot = (own_ids_ref[:, t : t + 1] == rows).astype(f32).astype(bf16)
        small_out[t] = jnp.dot(hot, tables[t], preferred_element_type=f32).astype(bf16)
    mine.wait()
    run(1, groups, lambda k: block_in(k).wait_recv())
    run(1, groups, lambda k: block(k).wait_send())


def forward(pooled, own_ids, tables):
    groups = pooled.shape[0]
    small = jax.ShapeDtypeStruct(
        (tables.shape[0], own_ids.shape[0], tables.shape[2]), tables.dtype
    )
    return pl.pallas_call(
        forward_kernel,
        out_shape=(jax.ShapeDtypeStruct(pooled.shape, pooled.dtype), small),
        in_specs=[whole(pltpu.VMEM)] * 2 + [whole(pl.ANY)],
        out_specs=(whole(pltpu.VMEM),) * 2,
        scratch_shapes=[pltpu.SemaphoreType.DMA((groups,))] * 2
        + [pltpu.SemaphoreType.DMA((2,)), pltpu.VMEM(tables.shape, tables.dtype)],
        compiler_params=pltpu.CompilerParams(
            collective_id=0, has_side_effects=True,
            vmem_limit_bytes=grant(pooled, pooled, own_ids, tables, small),
        ),
        name="forward",
    )(pooled, own_ids, tables)


def tail_kernel(
    ids_ref, grads_ref, fold_ref, rows_ref, ends_ref, table_ref, tables_ref, small_out, large_out,
    peer_ids, peer_grads, folds, acc, lhs, rhs, keep, sent, came, sent_2, came_2, sent_3, came_3,
    prior, local, peer_s, peer_r, fold_s, fold_r, far_s, far_r, rs1_s, rs1_r, rs2_s, rs2_r,
    rs3_s, rs3_r, ag_z, ag_1, ag_2, ag_core, ag_r,
):
    groups = lax.axis_size("shard")
    ring = groups // 4
    rep, me = lax.axis_index("rep"), lax.axis_index("shard")
    z, y, core = me // 4, lax.rem(me, 4) // 2, lax.rem(me, 2)
    other = 1 - rep
    small_count, batch = ids_ref.shape
    half_count = small_count // 2
    per_unit = small_count // 16
    small_rows = keep.shape[2] // per_unit
    part = small_out.shape[5]
    slots = rows_ref.shape[1]
    spots = acc.shape[0]
    width = table_ref.shape[1]
    blocks = acc.shape[1] // width

    def shard_of(z_at, y_at, core_at):
        return z_at * 4 + y_at * 2 + core_at

    def loop(low, high, act):
        def body(k, c):
            act(k)
            return c

        lax.fori_loop(low, high, body, 0)

    peer = shard_of(z, y, 1 - core)
    away = (1 - core) * half_count
    swap = [
        remote(ids_ref.at[pl.ds(pl.multiple_of(away, 8), half_count)], peer_ids, peer_s.at[0], peer_r.at[0], rep, peer),
        remote(grads_ref.at[pl.ds(away, half_count)], peer_grads, peer_s.at[1], peer_r.at[1], rep, peer),
    ]

    def out_block(k):
        to = lax.rem(me + k, groups)
        return remote(fold_ref.at[to], folds.at[rep * groups + me], fold_s.at[k], fold_r.at[k], rep, to)

    def in_block(k):
        at = lax.rem(me + groups - k, groups)
        return remote(fold_ref.at[at], folds.at[rep * groups + at], fold_s.at[k], fold_r.at[k], rep, at)

    def far_out(k):
        slot = folds.at[rep * groups + lax.rem(me + groups - k, groups)]
        return remote(slot, slot, far_s.at[k], far_r.at[k], other, me)

    def far_in(k):
        slot = folds.at[other * groups + lax.rem(me + groups - k, groups)]
        return remote(slot, slot, far_s.at[k], far_r.at[k], other, me)

    own_far = remote(fold_ref.at[me], folds.at[rep * groups + me], far_s.at[0], far_r.at[0], other, me)

    greet_all()
    for copy in swap:
        copy.start()
    loop(1, groups, lambda k: out_block(k).start())
    own_far.start()
    fetch = [
        pltpu.make_async_copy(tables_ref.at[core, h, rep, y, z], prior.at[h], local.at[h])
        for h in range(2)
    ]
    for copy in fetch:
        copy.start()
    folds[rep * groups + me] = fold_ref[me]
    acc[...] = jnp.zeros_like(acc)
    for copy in swap:
        copy.wait_recv()

    row = iota((small_rows, batch), 0)

    def dense(t):
        own = (row == ids_ref[pl.ds(core * half_count + t, 1), :]).astype(f32).astype(bf16)
        far = (row == peer_ids[pl.ds(t, 1), :]).astype(f32).astype(bf16)
        return jnp.dot(
            own, grads_ref[core * half_count + t], preferred_element_type=f32
        ) + jnp.dot(far, peer_grads[t], preferred_element_type=f32)

    def first_hop(h, s):
        to_rep = rep + (1 - h) * (1 - 2 * rep)
        to_y = y + h * (1 - 2 * y)
        return remote(
            sent.at[h, s], came.at[h, s], rs1_s.at[h, s], rs1_r.at[h, s], to_rep, shard_of(z, to_y, core)
        )

    def second_hop(h):
        to_rep = rep + h * (1 - 2 * rep)
        to_y = y + (1 - h) * (1 - 2 * y)
        return remote(
            sent_2.at[h], came_2.at[h], rs2_s.at[h], rs2_r.at[h], to_rep, shard_of(z, to_y, core)
        )

    def third_hop(h, k):
        to = lax.rem(z + k, ring)
        return remote(
            sent_3.at[h, to], came_3.at[h, z], rs3_s.at[h, k], rs3_r.at[h, k], rep, shard_of(to, y, core)
        )

    def third_in(h, k):
        at = lax.rem(z + ring - k, ring)
        return remote(
            sent_3.at[h, at], came_3.at[h, at], rs3_s.at[h, k], rs3_r.at[h, k], rep, shard_of(at, y, core)
        )

    def give(i):
        s, h = i // 2, lax.rem(i, 2)
        r_at = other + h * s * (2 * rep - 1)
        y_at = (1 - y) + (1 - h) * s * (2 * y - 1)
        first = ((h * 2 + r_at) * 2 + y_at) * per_unit
        for j in range(per_unit):
            sent[h, s, j * small_rows : (j + 1) * small_rows, :] = dense(first + j).astype(bf16)
        first_hop(h, s).start()

    def hold(i):
        s, h = i // 2, lax.rem(i, 2)
        r_at = rep + h * (1 - s) * (1 - 2 * rep)
        y_at = y + (1 - h) * (1 - s) * (1 - 2 * y)
        first = ((h * 2 + r_at) * 2 + y_at) * per_unit
        for j in range(per_unit):
            keep[h, s, j * small_rows : (j + 1) * small_rows, :] = dense(first + j)

    loop(0, 4, give)
    loop(0, 4, hold)

    spot = iota((spots, slots), 0)

    def spread_one(d, v):
        members = members_of(ends_ref[pl.ds(d, 1), :], slots)
        moved = jnp.dot(members, folds[d], preferred_element_type=f32)
        at = rows_ref[pl.ds(d, 1), :]
        block = at // spots
        wide = jnp.transpose(jnp.broadcast_to(block.astype(f32), (width, slots)))
        for q in range(blocks):
            rhs[v * slots : (v + 1) * slots, q * width : (q + 1) * width] = jnp.where(
                wide == q, moved, 0.0
            ).astype(bf16)
        lhs[:, v * slots : (v + 1) * slots] = (spot == at - block * spots).astype(f32).astype(bf16)

    step = 2 * width

    def spread_pair(d, e):
        spread_one(d, 0)
        spread_one(e, 1)

        def add(n):
            at = pl.ds(pl.multiple_of(n * step, step), step)
            acc[:, at] += jnp.dot(lhs[...], rhs[:, at], preferred_element_type=f32)

        loop(0, acc.shape[1] // step, add)

    def take(k):
        in_block(k).wait_recv()
        far_out(k).start()

    def near(k):
        return rep * groups + lax.rem(me + groups - k, groups)

    def near_pair(p):
        @pl.when(p > 0)
        def _():
            take(2 * p)

        take(2 * p + 1)
        spread_pair(near(2 * p), near(2 * p + 1))

    def far_pair(p):
        far_in(2 * p).wait_recv()
        far_in(2 * p + 1).wait_recv()
        spread_pair(
            other * groups + lax.rem(me + groups - 2 * p, groups),
            other * groups + lax.rem(me + groups - 2 * p - 1, groups),
        )

    pairs = groups // 2
    cut_1, cut_2 = pairs * 3 // 8, pairs // 2
    loop(0, cut_1, near_pair)

    def turn(h):
        first_hop(h, 0).wait_recv()
        sent_2[h] = (keep[h, 0] + came[h, 0].astype(f32)).astype(bf16)
        second_hop(h).start()

    loop(0, 2, turn)
    loop(cut_1, pairs, near_pair)

    def along(h):
        first_hop(h, 1).wait_recv()
        second_hop(h).wait_recv()
        total = keep[h, 1] + came[h, 1].astype(f32) + came_2[h].astype(f32)
        keep[h, 1] = total
        sent_3[h] = total.astype(bf16).reshape(ring, part, width)
        loop(1, ring, lambda k: third_hop(h, k).start())

    loop(0, 2, along)
    loop(0, cut_2, far_pair)

    for copy in fetch:
        copy.wait()

    def own_part(h):
        total = keep[h, 1, pl.ds(pl.multiple_of(z * part, part), part), :]
        for k in range(1, ring):
            third_in(h, k).wait_recv()
            total = total + came_3[h, lax.rem(z + ring - k, ring)].astype(f32)
        small_out[core, h, rep, y, z] = (prior[h].astype(f32) - step_size * total).astype(bf16)

    loop(0, 2, own_part)

    pending = []

    def place(h, rep_at, z_at, y_at, core_at):
        return small_out.at[core_at, h, rep_at, y_at, z_at]

    def slot_of(rep_at, z_at, y_at, core_at):
        return rep_at * groups + shard_of(z_at, y_at, core_at)

    def send(h, rep_at, z_at, y_at, sem, to_rep, to_z, to_y, to_core):
        block = place(h, rep_at, z_at, y_at, core)
        copy = remote(
            block, block, sem, ag_r.at[h, slot_of(rep_at, z_at, y_at, core)],
            to_rep, shard_of(to_z, to_y, to_core),
        )
        copy.start()
        pending.append(copy)

    def arrived(h, rep_at, z_at, y_at, core_at):
        block = place(h, rep_at, z_at, y_at, core_at)
        remote(
            block, block, local.at[2], ag_r.at[h, slot_of(rep_at, z_at, y_at, core_at)], rep, peer
        ).wait_recv()

    def second(h, k, rep_at, z_at, y_at):
        hop = (rep, z, 1 - y, core) if h == 0 else (other, z, y, core)
        send(h, rep_at, z_at, y_at, ag_1.at[h, k], *hop)

    def third(h, k, rep_at, z_at, y_at):
        hop = (other, z, y, core) if h == 0 else (rep, z, 1 - y, core)
        send(h, rep_at, z_at, y_at, ag_2.at[h, k], *hop)

    def last(h, k, rep_at, z_at, y_at):
        send(h, rep_at, z_at, y_at, ag_core.at[h, k], rep, z, y, 1 - core)

    for k in range(1, ring):
        for h in range(2):
            send(h, rep, z, y, ag_z.at[h, k], rep, lax.rem(z + k, ring), y, core)
    for h in range(2):
        second(h, 0, rep, z, y)
        third(h, 0, rep, z, y)
        last(h, 0, rep, z, y)

    loop(cut_2, pairs, far_pair)
    for q in range(blocks):
        at = slice(q * spots, (q + 1) * spots)
        large_out[at, :] = (
            table_ref[at, :].astype(f32) - step_size * acc[:, q * width : (q + 1) * width]
        ).astype(bf16)

    for k in range(1, ring):
        z_at = lax.rem(z + ring - k, ring)
        for h in range(2):
            arrived(h, rep, z_at, y, core)
            second(h, k, rep, z_at, y)
            third(h, k, rep, z_at, y)
            last(h, k, rep, z_at, y)
    for k in range(ring):
        z_at = lax.rem(z + ring - k, ring)
        for h in range(2):
            where = (rep, z_at, 1 - y) if h == 0 else (other, z_at, y)
            arrived(h, *where, core)
            third(h, ring + k, *where)
            last(h, ring + k, *where)
    for k in range(2 * ring):
        z_at = lax.rem(z + ring - k % ring, ring)
        for h in range(2):
            if h == 0:
                where = (other, z_at, y if k < ring else 1 - y)
            else:
                where = (rep if k < ring else other, z_at, 1 - y)
            arrived(h, *where, core)
            last(h, 2 * ring + k, *where)
    for r in range(2):
        for k in range(ring):
            for y_at in range(2):
                for h in range(2):
                    arrived(h, r, k, y_at, 1 - core)

    for copy in pending + swap:
        copy.wait_send()
    own_far.wait_send()
    loop(1, groups, lambda k: out_block(k).wait_send())
    loop(1, groups, lambda k: far_out(k).wait_send())
    loop(0, 4, lambda i: first_hop(lax.rem(i, 2), i // 2).wait_send())
    loop(0, 2, lambda h: second_hop(h).wait_send())
    for h in range(2):
        loop(1, ring, lambda k: third_hop(h, k).wait_send())


def tail(ids, grads, fold, rows, ends, table, tables):
    groups = fold.shape[0]
    devices, slots = rows.shape
    ring = groups // 4
    small_count, small_rows, width = tables.shape
    part = small_count * small_rows // devices // 2
    unit = small_count * small_rows // 16
    blocks = 8
    split = (2, 2, 2, 2, ring, part, width)
    scratch = [
        pltpu.VMEM((small_count // 2, ids.shape[1]), ids.dtype),
        pltpu.VMEM((small_count // 2,) + grads.shape[1:], bf16),
        pltpu.VMEM((devices,) + fold.shape[1:], bf16),
        pltpu.VMEM((table.shape[0] // blocks, blocks * width), f32),
        pltpu.VMEM((table.shape[0] // blocks, 2 * slots), bf16),
        pltpu.VMEM((2 * slots, blocks * width), bf16),
        pltpu.VMEM((2, 2, unit, width), f32),
        pltpu.VMEM((2, 2, unit, width), bf16),
        pltpu.VMEM((2, 2, unit, width), bf16),
        pltpu.VMEM((2, unit, width), bf16),
        pltpu.VMEM((2, unit, width), bf16),
        pltpu.VMEM((2, ring, part, width), bf16),
        pltpu.VMEM((2, ring, part, width), bf16),
        pltpu.VMEM((2, part, width), bf16),
    ]
    dma = pltpu.SemaphoreType.DMA
    small, large = pl.pallas_call(
        tail_kernel,
        out_shape=(
            jax.ShapeDtypeStruct(split, bf16),
            jax.ShapeDtypeStruct(table.shape, bf16),
        ),
        in_specs=[whole(pltpu.VMEM)] * 6 + [whole(pl.ANY)],
        out_specs=(whole(pltpu.VMEM),) * 2,
        scratch_shapes=scratch + [
            dma((3,)), dma((2,)), dma((2,)),
            dma((groups,)), dma((groups,)), dma((groups,)), dma((groups,)),
            dma((2, 2)), dma((2, 2)), dma((2,)), dma((2,)), dma((2, ring)), dma((2, ring)),
            dma((2, ring)), dma((2, ring)), dma((2, 2 * ring)), dma((2, 4 * ring)), dma((2, devices)),
        ],
        compiler_params=pltpu.CompilerParams(
            collective_id=1, has_side_effects=True,
            vmem_limit_bytes=grant(ids, grads, fold, rows, ends, table, table, tables, *scratch),
        ),
        name="tail",
    )(ids, grads, fold, rows, ends, table, tables.reshape(split))
    return small.reshape(tables.shape), large


def store_kernel(small_ref, large_ref, small_out, large_out, sems):
    pieces = 4
    copies = []
    for n, (src, dst) in enumerate(((small_ref, small_out), (large_ref, large_out))):
        size = src.shape[0] // pieces
        for p in range(pieces):
            at = pl.ds(p * size, size)
            copies.append(pltpu.make_async_copy(src.at[at], dst.at[at], sems.at[n, p]))
    for copy in copies:
        copy.start()
    for copy in copies:
        copy.wait()


def store(small, large):
    return pl.pallas_call(
        store_kernel,
        out_shape=(
            jax.ShapeDtypeStruct(small.shape, small.dtype),
            jax.ShapeDtypeStruct(large.shape, large.dtype),
        ),
        in_specs=[whole(pltpu.VMEM)] * 2,
        out_specs=(whole(pl.ANY),) * 2,
        scratch_shapes=[pltpu.SemaphoreType.DMA((2, 4))],
        compiler_params=pltpu.CompilerParams(vmem_limit_bytes=16 * 1024 * 1024),
        name="store",
    )(small, large)


def shards(
    dense, small_ids, labels, small_tables, large_tables, batch_sizes, bag_ends,
    owner_row_index, w_first, b_first, w_out,
):
    groups = lax.axis_size("shard")
    first = lax.axis_index("rep") * groups
    index = first + lax.axis_index("shard")
    ends, rows, table = bag_ends[0], owner_row_index[0], large_tables[0]
    ids = jnp.transpose(small_ids)

    pooled, own_ids = pool(first[None], groups, rows, ends, table, ids)
    large, small = forward(pooled, own_ids, small_tables)
    small_grads, fold = top(
        index[None], batch_sizes, dense, labels, small, large, w_first, b_first, w_out
    )
    small_new, large_new = tail(ids, small_grads, fold, rows, ends, table, small_tables)
    small_new, large_new = store(small_new, large_new)
    return small_new, large_new[None]


def solution(mesh):
    both = ("rep", "shard")
    placed = (
        P(both, None), P(both, None), P(both), P(), P("shard", None, None), P(),
        P("shard", None, None), P("shard", None, None), P(), P(), P(),
    )
    return jax.shard_map(
        shards, mesh=mesh, in_specs=placed, out_specs=(P(), P("shard", None, None)), check_vma=False
    )
```

```python
import functools
import math

import jax
import jax.numpy as jnp
from jax import lax
from jax.experimental import pallas as pl
from jax.experimental.pallas import tpu as pltpu
from jax.sharding import PartitionSpec as P

step_size = 32.0
LANES = 128
VMEM_LIMIT = 60 * 1024 * 1024
MIB = 1024 * 1024
f32 = jnp.float32
bf16 = jnp.bfloat16


def whole(space):
    return pl.BlockSpec(memory_space=space)


def size_of(*arrays):
    return sum(math.prod(a.shape) * jnp.dtype(a.dtype).itemsize for a in arrays)


def grant(*arrays):
    return min(VMEM_LIMIT, size_of(*arrays) + 6 * MIB)


def all_but(*arrays):
    return min(VMEM_LIMIT, 63 * MIB - size_of(*arrays))


def iota(shape, axis):
    return lax.broadcasted_iota(jnp.int32, shape, axis)


def members_of(ends, slots):
    span = ends.shape[-1]
    starts = jnp.where(iota((1, span), 1) == 0, 0, pltpu.roll(ends, 1, 1))
    places = iota((slots, span), 0)
    return ((places >= starts) & (places < ends)).astype(f32).astype(bf16)


def spans_of(vec_count):
    return [(i, i * (i - 1) // 2) for i in range(1, vec_count)]


def top_kernel(
    vec_count, pad, index_ref, sizes_ref, dense_ref, labels_ref, small_ref, large_ref,
    w_ref, bias_ref, wout_ref, small_out, fold_out, vecs, gram, pairs, spread,
):
    batch, width = dense_ref.shape
    small_count = small_ref.shape[0]
    feats, bag_span = large_ref.shape[0], large_ref.shape[1]
    pair_pad = pairs.shape[1]
    pair_count = vec_count * (vec_count - 1) // 2
    scale = width ** (-0.5)
    spans = spans_of(vec_count)

    def rows_of(i):
        return pl.ds(i, batch, stride=pad)

    vecs[rows_of(0), :] = dense_ref[...].astype(f32)
    for t in range(small_count):
        vecs[rows_of(1 + t), :] = small_ref[t].astype(f32)
    sample = iota((batch, bag_span), 0)
    bag = iota((batch, bag_span), 1) * batch
    for f in range(feats):
        reach = sample * sizes_ref[f, index_ref[0]]
        hot = ((reach >= bag) & (reach < bag + batch)).astype(f32).astype(bf16)
        vecs[rows_of(1 + small_count + f), :] = jnp.dot(
            hot, large_ref[f], preferred_element_type=f32
        )
    for i in range(vec_count, pad):
        vecs[rows_of(i), :] = jnp.zeros((batch, width), f32)

    unroll = 8

    def gram_step(g, c):
        for u in range(unroll):
            at = pl.ds(pl.multiple_of((g * unroll + u) * pad, 8), pad)
            own = vecs[at, :].astype(bf16)
            gram[at, 0:pad] = lax.dot_general(
                own, own, (((1,), (1,)), ((), ())), preferred_element_type=f32
            )
        return c

    lax.fori_loop(0, batch // unroll, gram_step, 0)

    lane = iota((1, LANES), 1)
    chunk = 64
    for start in range(0, batch, chunk):
        tile = jnp.zeros((chunk, LANES), f32)
        at_tile = 0
        for i, off in spans:
            piece = gram[pl.ds(start * pad + i, chunk, stride=pad), :]
            turn = off % LANES
            if turn:
                piece = pltpu.roll(piece, turn, 1)
            low = off - at_tile * LANES
            tile = jnp.where((lane >= low) & (lane < low + i), piece, tile)
            if low + i >= LANES:
                pairs[start : start + chunk, at_tile * LANES : (at_tile + 1) * LANES] = (
                    tile * scale
                ).astype(bf16)
                at_tile += 1
                rest = low + i - LANES
                tile = jnp.where(lane < rest, piece, jnp.zeros_like(piece))
        if at_tile * LANES < pair_pad:
            pairs[start : start + chunk, at_tile * LANES : pair_pad] = (tile * scale).astype(bf16)

    block = 128
    labels_col = jnp.transpose(
        jnp.broadcast_to(labels_ref[...].astype(f32), (LANES, batch))
    )[:, 0:1]
    for start in range(0, batch, block):
        at = slice(start, start + block)
        preact = (
            jnp.dot(pairs[at, :], w_ref[0:pair_pad, :], preferred_element_type=f32)
            + jnp.dot(dense_ref[at, :], w_ref[pair_count : pair_count + width, :], preferred_element_type=f32)
            + bias_ref[...]
        )
        squash = jax.nn.sigmoid(preact)
        logits = jnp.sum(preact * squash * wout_ref[...], axis=1, keepdims=True)
        grad = jax.nn.sigmoid(logits) - labels_col[at, :]
        pre_grad = (
            grad * wout_ref[...] * (squash * (1.0 + preact * (1.0 - squash)))
        ).astype(bf16)
        for q in range(0, pair_pad, LANES):
            spread[at, q : q + LANES] = lax.dot_general(
                pre_grad, w_ref[q : q + LANES, :], (((1,), (1,)), ((), ())),
                preferred_element_type=f32,
            ) * scale

    gram[rows_of(0), :] = jnp.zeros((batch, LANES), f32)
    for i in range(vec_count, pad):
        gram[rows_of(i), :] = jnp.zeros((batch, LANES), f32)
    for start in range(0, batch, chunk):
        for i, off in spans:
            first = off // LANES
            low = off - first * LANES
            here = spread[start : start + chunk, first * LANES : (first + 1) * LANES]
            if low + i > LANES:
                after = spread[start : start + chunk, (first + 1) * LANES : (first + 2) * LANES]
                here = jnp.where(lane >= low, here, after)
            if low:
                here = pltpu.roll(here, LANES - low, 1)
            gram[pl.ds(start * pad + i, chunk, stride=pad), :] = jnp.where(lane < i, here, 0.0)

    def back_step(g, c):
        for u in range(unroll):
            at = pl.ds(pl.multiple_of((g * unroll + u) * pad, 8), pad)
            lower = gram[at, :]
            both = lower[:, 0:pad] + jnp.transpose(lower)[0:pad, :]
            vecs[at, :] = jnp.dot(
                both.astype(bf16), vecs[at, :].astype(bf16), preferred_element_type=f32
            )
        return c

    lax.fori_loop(0, batch // unroll, back_step, 0)

    for t in range(small_count):
        small_out[t] = vecs[rows_of(1 + t), :].astype(bf16)
    sample_lane = iota((bag_span, batch), 1)
    bag_row = iota((bag_span, batch), 0) * batch
    for f in range(feats):
        reach = sample_lane * sizes_ref[f, index_ref[0]]
        hot = ((reach >= bag_row) & (reach < bag_row + batch)).astype(f32).astype(bf16)
        fold_out[f] = jnp.dot(
            hot, vecs[rows_of(1 + small_count + f), :].astype(bf16), preferred_element_type=f32
        ).astype(bf16)


def top(index, sizes, dense, labels, small, large, w_first, bias, wout):
    batch, width = dense.shape
    small_count, feats, bag_span = small.shape[0], large.shape[0], large.shape[1]
    vec_count = 1 + small_count + feats
    pad = -(-vec_count // 8) * 8
    pair_count = vec_count * (vec_count - 1) // 2
    pair_pad = -(-pair_count // LANES) * LANES
    scratch = [
        pltpu.VMEM((batch * pad, width), f32),
        pltpu.VMEM((batch * pad, LANES), f32),
        pltpu.VMEM((batch, pair_pad), bf16),
        pltpu.VMEM((batch, pair_pad), f32),
    ]
    return pl.pallas_call(
        functools.partial(top_kernel, vec_count, pad),
        out_shape=(
            jax.ShapeDtypeStruct((small_count, batch, width), bf16),
            jax.ShapeDtypeStruct((feats, bag_span, width), bf16),
        ),
        in_specs=[whole(pltpu.SMEM)] * 2 + [whole(pltpu.VMEM)] * 7,
        out_specs=(whole(pltpu.VMEM), whole(pltpu.VMEM)),
        scratch_shapes=scratch,
        compiler_params=pltpu.CompilerParams(
            vmem_limit_bytes=grant(dense, small, large, small, large, w_first, *scratch)
        ),
        name="top",
    )(
        index, sizes, dense, labels[None, :], small, large, w_first,
        bias[None, :], wout[None, :],
    )


def greet_all():
    copies, groups = lax.axis_size("rep"), lax.axis_size("shard")
    devices = copies * groups
    index = lax.axis_index("rep") * groups + lax.axis_index("shard")
    barrier = pltpu.get_barrier_semaphore()

    def greet(k, c):
        other = lax.rem(index + k, devices)
        pl.semaphore_signal(
            barrier, inc=1, device_id={"rep": other // groups, "shard": lax.rem(other, groups)},
            device_id_type=pl.DeviceIdType.MESH,
        )
        return c

    lax.fori_loop(1, devices, greet, 0)
    pl.semaphore_wait(barrier, devices - 1)


def remote(src, dst, send, recv, rep, shard):
    return pltpu.make_async_remote_copy(
        src_ref=src, dst_ref=dst, send_sem=send, recv_sem=recv,
        device_id={"rep": rep, "shard": shard}, device_id_type=pl.DeviceIdType.MESH,
    )


def head_kernel(
    rows_hbm, ends_hbm, ids_hbm, table_hbm, tables_hbm, large_out, small_out,
    rows, ends, ids, narrow, wide, tables, by_sample, outbox, send, recv, local,
):
    groups = lax.axis_size("shard")
    rep, me = lax.axis_index("rep"), lax.axis_index("shard")
    slots = rows.shape[1]
    arrays = ((rows_hbm, rows), (ends_hbm, ends), (ids_hbm, ids), (table_hbm, narrow), (tables_hbm, tables))
    fetch = [pltpu.make_async_copy(src, dst, local.at[n]) for n, (src, dst) in enumerate(arrays)]
    for copy in fetch:
        copy.start()
    greet_all()
    for copy in fetch[:4]:
        copy.wait()
    wide[...] = narrow[...].astype(f32)

    def block(off):
        to = lax.rem(me + off, groups)
        return remote(outbox.at[to], large_out.at[me], send.at[off], recv.at[off], rep, to)

    def block_in(off):
        at = lax.rem(me + groups - off, groups)
        return remote(outbox.at[at], large_out.at[at], send.at[off], recv.at[off], rep, at)

    def loop(low, high, act):
        def body(k, c):
            act(k)
            return c

        lax.fori_loop(low, high, body, 0)

    def give(i):
        off = lax.rem(groups // 2 + i, groups)
        to = lax.rem(me + off, groups)
        d = rep * groups + to
        picked = [
            jnp.concatenate([wide[pl.ds(rows[d, s + u], 1), :] for u in range(8)], axis=0)
            for s in range(0, slots, 8)
        ]
        pooled = lax.dot_general(
            members_of(ends[pl.ds(d, 1), :], slots), jnp.concatenate(picked, axis=0).astype(bf16),
            (((0,), (0,)), ((), ())), preferred_element_type=f32,
        )
        outbox[to] = pooled.astype(bf16)

        @pl.when(off != 0)
        def _():
            block(off).start()

    loop(0, groups, give)
    by_sample[...] = jnp.transpose(ids[...])
    large_out[me] = outbox[me]
    fetch[4].wait()
    at_row = iota((by_sample.shape[0], tables.shape[1]), 1)
    for t in range(tables.shape[0]):
        hot = (by_sample[:, t : t + 1] == at_row).astype(f32).astype(bf16)
        small_out[t] = jnp.dot(hot, tables[t], preferred_element_type=f32).astype(bf16)
    loop(1, groups, lambda off: block_in(off).wait_recv())
    loop(1, groups, lambda off: block(off).wait_send())


def head(groups, rows, ends, ids, table, tables, w_first):
    large = jax.ShapeDtypeStruct((groups, ends.shape[1], table.shape[1]), bf16)
    small = jax.ShapeDtypeStruct((tables.shape[0], ids.shape[1], tables.shape[2]), tables.dtype)
    scratch = [
        pltpu.VMEM(ends.shape, ends.dtype),
        pltpu.VMEM(ids.shape, ids.dtype),
        pltpu.VMEM(table.shape, table.dtype),
        pltpu.VMEM(table.shape, f32),
        pltpu.VMEM(tables.shape, tables.dtype),
        pltpu.VMEM((ids.shape[1], ids.shape[0]), ids.dtype),
        pltpu.VMEM(large.shape, bf16),
    ]
    dma = pltpu.SemaphoreType.DMA
    return pl.pallas_call(
        head_kernel,
        out_shape=(large, small),
        in_specs=[whole(pltpu.HBM)] * 5,
        out_specs=(whole(pltpu.VMEM),) * 2,
        scratch_shapes=[pltpu.SMEM(rows.shape, rows.dtype)] + scratch
        + [dma((groups,)), dma((groups,)), dma((5,))],
        compiler_params=pltpu.CompilerParams(
            collective_id=0, has_side_effects=True,
            vmem_limit_bytes=max(grant(large, small, *scratch), all_but(large, small, w_first)),
        ),
        name="head",
    )(rows, ends, ids, table, tables)


def tail_kernel(
    ids_ref, grads_ref, fold_ref, rows_ref, ends_ref, table_ref, tables_ref, small_out, large_out,
    peer_ids, peer_grads, folds, acc, lhs_0, lhs_1, rhs_0, rhs_1, keep, sent, came, sent_2, came_2, sent_3, came_3,
    prior, local, peer_s, peer_r, fold_s, fold_r, far_s, far_r, rs1_s, rs1_r, rs2_s, rs2_r,
    rs3_s, rs3_r, ag_z, ag_1, ag_2, ag_core, ag_r,
):
    groups = lax.axis_size("shard")
    ring = groups // 4
    rep, me = lax.axis_index("rep"), lax.axis_index("shard")
    z, y, core = me // 4, lax.rem(me, 4) // 2, lax.rem(me, 2)
    other = 1 - rep
    small_count, batch = ids_ref.shape
    half_count = small_count // 2
    per_unit = small_count // 16
    small_rows = keep.shape[2] // per_unit
    part = small_out.shape[5]
    slots = rows_ref.shape[1]
    spots = acc.shape[0]
    width = table_ref.shape[1]
    blocks = acc.shape[1] // width

    def shard_of(z_at, y_at, core_at):
        return z_at * 4 + y_at * 2 + core_at

    def loop(low, high, act):
        def body(k, c):
            act(k)
            return c

        lax.fori_loop(low, high, body, 0)

    peer = shard_of(z, y, 1 - core)
    away = (1 - core) * half_count
    swap = [
        remote(ids_ref.at[pl.ds(pl.multiple_of(away, 8), half_count)], peer_ids, peer_s.at[0], peer_r.at[0], rep, peer),
        remote(grads_ref.at[pl.ds(away, half_count)], peer_grads, peer_s.at[1], peer_r.at[1], rep, peer),
    ]

    def out_block(k):
        to = lax.rem(me + k, groups)
        return remote(fold_ref.at[to], folds.at[rep * groups + me], fold_s.at[k], fold_r.at[k], rep, to)

    def in_block(k):
        at = lax.rem(me + groups - k, groups)
        return remote(fold_ref.at[at], folds.at[rep * groups + at], fold_s.at[k], fold_r.at[k], rep, at)

    def far_out(k):
        slot = folds.at[rep * groups + lax.rem(me + groups - k, groups)]
        return remote(slot, slot, far_s.at[k], far_r.at[k], other, me)

    def far_in(k):
        slot = folds.at[other * groups + lax.rem(me + groups - k, groups)]
        return remote(slot, slot, far_s.at[k], far_r.at[k], other, me)

    own_far = remote(fold_ref.at[me], folds.at[rep * groups + me], far_s.at[0], far_r.at[0], other, me)

    greet_all()
    for copy in swap:
        copy.start()
    loop(1, groups, lambda k: out_block(k).start())
    own_far.start()
    fetch = [
        pltpu.make_async_copy(tables_ref.at[core, h, rep, y, z], prior.at[h], local.at[h])
        for h in range(2)
    ]
    for copy in fetch:
        copy.start()
    folds[rep * groups + me] = fold_ref[me]
    acc[...] = jnp.zeros_like(acc)
    for copy in swap:
        copy.wait_recv()

    row = iota((small_rows, batch), 0)

    def dense(t):
        own = (row == ids_ref[pl.ds(core * half_count + t, 1), :]).astype(f32).astype(bf16)
        far = (row == peer_ids[pl.ds(t, 1), :]).astype(f32).astype(bf16)
        return jnp.dot(
            own, grads_ref[core * half_count + t], preferred_element_type=f32
        ) + jnp.dot(far, peer_grads[t], preferred_element_type=f32)

    def first_hop(h, s):
        to_rep = rep + (1 - h) * (1 - 2 * rep)
        to_y = y + h * (1 - 2 * y)
        return remote(
            sent.at[h, s], came.at[h, s], rs1_s.at[h, s], rs1_r.at[h, s], to_rep, shard_of(z, to_y, core)
        )

    def second_hop(h):
        to_rep = rep + h * (1 - 2 * rep)
        to_y = y + (1 - h) * (1 - 2 * y)
        return remote(
            sent_2.at[h], came_2.at[h], rs2_s.at[h], rs2_r.at[h], to_rep, shard_of(z, to_y, core)
        )

    def third_hop(h, k):
        to = lax.rem(z + k, ring)
        return remote(
            sent_3.at[h, to], came_3.at[h, z], rs3_s.at[h, k], rs3_r.at[h, k], rep, shard_of(to, y, core)
        )

    def third_in(h, k):
        at = lax.rem(z + ring - k, ring)
        return remote(
            sent_3.at[h, at], came_3.at[h, at], rs3_s.at[h, k], rs3_r.at[h, k], rep, shard_of(at, y, core)
        )

    def give(i):
        s, h = i // 2, lax.rem(i, 2)
        r_at = other + h * s * (2 * rep - 1)
        y_at = (1 - y) + (1 - h) * s * (2 * y - 1)
        first = ((h * 2 + r_at) * 2 + y_at) * per_unit
        for j in range(per_unit):
            sent[h, s, j * small_rows : (j + 1) * small_rows, :] = dense(first + j).astype(bf16)
        first_hop(h, s).start()

    def hold(i):
        s, h = i // 2, lax.rem(i, 2)
        r_at = rep + h * (1 - s) * (1 - 2 * rep)
        y_at = y + (1 - h) * (1 - s) * (1 - 2 * y)
        first = ((h * 2 + r_at) * 2 + y_at) * per_unit
        for j in range(per_unit):
            keep[h, s, j * small_rows : (j + 1) * small_rows, :] = dense(first + j)

    loop(0, 4, give)
    loop(0, 4, hold)

    spot = iota((spots, slots), 0)

    def place_rows(d, v, lhs, rhs):
        members = members_of(ends_ref[pl.ds(d, 1), :], slots)
        moved = jnp.dot(members, folds[d], preferred_element_type=f32)
        at = rows_ref[pl.ds(d, 1), :]
        block = at // spots
        wide = jnp.transpose(jnp.broadcast_to(block.astype(f32), (width, slots)))
        for q in range(blocks):
            rhs[v * slots : (v + 1) * slots, q * width : (q + 1) * width] = jnp.where(
                wide == q, moved, 0.0
            ).astype(bf16)
        lhs[:, v * slots : (v + 1) * slots] = (spot == at - block * spots).astype(f32).astype(bf16)

    def take(k):
        in_block(k).wait_recv()
        far_out(k).start()

    def get(p):
        @pl.when((p > 0) & (p < groups // 2))
        def _():
            take(2 * p)

        @pl.when(p < groups // 2)
        def _():
            take(2 * p + 1)

        @pl.when((p >= groups // 2) & (p < groups))
        def _():
            far_in(2 * p - groups).wait_recv()
            far_in(2 * p + 1 - groups).wait_recv()

    def owner(k):
        side = k // groups
        at = lax.rem(me + groups - (k - side * groups), groups)
        return (rep + side * (1 - 2 * rep)) * groups + at

    step = 2 * width

    def make(p, lhs, rhs):
        place_rows(owner(2 * p), 0, lhs, rhs)
        place_rows(owner(2 * p + 1), 1, lhs, rhs)

    def multiply(lhs, rhs):
        for n in range(0, acc.shape[1], step):
            acc[:, n : n + step] += jnp.dot(lhs[...], rhs[:, n : n + step], preferred_element_type=f32)

    def pairs(i):
        get(2 * i + 1)
        make(2 * i + 1, lhs_1, rhs_1)
        multiply(lhs_0, rhs_0)
        get(2 * i + 2)
        make(jnp.minimum(2 * i + 2, groups - 1), lhs_0, rhs_0)
        multiply(lhs_1, rhs_1)

    turns = groups // 2
    cut_1, cut_2, cut_3 = turns // 8, turns // 2, turns * 7 // 8
    get(0)
    make(0, lhs_0, rhs_0)
    loop(0, cut_1, pairs)

    def turn(h):
        first_hop(h, 0).wait_recv()
        sent_2[h] = (keep[h, 0] + came[h, 0].astype(f32)).astype(bf16)
        second_hop(h).start()

    loop(0, 2, turn)
    loop(cut_1, cut_2, pairs)

    def along(h):
        first_hop(h, 1).wait_recv()
        second_hop(h).wait_recv()
        total = keep[h, 1] + came[h, 1].astype(f32) + came_2[h].astype(f32)
        keep[h, 1] = total
        sent_3[h] = total.astype(bf16).reshape(ring, part, width)
        loop(1, ring, lambda k: third_hop(h, k).start())

    loop(0, 2, along)
    loop(cut_2, cut_3, pairs)

    for copy in fetch:
        copy.wait()

    def own_part(h):
        total = keep[h, 1, pl.ds(pl.multiple_of(z * part, part), part), :]
        for k in range(1, ring):
            third_in(h, k).wait_recv()
            total = total + came_3[h, lax.rem(z + ring - k, ring)].astype(f32)
        small_out[core, h, rep, y, z] = (prior[h].astype(f32) - step_size * total).astype(bf16)

    loop(0, 2, own_part)

    pending = []

    def place(h, rep_at, z_at, y_at, core_at):
        return small_out.at[core_at, h, rep_at, y_at, z_at]

    def slot_of(rep_at, z_at, y_at, core_at):
        return rep_at * groups + shard_of(z_at, y_at, core_at)

    def send(h, rep_at, z_at, y_at, sem, to_rep, to_z, to_y, to_core):
        block = place(h, rep_at, z_at, y_at, core)
        copy = remote(
            block, block, sem, ag_r.at[h, slot_of(rep_at, z_at, y_at, core)],
            to_rep, shard_of(to_z, to_y, to_core),
        )
        copy.start()
        pending.append(copy)

    def arrived(h, rep_at, z_at, y_at, core_at):
        block = place(h, rep_at, z_at, y_at, core_at)
        remote(
            block, block, local.at[2], ag_r.at[h, slot_of(rep_at, z_at, y_at, core_at)], rep, peer
        ).wait_recv()

    def second(h, k, rep_at, z_at, y_at):
        hop = (rep, z, 1 - y, core) if h == 0 else (other, z, y, core)
        send(h, rep_at, z_at, y_at, ag_1.at[h, k], *hop)

    def third(h, k, rep_at, z_at, y_at):
        hop = (other, z, y, core) if h == 0 else (rep, z, 1 - y, core)
        send(h, rep_at, z_at, y_at, ag_2.at[h, k], *hop)

    def last(h, k, rep_at, z_at, y_at):
        send(h, rep_at, z_at, y_at, ag_core.at[h, k], rep, z, y, 1 - core)

    for k in range(1, ring):
        for h in range(2):
            send(h, rep, z, y, ag_z.at[h, k], rep, lax.rem(z + k, ring), y, core)
    for h in range(2):
        second(h, 0, rep, z, y)
        third(h, 0, rep, z, y)
        last(h, 0, rep, z, y)

    loop(cut_3, turns, pairs)
    for q in range(blocks):
        at = slice(q * spots, (q + 1) * spots)
        large_out[at, :] = (
            table_ref[at, :].astype(f32) - step_size * acc[:, q * width : (q + 1) * width]
        ).astype(bf16)

    for k in range(1, ring):
        z_at = lax.rem(z + ring - k, ring)
        for h in range(2):
            arrived(h, rep, z_at, y, core)
            second(h, k, rep, z_at, y)
            third(h, k, rep, z_at, y)
            last(h, k, rep, z_at, y)
    for k in range(ring):
        z_at = lax.rem(z + ring - k, ring)
        for h in range(2):
            where = (rep, z_at, 1 - y) if h == 0 else (other, z_at, y)
            arrived(h, *where, core)
            third(h, ring + k, *where)
            last(h, ring + k, *where)
    for k in range(2 * ring):
        z_at = lax.rem(z + ring - k % ring, ring)
        for h in range(2):
            if h == 0:
                where = (other, z_at, y if k < ring else 1 - y)
            else:
                where = (rep if k < ring else other, z_at, 1 - y)
            arrived(h, *where, core)
            last(h, 2 * ring + k, *where)
    for r in range(2):
        for k in range(ring):
            for y_at in range(2):
                for h in range(2):
                    arrived(h, r, k, y_at, 1 - core)

    for copy in pending + swap:
        copy.wait_send()
    own_far.wait_send()
    loop(1, groups, lambda k: out_block(k).wait_send())
    loop(1, groups, lambda k: far_out(k).wait_send())
    loop(0, 4, lambda i: first_hop(lax.rem(i, 2), i // 2).wait_send())
    loop(0, 2, lambda h: second_hop(h).wait_send())
    for h in range(2):
        loop(1, ring, lambda k: third_hop(h, k).wait_send())


def tail(ids, grads, fold, rows, ends, table, tables):
    groups = fold.shape[0]
    devices, slots = rows.shape
    ring = groups // 4
    small_count, small_rows, width = tables.shape
    part = small_count * small_rows // devices // 2
    unit = small_count * small_rows // 16
    blocks = 8
    split = (2, 2, 2, 2, ring, part, width)
    scratch = [
        pltpu.VMEM((small_count // 2, ids.shape[1]), ids.dtype),
        pltpu.VMEM((small_count // 2,) + grads.shape[1:], bf16),
        pltpu.VMEM((devices,) + fold.shape[1:], bf16),
        pltpu.VMEM((table.shape[0] // blocks, blocks * width), f32),
        pltpu.VMEM((table.shape[0] // blocks, 2 * slots), bf16),
        pltpu.VMEM((table.shape[0] // blocks, 2 * slots), bf16),
        pltpu.VMEM((2 * slots, blocks * width), bf16),
        pltpu.VMEM((2 * slots, blocks * width), bf16),
        pltpu.VMEM((2, 2, unit, width), f32),
        pltpu.VMEM((2, 2, unit, width), bf16),
        pltpu.VMEM((2, 2, unit, width), bf16),
        pltpu.VMEM((2, unit, width), bf16),
        pltpu.VMEM((2, unit, width), bf16),
        pltpu.VMEM((2, ring, part, width), bf16),
        pltpu.VMEM((2, ring, part, width), bf16),
        pltpu.VMEM((2, part, width), bf16),
    ]
    dma = pltpu.SemaphoreType.DMA
    small, large = pl.pallas_call(
        tail_kernel,
        out_shape=(
            jax.ShapeDtypeStruct(split, bf16),
            jax.ShapeDtypeStruct(table.shape, bf16),
        ),
        in_specs=[whole(pltpu.VMEM)] * 6 + [whole(pl.ANY)],
        out_specs=(whole(pltpu.VMEM),) * 2,
        scratch_shapes=scratch + [
            dma((3,)), dma((2,)), dma((2,)),
            dma((groups,)), dma((groups,)), dma((groups,)), dma((groups,)),
            dma((2, 2)), dma((2, 2)), dma((2,)), dma((2,)), dma((2, ring)), dma((2, ring)),
            dma((2, ring)), dma((2, ring)), dma((2, 2 * ring)), dma((2, 4 * ring)), dma((2, devices)),
        ],
        compiler_params=pltpu.CompilerParams(
            collective_id=1, has_side_effects=True,
            vmem_limit_bytes=grant(ids, grads, fold, rows, ends, table, table, tables, *scratch),
        ),
        name="tail",
    )(ids, grads, fold, rows, ends, table, tables.reshape(split))
    return small.reshape(tables.shape), large


def store_kernel(small_ref, large_ref, small_out, large_out, sems):
    pieces = 4
    copies = []
    for n, (src, dst) in enumerate(((small_ref, small_out), (large_ref, large_out))):
        size = src.shape[0] // pieces
        for p in range(pieces):
            at = pl.ds(p * size, size)
            copies.append(pltpu.make_async_copy(src.at[at], dst.at[at], sems.at[n, p]))
    for copy in copies:
        copy.start()
    for copy in copies:
        copy.wait()


def store(small, large):
    return pl.pallas_call(
        store_kernel,
        out_shape=(
            jax.ShapeDtypeStruct(small.shape, small.dtype),
            jax.ShapeDtypeStruct(large.shape, large.dtype),
        ),
        in_specs=[whole(pltpu.VMEM)] * 2,
        out_specs=(whole(pl.ANY),) * 2,
        scratch_shapes=[pltpu.SemaphoreType.DMA((2, 4))],
        compiler_params=pltpu.CompilerParams(vmem_limit_bytes=16 * 1024 * 1024),
        name="store",
    )(small, large)


def shards(
    dense, small_ids, labels, small_tables, large_tables, batch_sizes, bag_ends,
    owner_row_index, w_first, b_first, w_out,
):
    groups = lax.axis_size("shard")
    index = lax.axis_index("rep") * groups + lax.axis_index("shard")
    ends, rows, table = bag_ends[0], owner_row_index[0], large_tables[0]
    ids = jnp.transpose(small_ids)

    large, small = head(groups, rows, ends, ids, table, small_tables, w_first)
    small_grads, fold = top(
        index[None], batch_sizes, dense, labels, small, large, w_first, b_first, w_out
    )
    small_new, large_new = tail(ids, small_grads, fold, rows, ends, table, small_tables)
    small_new, large_new = store(small_new, large_new)
    return small_new, large_new[None]


def solution(mesh):
    both = ("rep", "shard")
    placed = (
        P(both, None), P(both, None), P(both), P(), P("shard", None, None), P(),
        P("shard", None, None), P("shard", None, None), P(), P(), P(),
    )
    return jax.shard_map(
        shards, mesh=mesh, in_specs=placed, out_specs=(P(), P("shard", None, None)), check_vma=False
    )
```

```python
import functools
import math

import jax
import jax.numpy as jnp
from jax import lax
from jax.experimental import pallas as pl
from jax.experimental.pallas import tpu as pltpu
from jax.sharding import PartitionSpec as P

step_size = 32.0
LANES = 128
VMEM_LIMIT = 60 * 1024 * 1024
MIB = 1024 * 1024
f32 = jnp.float32
bf16 = jnp.bfloat16


def whole(space):
    return pl.BlockSpec(memory_space=space)


def size_of(*arrays):
    return sum(math.prod(a.shape) * jnp.dtype(a.dtype).itemsize for a in arrays)


def grant(*arrays):
    return min(VMEM_LIMIT, size_of(*arrays) + 6 * MIB)


def all_but(*arrays):
    return min(VMEM_LIMIT, 63 * MIB - size_of(*arrays))


def iota(shape, axis):
    return lax.broadcasted_iota(jnp.int32, shape, axis)


def members_of(ends, slots):
    span = ends.shape[-1]
    starts = jnp.where(iota((1, span), 1) == 0, 0, pltpu.roll(ends, 1, 1))
    places = iota((slots, span), 0)
    return ((places >= starts) & (places < ends)).astype(f32).astype(bf16)


def spans_of(vec_count):
    return [(i, i * (i - 1) // 2) for i in range(1, vec_count)]


def top_kernel(
    vec_count, group, pad, index_ref, sizes_ref, dense_ref, labels_ref, small_ref, large_ref,
    w_ref, bias_ref, wout_ref, small_out, fold_out, vecs, gram, pairs, spread,
):
    batch, width = dense_ref.shape
    small_count = small_ref.shape[0]
    feats, bag_span = large_ref.shape[0], large_ref.shape[1]
    pair_pad = pairs.shape[1]
    pair_count = vec_count * (vec_count - 1) // 2
    scale = width ** (-0.5)
    spans = spans_of(vec_count)

    def rows_of(i):
        return pl.ds(i, batch, stride=pad)

    vecs[rows_of(0), :] = dense_ref[...].astype(f32)
    for t in range(small_count):
        vecs[rows_of(1 + t), :] = small_ref[t].astype(f32)
    sample = iota((batch, bag_span), 0)
    bag = iota((batch, bag_span), 1) * batch
    for f in range(feats):
        reach = sample * sizes_ref[f, index_ref[0]]
        hot = ((reach >= bag) & (reach < bag + batch)).astype(f32).astype(bf16)
        vecs[rows_of(1 + small_count + f), :] = jnp.dot(
            hot, large_ref[f], preferred_element_type=f32
        )
    for i in range(vec_count, pad):
        vecs[rows_of(i), :] = jnp.zeros((batch, width), f32)

    unroll = 8

    many = batch // group
    tall = group * pad

    def gram_step(g, c):
        for u in range(unroll):
            at = pl.ds(pl.multiple_of((g * unroll + u) * tall, 8), tall)
            own = vecs[at, :].astype(bf16)
            gram[at, 0:tall] = lax.dot_general(
                own, own, (((1,), (1,)), ((), ())), preferred_element_type=f32
            )
        return c

    lax.fori_loop(0, many // unroll, gram_step, 0)

    lane = iota((1, LANES), 1)
    chunk = 64
    places = [(v, start) for v in range(group) for start in range(0, many, chunk)]

    def strided(v, start, i, size):
        return pl.ds((start * group + v) * pad + i, size, stride=tall)

    for v, start in places:
        tile = jnp.zeros((chunk, LANES), f32)
        at_tile = 0
        row = v * many + start
        for i, off in spans:
            piece = gram[strided(v, start, i, chunk), :]
            turn = (off - v * pad) % LANES
            if turn:
                piece = pltpu.roll(piece, turn, 1)
            low = off - at_tile * LANES
            tile = jnp.where((lane >= low) & (lane < low + i), piece, tile)
            if low + i >= LANES:
                pairs[row : row + chunk, at_tile * LANES : (at_tile + 1) * LANES] = (
                    tile * scale
                ).astype(bf16)
                at_tile += 1
                rest = low + i - LANES
                tile = jnp.where(lane < rest, piece, jnp.zeros_like(piece))
        if at_tile * LANES < pair_pad:
            pairs[row : row + chunk, at_tile * LANES : pair_pad] = (tile * scale).astype(bf16)

    block = min(128, many)
    gram[0:batch, :] = jnp.transpose(
        jnp.broadcast_to(labels_ref[...].astype(f32), (LANES, batch))
    )
    labels_of = [gram[pl.ds(v, many, stride=group), :][:, 0:1] for v in range(group)]
    for v, start in [(v, start) for v in range(group) for start in range(0, many, block)]:
        at = slice(v * many + start, v * many + start + block)
        own_dense = vecs[strided(v, start, 0, block), :].astype(bf16)
        preact = (
            jnp.dot(pairs[at, :], w_ref[0:pair_pad, :], preferred_element_type=f32)
            + jnp.dot(own_dense, w_ref[pair_count : pair_count + width, :], preferred_element_type=f32)
            + bias_ref[...]
        )
        squash = jax.nn.sigmoid(preact)
        logits = jnp.sum(preact * squash * wout_ref[...], axis=1, keepdims=True)
        grad = jax.nn.sigmoid(logits) - labels_of[v][start : start + block, :]
        pre_grad = (
            grad * wout_ref[...] * (squash * (1.0 + preact * (1.0 - squash)))
        ).astype(bf16)
        for q in range(0, pair_pad, LANES):
            spread[at, q : q + LANES] = lax.dot_general(
                pre_grad, w_ref[q : q + LANES, :], (((1,), (1,)), ((), ())),
                preferred_element_type=f32,
            ) * scale

    gram[rows_of(0), :] = jnp.zeros((batch, LANES), f32)
    for i in range(vec_count, pad):
        gram[rows_of(i), :] = jnp.zeros((batch, LANES), f32)
    for v, start in places:
        row = v * many + start
        for i, off in spans:
            first = off // LANES
            low = off - first * LANES
            here = spread[row : row + chunk, first * LANES : (first + 1) * LANES]
            if low + i > LANES:
                after = spread[row : row + chunk, (first + 1) * LANES : (first + 2) * LANES]
                here = jnp.where(lane >= low, here, after)
            turn = (v * pad - low) % LANES
            if turn:
                here = pltpu.roll(here, turn, 1)
            gram[strided(v, start, i, chunk), :] = jnp.where(
                (lane >= v * pad) & (lane < v * pad + i), here, 0.0
            )

    def back_step(g, c):
        for u in range(unroll):
            at = pl.ds(pl.multiple_of((g * unroll + u) * tall, 8), tall)
            lower = gram[at, :]
            both = lower[:, 0:tall] + jnp.transpose(lower)[0:tall, :]
            vecs[at, :] = jnp.dot(
                both.astype(bf16), vecs[at, :].astype(bf16), preferred_element_type=f32
            )
        return c

    lax.fori_loop(0, many // unroll, back_step, 0)

    for t in range(small_count):
        small_out[t] = vecs[rows_of(1 + t), :].astype(bf16)
    sample_lane = iota((bag_span, batch), 1)
    bag_row = iota((bag_span, batch), 0) * batch
    for f in range(feats):
        reach = sample_lane * sizes_ref[f, index_ref[0]]
        hot = ((reach >= bag_row) & (reach < bag_row + batch)).astype(f32).astype(bf16)
        fold_out[f] = jnp.dot(
            hot, vecs[rows_of(1 + small_count + f), :].astype(bf16), preferred_element_type=f32
        ).astype(bf16)


def top(index, sizes, dense, labels, small, large, w_first, bias, wout):
    batch, width = dense.shape
    small_count, feats, bag_span = small.shape[0], large.shape[0], large.shape[1]
    vec_count = 1 + small_count + feats
    group = max(1, LANES // (-(-vec_count // 8) * 8))
    tiles = -(-group * vec_count // 8)
    if tiles % 2 == 0 and (tiles + 1) * 8 <= LANES:
        tiles += 1
    pad = tiles * 8 // group
    pair_count = vec_count * (vec_count - 1) // 2
    pair_pad = -(-pair_count // LANES) * LANES
    scratch = [
        pltpu.VMEM((batch * pad, width), f32),
        pltpu.VMEM((batch * pad, LANES), f32),
        pltpu.VMEM((batch, pair_pad), bf16),
        pltpu.VMEM((batch, pair_pad), f32),
    ]
    return pl.pallas_call(
        functools.partial(top_kernel, vec_count, group, pad),
        out_shape=(
            jax.ShapeDtypeStruct((small_count, batch, width), bf16),
            jax.ShapeDtypeStruct((feats, bag_span, width), bf16),
        ),
        in_specs=[whole(pltpu.SMEM)] * 2 + [whole(pltpu.VMEM)] * 7,
        out_specs=(whole(pltpu.VMEM), whole(pltpu.VMEM)),
        scratch_shapes=scratch,
        compiler_params=pltpu.CompilerParams(
            vmem_limit_bytes=grant(dense, small, large, small, large, w_first, *scratch)
        ),
        name="top",
    )(
        index, sizes, dense, labels[None, :], small, large, w_first,
        bias[None, :], wout[None, :],
    )


def greet_all():
    copies, groups = lax.axis_size("rep"), lax.axis_size("shard")
    devices = copies * groups
    index = lax.axis_index("rep") * groups + lax.axis_index("shard")
    barrier = pltpu.get_barrier_semaphore()

    def greet(k, c):
        other = lax.rem(index + k, devices)
        pl.semaphore_signal(
            barrier, inc=1, device_id={"rep": other // groups, "shard": lax.rem(other, groups)},
            device_id_type=pl.DeviceIdType.MESH,
        )
        return c

    lax.fori_loop(1, devices, greet, 0)
    pl.semaphore_wait(barrier, devices - 1)


def remote(src, dst, send, recv, rep, shard):
    return pltpu.make_async_remote_copy(
        src_ref=src, dst_ref=dst, send_sem=send, recv_sem=recv,
        device_id={"rep": rep, "shard": shard}, device_id_type=pl.DeviceIdType.MESH,
    )


def head_kernel(
    rows_hbm, ends_hbm, ids_hbm, table_hbm, tables_hbm, large_out, small_out,
    rows, ends, ids, narrow, wide, tables, by_sample, outbox, send, recv, local,
):
    groups = lax.axis_size("shard")
    rep, me = lax.axis_index("rep"), lax.axis_index("shard")
    slots = rows.shape[1]
    arrays = ((rows_hbm, rows), (ends_hbm, ends), (ids_hbm, ids), (table_hbm, narrow), (tables_hbm, tables))
    fetch = [pltpu.make_async_copy(src, dst, local.at[n]) for n, (src, dst) in enumerate(arrays)]
    for copy in fetch:
        copy.start()
    greet_all()
    for copy in fetch[:4]:
        copy.wait()
    wide[...] = narrow[...].astype(f32)

    def block(off):
        to = lax.rem(me + off, groups)
        return remote(outbox.at[to], large_out.at[me], send.at[off], recv.at[off], rep, to)

    def block_in(off):
        at = lax.rem(me + groups - off, groups)
        return remote(outbox.at[at], large_out.at[at], send.at[off], recv.at[off], rep, at)

    def loop(low, high, act):
        def body(k, c):
            act(k)
            return c

        lax.fori_loop(low, high, body, 0)

    def give(i):
        off = lax.rem(groups // 2 + i, groups)
        to = lax.rem(me + off, groups)
        d = rep * groups + to
        picked = [
            jnp.concatenate([wide[pl.ds(rows[d, s + u], 1), :] for u in range(8)], axis=0)
            for s in range(0, slots, 8)
        ]
        pooled = lax.dot_general(
            members_of(ends[pl.ds(d, 1), :], slots), jnp.concatenate(picked, axis=0).astype(bf16),
            (((0,), (0,)), ((), ())), preferred_element_type=f32,
        )
        outbox[to] = pooled.astype(bf16)

        @pl.when(off != 0)
        def _():
            block(off).start()

    loop(0, groups, give)
    by_sample[...] = jnp.transpose(ids[...])
    large_out[me] = outbox[me]
    fetch[4].wait()
    at_row = iota((by_sample.shape[0], tables.shape[1]), 1)
    for t in range(tables.shape[0]):
        hot = (by_sample[:, t : t + 1] == at_row).astype(f32).astype(bf16)
        small_out[t] = jnp.dot(hot, tables[t], preferred_element_type=f32).astype(bf16)
    loop(1, groups, lambda off: block_in(off).wait_recv())
    loop(1, groups, lambda off: block(off).wait_send())


def head(groups, rows, ends, ids, table, tables, w_first):
    large = jax.ShapeDtypeStruct((groups, ends.shape[1], table.shape[1]), bf16)
    small = jax.ShapeDtypeStruct((tables.shape[0], ids.shape[1], tables.shape[2]), tables.dtype)
    scratch = [
        pltpu.VMEM(ends.shape, ends.dtype),
        pltpu.VMEM(ids.shape, ids.dtype),
        pltpu.VMEM(table.shape, table.dtype),
        pltpu.VMEM(table.shape, f32),
        pltpu.VMEM(tables.shape, tables.dtype),
        pltpu.VMEM((ids.shape[1], ids.shape[0]), ids.dtype),
        pltpu.VMEM(large.shape, bf16),
    ]
    dma = pltpu.SemaphoreType.DMA
    return pl.pallas_call(
        head_kernel,
        out_shape=(large, small),
        in_specs=[whole(pltpu.HBM)] * 5,
        out_specs=(whole(pltpu.VMEM),) * 2,
        scratch_shapes=[pltpu.SMEM(rows.shape, rows.dtype)] + scratch
        + [dma((groups,)), dma((groups,)), dma((5,))],
        compiler_params=pltpu.CompilerParams(
            collective_id=0, has_side_effects=True,
            vmem_limit_bytes=max(grant(large, small, *scratch), all_but(large, small, w_first)),
        ),
        name="head",
    )(rows, ends, ids, table, tables)


def tail_kernel(
    ids_ref, grads_ref, fold_ref, rows_ref, ends_ref, table_ref, tables_ref, small_out, large_out,
    peer_ids, peer_grads, folds, acc, lhs_0, lhs_1, rhs_0, rhs_1, keep, sent, came, sent_2, came_2, sent_3, came_3,
    prior, local, peer_s, peer_r, fold_s, fold_r, far_s, far_r, rs1_s, rs1_r, rs2_s, rs2_r,
    rs3_s, rs3_r, ag_z, ag_1, ag_2, ag_core, ag_r,
):
    groups = lax.axis_size("shard")
    ring = groups // 4
    rep, me = lax.axis_index("rep"), lax.axis_index("shard")
    z, y, core = me // 4, lax.rem(me, 4) // 2, lax.rem(me, 2)
    other = 1 - rep
    small_count, batch = ids_ref.shape
    half_count = small_count // 2
    per_unit = small_count // 16
    small_rows = keep.shape[2] // per_unit
    part = small_out.shape[5]
    slots = rows_ref.shape[1]
    spots = acc.shape[0]
    width = table_ref.shape[1]
    blocks = acc.shape[1] // width

    def shard_of(z_at, y_at, core_at):
        return z_at * 4 + y_at * 2 + core_at

    def loop(low, high, act):
        def body(k, c):
            act(k)
            return c

        lax.fori_loop(low, high, body, 0)

    peer = shard_of(z, y, 1 - core)
    away = (1 - core) * half_count
    swap = [
        remote(ids_ref.at[pl.ds(pl.multiple_of(away, 8), half_count)], peer_ids, peer_s.at[0], peer_r.at[0], rep, peer),
        remote(grads_ref.at[pl.ds(away, half_count)], peer_grads, peer_s.at[1], peer_r.at[1], rep, peer),
    ]

    def out_block(k):
        to = lax.rem(me + k, groups)
        return remote(fold_ref.at[to], folds.at[rep * groups + me], fold_s.at[k], fold_r.at[k], rep, to)

    def in_block(k):
        at = lax.rem(me + groups - k, groups)
        return remote(fold_ref.at[at], folds.at[rep * groups + at], fold_s.at[k], fold_r.at[k], rep, at)

    def far_out(k):
        slot = folds.at[rep * groups + lax.rem(me + groups - k, groups)]
        return remote(slot, slot, far_s.at[k], far_r.at[k], other, me)

    def far_in(k):
        slot = folds.at[other * groups + lax.rem(me + groups - k, groups)]
        return remote(slot, slot, far_s.at[k], far_r.at[k], other, me)

    own_far = remote(fold_ref.at[me], folds.at[rep * groups + me], far_s.at[0], far_r.at[0], other, me)

    greet_all()
    for copy in swap:
        copy.start()
    loop(1, groups, lambda k: out_block(k).start())
    own_far.start()
    fetch = [
        pltpu.make_async_copy(tables_ref.at[core, h, rep, y, z], prior.at[h], local.at[h])
        for h in range(2)
    ]
    for copy in fetch:
        copy.start()
    folds[rep * groups + me] = fold_ref[me]
    acc[...] = jnp.zeros_like(acc)
    for copy in swap:
        copy.wait_recv()

    row = iota((small_rows, batch), 0)

    def dense(t):
        own = (row == ids_ref[pl.ds(core * half_count + t, 1), :]).astype(f32).astype(bf16)
        far = (row == peer_ids[pl.ds(t, 1), :]).astype(f32).astype(bf16)
        return jnp.dot(
            own, grads_ref[core * half_count + t], preferred_element_type=f32
        ) + jnp.dot(far, peer_grads[t], preferred_element_type=f32)

    def first_hop(h, s):
        to_rep = rep + (1 - h) * (1 - 2 * rep)
        to_y = y + h * (1 - 2 * y)
        return remote(
            sent.at[h, s], came.at[h, s], rs1_s.at[h, s], rs1_r.at[h, s], to_rep, shard_of(z, to_y, core)
        )

    def second_hop(h):
        to_rep = rep + h * (1 - 2 * rep)
        to_y = y + (1 - h) * (1 - 2 * y)
        return remote(
            sent_2.at[h], came_2.at[h], rs2_s.at[h], rs2_r.at[h], to_rep, shard_of(z, to_y, core)
        )

    def third_hop(h, k):
        to = lax.rem(z + k, ring)
        return remote(
            sent_3.at[h, to], came_3.at[h, z], rs3_s.at[h, k], rs3_r.at[h, k], rep, shard_of(to, y, core)
        )

    def third_in(h, k):
        at = lax.rem(z + ring - k, ring)
        return remote(
            sent_3.at[h, at], came_3.at[h, at], rs3_s.at[h, k], rs3_r.at[h, k], rep, shard_of(at, y, core)
        )

    def give(i):
        s, h = i // 2, lax.rem(i, 2)
        r_at = other + h * s * (2 * rep - 1)
        y_at = (1 - y) + (1 - h) * s * (2 * y - 1)
        first = ((h * 2 + r_at) * 2 + y_at) * per_unit
        for j in range(per_unit):
            sent[h, s, j * small_rows : (j + 1) * small_rows, :] = dense(first + j).astype(bf16)
        first_hop(h, s).start()

    def hold(i):
        s, h = i // 2, lax.rem(i, 2)
        r_at = rep + h * (1 - s) * (1 - 2 * rep)
        y_at = y + (1 - h) * (1 - s) * (1 - 2 * y)
        first = ((h * 2 + r_at) * 2 + y_at) * per_unit
        for j in range(per_unit):
            keep[h, s, j * small_rows : (j + 1) * small_rows, :] = dense(first + j)

    loop(0, 4, give)
    loop(0, 4, hold)

    spot = iota((spots, slots), 0)

    def place_rows(d, v, lhs, rhs):
        members = members_of(ends_ref[pl.ds(d, 1), :], slots)
        moved = jnp.dot(members, folds[d], preferred_element_type=f32)
        at = rows_ref[pl.ds(d, 1), :]
        block = at // spots
        wide = jnp.transpose(jnp.broadcast_to(block.astype(f32), (width, slots)))
        for q in range(blocks):
            rhs[v * slots : (v + 1) * slots, q * width : (q + 1) * width] = jnp.where(
                wide == q, moved, 0.0
            ).astype(bf16)
        lhs[:, v * slots : (v + 1) * slots] = (spot == at - block * spots).astype(f32).astype(bf16)

    turns = groups // 2
    cut_1, cut_2, cut_3 = turns // 4, turns // 2, turns * 7 // 8

    def take(k):
        in_block(k).wait_recv()

        @pl.when(k > 4 * cut_1 + 1)
        def _():
            far_out(k).start()

    def get(p):
        @pl.when((p > 0) & (p < groups // 2))
        def _():
            take(2 * p)

        @pl.when(p < groups // 2)
        def _():
            take(2 * p + 1)

        @pl.when((p >= groups // 2) & (p < groups))
        def _():
            far_in(2 * p - groups).wait_recv()
            far_in(2 * p + 1 - groups).wait_recv()

    def owner(k):
        side = k // groups
        at = lax.rem(me + groups - (k - side * groups), groups)
        return (rep + side * (1 - 2 * rep)) * groups + at

    step = 2 * width

    def make(p, lhs, rhs):
        place_rows(owner(2 * p), 0, lhs, rhs)
        place_rows(owner(2 * p + 1), 1, lhs, rhs)

    def multiply(lhs, rhs):
        for n in range(0, acc.shape[1], step):
            acc[:, n : n + step] += jnp.dot(lhs[...], rhs[:, n : n + step], preferred_element_type=f32)

    def pairs(i):
        get(2 * i + 1)
        make(2 * i + 1, lhs_1, rhs_1)
        multiply(lhs_0, rhs_0)
        get(2 * i + 2)
        make(jnp.minimum(2 * i + 2, groups - 1), lhs_0, rhs_0)
        multiply(lhs_1, rhs_1)

    loop(0, 1, get)
    make(0, lhs_0, rhs_0)
    loop(0, cut_1, pairs)

    def turn(h):
        first_hop(h, 0).wait_recv()
        sent_2[h] = (keep[h, 0] + came[h, 0].astype(f32)).astype(bf16)
        second_hop(h).start()

    loop(0, 2, turn)
    loop(1, 4 * cut_1 + 2, lambda k: far_out(k).start())
    loop(cut_1, cut_2, pairs)

    def along(h):
        first_hop(h, 1).wait_recv()
        second_hop(h).wait_recv()
        total = keep[h, 1] + came[h, 1].astype(f32) + came_2[h].astype(f32)
        keep[h, 1] = total
        sent_3[h] = total.astype(bf16).reshape(ring, part, width)
        loop(1, ring, lambda k: third_hop(h, k).start())

    loop(0, 2, along)
    loop(cut_2, cut_3, pairs)

    for copy in fetch:
        copy.wait()

    def own_part(h):
        total = keep[h, 1, pl.ds(pl.multiple_of(z * part, part), part), :]
        for k in range(1, ring):
            third_in(h, k).wait_recv()
            total = total + came_3[h, lax.rem(z + ring - k, ring)].astype(f32)
        small_out[core, h, rep, y, z] = (prior[h].astype(f32) - step_size * total).astype(bf16)

    loop(0, 2, own_part)

    pending = []

    def place(h, rep_at, z_at, y_at, core_at):
        return small_out.at[core_at, h, rep_at, y_at, z_at]

    def slot_of(rep_at, z_at, y_at, core_at):
        return rep_at * groups + shard_of(z_at, y_at, core_at)

    def send(h, rep_at, z_at, y_at, sem, to_rep, to_z, to_y, to_core):
        block = place(h, rep_at, z_at, y_at, core)
        copy = remote(
            block, block, sem, ag_r.at[h, slot_of(rep_at, z_at, y_at, core)],
            to_rep, shard_of(to_z, to_y, to_core),
        )
        copy.start()
        pending.append(copy)

    def arrived(h, rep_at, z_at, y_at, core_at):
        block = place(h, rep_at, z_at, y_at, core_at)
        remote(
            block, block, local.at[2], ag_r.at[h, slot_of(rep_at, z_at, y_at, core_at)], rep, peer
        ).wait_recv()

    def second(h, k, rep_at, z_at, y_at):
        hop = (rep, z, 1 - y, core) if h == 0 else (other, z, y, core)
        send(h, rep_at, z_at, y_at, ag_1.at[h, k], *hop)

    def third(h, k, rep_at, z_at, y_at):
        hop = (other, z, y, core) if h == 0 else (rep, z, 1 - y, core)
        send(h, rep_at, z_at, y_at, ag_2.at[h, k], *hop)

    def last(h, k, rep_at, z_at, y_at):
        send(h, rep_at, z_at, y_at, ag_core.at[h, k], rep, z, y, 1 - core)

    for k in range(1, ring):
        for h in range(2):
            send(h, rep, z, y, ag_z.at[h, k], rep, lax.rem(z + k, ring), y, core)
    for h in range(2):
        second(h, 0, rep, z, y)
        third(h, 0, rep, z, y)
        last(h, 0, rep, z, y)

    loop(cut_3, turns, pairs)
    for q in range(blocks):
        at = slice(q * spots, (q + 1) * spots)
        large_out[at, :] = (
            table_ref[at, :].astype(f32) - step_size * acc[:, q * width : (q + 1) * width]
        ).astype(bf16)

    for k in range(1, ring):
        z_at = lax.rem(z + ring - k, ring)
        for h in range(2):
            arrived(h, rep, z_at, y, core)
            second(h, k, rep, z_at, y)
            third(h, k, rep, z_at, y)
            last(h, k, rep, z_at, y)
    for k in range(ring):
        z_at = lax.rem(z + ring - k, ring)
        for h in range(2):
            where = (rep, z_at, 1 - y) if h == 0 else (other, z_at, y)
            arrived(h, *where, core)
            third(h, ring + k, *where)
            last(h, ring + k, *where)
    for k in range(2 * ring):
        z_at = lax.rem(z + ring - k % ring, ring)
        for h in range(2):
            if h == 0:
                where = (other, z_at, y if k < ring else 1 - y)
            else:
                where = (rep if k < ring else other, z_at, 1 - y)
            arrived(h, *where, core)
            last(h, 2 * ring + k, *where)
    for r in range(2):
        for k in range(ring):
            for y_at in range(2):
                for h in range(2):
                    arrived(h, r, k, y_at, 1 - core)

    for copy in pending + swap:
        copy.wait_send()
    own_far.wait_send()
    loop(1, groups, lambda k: out_block(k).wait_send())
    loop(1, groups, lambda k: far_out(k).wait_send())
    loop(0, 4, lambda i: first_hop(lax.rem(i, 2), i // 2).wait_send())
    loop(0, 2, lambda h: second_hop(h).wait_send())
    for h in range(2):
        loop(1, ring, lambda k: third_hop(h, k).wait_send())


def tail(ids, grads, fold, rows, ends, table, tables):
    groups = fold.shape[0]
    devices, slots = rows.shape
    ring = groups // 4
    small_count, small_rows, width = tables.shape
    part = small_count * small_rows // devices // 2
    unit = small_count * small_rows // 16
    blocks = 8
    split = (2, 2, 2, 2, ring, part, width)
    scratch = [
        pltpu.VMEM((small_count // 2, ids.shape[1]), ids.dtype),
        pltpu.VMEM((small_count // 2,) + grads.shape[1:], bf16),
        pltpu.VMEM((devices,) + fold.shape[1:], bf16),
        pltpu.VMEM((table.shape[0] // blocks, blocks * width), f32),
        pltpu.VMEM((table.shape[0] // blocks, 2 * slots), bf16),
        pltpu.VMEM((table.shape[0] // blocks, 2 * slots), bf16),
        pltpu.VMEM((2 * slots, blocks * width), bf16),
        pltpu.VMEM((2 * slots, blocks * width), bf16),
        pltpu.VMEM((2, 2, unit, width), f32),
        pltpu.VMEM((2, 2, unit, width), bf16),
        pltpu.VMEM((2, 2, unit, width), bf16),
        pltpu.VMEM((2, unit, width), bf16),
        pltpu.VMEM((2, unit, width), bf16),
        pltpu.VMEM((2, ring, part, width), bf16),
        pltpu.VMEM((2, ring, part, width), bf16),
        pltpu.VMEM((2, part, width), bf16),
    ]
    dma = pltpu.SemaphoreType.DMA
    small, large = pl.pallas_call(
        tail_kernel,
        out_shape=(
            jax.ShapeDtypeStruct(split, bf16),
            jax.ShapeDtypeStruct(table.shape, bf16),
        ),
        in_specs=[whole(pltpu.VMEM)] * 6 + [whole(pl.ANY)],
        out_specs=(whole(pltpu.VMEM),) * 2,
        scratch_shapes=scratch + [
            dma((3,)), dma((2,)), dma((2,)),
            dma((groups,)), dma((groups,)), dma((groups,)), dma((groups,)),
            dma((2, 2)), dma((2, 2)), dma((2,)), dma((2,)), dma((2, ring)), dma((2, ring)),
            dma((2, ring)), dma((2, ring)), dma((2, 2 * ring)), dma((2, 4 * ring)), dma((2, devices)),
        ],
        compiler_params=pltpu.CompilerParams(
            collective_id=1, has_side_effects=True,
            vmem_limit_bytes=grant(ids, grads, fold, rows, ends, table, table, tables, *scratch),
        ),
        name="tail",
    )(ids, grads, fold, rows, ends, table, tables.reshape(split))
    return small.reshape(tables.shape), large


def store_kernel(small_ref, large_ref, small_out, large_out, sems):
    pieces = 4
    copies = []
    for n, (src, dst) in enumerate(((small_ref, small_out), (large_ref, large_out))):
        size = src.shape[0] // pieces
        for p in range(pieces):
            at = pl.ds(p * size, size)
            copies.append(pltpu.make_async_copy(src.at[at], dst.at[at], sems.at[n, p]))
    for copy in copies:
        copy.start()
    for copy in copies:
        copy.wait()


def store(small, large):
    return pl.pallas_call(
        store_kernel,
        out_shape=(
            jax.ShapeDtypeStruct(small.shape, small.dtype),
            jax.ShapeDtypeStruct(large.shape, large.dtype),
        ),
        in_specs=[whole(pltpu.VMEM)] * 2,
        out_specs=(whole(pl.ANY),) * 2,
        scratch_shapes=[pltpu.SemaphoreType.DMA((2, 4))],
        compiler_params=pltpu.CompilerParams(vmem_limit_bytes=16 * 1024 * 1024),
        name="store",
    )(small, large)


def shards(
    dense, small_ids, labels, small_tables, large_tables, batch_sizes, bag_ends,
    owner_row_index, w_first, b_first, w_out,
):
    groups = lax.axis_size("shard")
    index = lax.axis_index("rep") * groups + lax.axis_index("shard")
    ends, rows, table = bag_ends[0], owner_row_index[0], large_tables[0]
    ids = jnp.transpose(small_ids)

    large, small = head(groups, rows, ends, ids, table, small_tables, w_first)
    small_grads, fold = top(
        index[None], batch_sizes, dense, labels, small, large, w_first, b_first, w_out
    )
    small_new, large_new = tail(ids, small_grads, fold, rows, ends, table, small_tables)
    small_new, large_new = store(small_new, large_new)
    return small_new, large_new[None]


def solution(mesh):
    both = ("rep", "shard")
    placed = (
        P(both, None), P(both, None), P(both), P(), P("shard", None, None), P(),
        P("shard", None, None), P("shard", None, None), P(), P(), P(),
    )
    return jax.shard_map(
        shards, mesh=mesh, in_specs=placed, out_specs=(P(), P("shard", None, None)), check_vma=False
    )
```

```python
import functools
import math

import jax
import jax.numpy as jnp
from jax import lax
from jax.experimental import pallas as pl
from jax.experimental.pallas import tpu as pltpu
from jax.sharding import PartitionSpec as P

step_size = 32.0
LANES = 128
VMEM_LIMIT = 60 * 1024 * 1024
MIB = 1024 * 1024
f32 = jnp.float32
bf16 = jnp.bfloat16


def whole(space):
    return pl.BlockSpec(memory_space=space)


def size_of(*arrays):
    return sum(math.prod(a.shape) * jnp.dtype(a.dtype).itemsize for a in arrays)


def grant(*arrays):
    return min(VMEM_LIMIT, size_of(*arrays) + 6 * MIB)


def all_but(*arrays):
    return min(VMEM_LIMIT, 63 * MIB - size_of(*arrays))


def iota(shape, axis):
    return lax.broadcasted_iota(jnp.int32, shape, axis)


def members_of(ends, slots):
    span = ends.shape[-1]
    starts = jnp.where(iota((1, span), 1) == 0, 0, pltpu.roll(ends, 1, 1))
    places = iota((slots, span), 0)
    return ((places >= starts) & (places < ends)).astype(f32).astype(bf16)


def spans_of(vec_count):
    return [(i, i * (i - 1) // 2) for i in range(1, vec_count)]


def top_kernel(
    vec_count, group, pad, hook, index_ref, sizes_ref, dense_ref, labels_ref, small_ref, large_ref,
    w_ref, bias_ref, wout_ref, small_out, fold_out, vecs, gram, pairs, spread,
):
    batch, width = dense_ref.shape
    small_count = small_ref.shape[0]
    feats, bag_span = large_ref.shape[0], large_ref.shape[1]
    pair_pad = pairs.shape[1]
    pair_count = vec_count * (vec_count - 1) // 2
    scale = width ** (-0.5)
    index = index_ref[0] if hook is None else position()
    spans = spans_of(vec_count)

    def rows_of(i):
        return pl.ds(i, batch, stride=pad)

    vecs[rows_of(0), :] = dense_ref[...].astype(f32)
    for t in range(small_count):
        vecs[rows_of(1 + t), :] = small_ref[t].astype(f32)
    sample = iota((batch, bag_span), 0)
    bag = iota((batch, bag_span), 1) * batch
    for f in range(feats):
        reach = sample * sizes_ref[f, index]
        hot = ((reach >= bag) & (reach < bag + batch)).astype(f32).astype(bf16)
        vecs[rows_of(1 + small_count + f), :] = jnp.dot(
            hot, large_ref[f], preferred_element_type=f32
        )
    for i in range(vec_count, pad):
        vecs[rows_of(i), :] = jnp.zeros((batch, width), f32)

    unroll = 8

    many = batch // group
    tall = group * pad

    def gram_step(g, c):
        for u in range(unroll):
            at = pl.ds(pl.multiple_of((g * unroll + u) * tall, 8), tall)
            own = vecs[at, :].astype(bf16)
            gram[at, 0:tall] = lax.dot_general(
                own, own, (((1,), (1,)), ((), ())), preferred_element_type=f32
            )
        return c

    lax.fori_loop(0, many // unroll, gram_step, 0)

    lane = iota((1, LANES), 1)
    chunk = 64
    places = [(v, start) for v in range(group) for start in range(0, many, chunk)]

    def strided(v, start, i, size):
        return pl.ds((start * group + v) * pad + i, size, stride=tall)

    for v, start in places:
        tile = jnp.zeros((chunk, LANES), f32)
        at_tile = 0
        row = v * many + start
        for i, off in spans:
            piece = gram[strided(v, start, i, chunk), :]
            turn = (off - v * pad) % LANES
            if turn:
                piece = pltpu.roll(piece, turn, 1)
            low = off - at_tile * LANES
            tile = jnp.where((lane >= low) & (lane < low + i), piece, tile)
            if low + i >= LANES:
                pairs[row : row + chunk, at_tile * LANES : (at_tile + 1) * LANES] = (
                    tile * scale
                ).astype(bf16)
                at_tile += 1
                rest = low + i - LANES
                tile = jnp.where(lane < rest, piece, jnp.zeros_like(piece))
        if at_tile * LANES < pair_pad:
            pairs[row : row + chunk, at_tile * LANES : pair_pad] = (tile * scale).astype(bf16)

    block = min(128, many)
    gram[0:batch, :] = jnp.transpose(
        jnp.broadcast_to(labels_ref[...].astype(f32), (LANES, batch))
    )
    labels_of = [gram[pl.ds(v, many, stride=group), :][:, 0:1] for v in range(group)]
    for v, start in [(v, start) for v in range(group) for start in range(0, many, block)]:
        at = slice(v * many + start, v * many + start + block)
        own_dense = vecs[strided(v, start, 0, block), :].astype(bf16)
        preact = (
            jnp.dot(pairs[at, :], w_ref[0:pair_pad, :], preferred_element_type=f32)
            + jnp.dot(own_dense, w_ref[pair_count : pair_count + width, :], preferred_element_type=f32)
            + bias_ref[...]
        )
        squash = jax.nn.sigmoid(preact)
        logits = jnp.sum(preact * squash * wout_ref[...], axis=1, keepdims=True)
        grad = jax.nn.sigmoid(logits) - labels_of[v][start : start + block, :]
        pre_grad = (
            grad * wout_ref[...] * (squash * (1.0 + preact * (1.0 - squash)))
        ).astype(bf16)
        for q in range(0, pair_pad, LANES):
            spread[at, q : q + LANES] = lax.dot_general(
                pre_grad, w_ref[q : q + LANES, :], (((1,), (1,)), ((), ())),
                preferred_element_type=f32,
            ) * scale

    gram[rows_of(0), :] = jnp.zeros((batch, LANES), f32)
    for i in range(vec_count, pad):
        gram[rows_of(i), :] = jnp.zeros((batch, LANES), f32)
    for v, start in places:
        row = v * many + start
        for i, off in spans:
            first = off // LANES
            low = off - first * LANES
            here = spread[row : row + chunk, first * LANES : (first + 1) * LANES]
            if low + i > LANES:
                after = spread[row : row + chunk, (first + 1) * LANES : (first + 2) * LANES]
                here = jnp.where(lane >= low, here, after)
            turn = (v * pad - low) % LANES
            if turn:
                here = pltpu.roll(here, turn, 1)
            gram[strided(v, start, i, chunk), :] = jnp.where(
                (lane >= v * pad) & (lane < v * pad + i), here, 0.0
            )

    def back_step(g, c):
        for u in range(unroll):
            at = pl.ds(pl.multiple_of((g * unroll + u) * tall, 8), tall)
            lower = gram[at, :]
            both = lower[:, 0:tall] + jnp.transpose(lower)[0:tall, :]
            vecs[at, :] = jnp.dot(
                both.astype(bf16), vecs[at, :].astype(bf16), preferred_element_type=f32
            )
        return c

    lax.fori_loop(0, many // unroll, back_step, 0)

    for t in range(small_count):
        small_out[t] = vecs[rows_of(1 + t), :].astype(bf16)
    sample_lane = iota((bag_span, batch), 1)
    bag_row = iota((bag_span, batch), 0) * batch
    for f in range(feats):
        if hook is not None and f == feats // 4:
            hook()
        reach = sample_lane * sizes_ref[f, index]
        hot = ((reach >= bag_row) & (reach < bag_row + batch)).astype(f32).astype(bf16)
        fold_out[f] = jnp.dot(
            hot, vecs[rows_of(1 + small_count + f), :].astype(bf16), preferred_element_type=f32
        ).astype(bf16)


def top_plan(dense, small, large):
    batch, width = dense.shape
    small_count, feats, bag_span = small.shape[0], large.shape[0], large.shape[1]
    vec_count = 1 + small_count + feats
    group = max(1, LANES // (-(-vec_count // 8) * 8))
    tiles = -(-group * vec_count // 8)
    if tiles % 2 == 0 and (tiles + 1) * 8 <= LANES:
        tiles += 1
    pad = tiles * 8 // group
    pair_count = vec_count * (vec_count - 1) // 2
    pair_pad = -(-pair_count // LANES) * LANES
    scratch = [
        pltpu.VMEM((batch * pad, width), f32),
        pltpu.VMEM((batch * pad, LANES), f32),
        pltpu.VMEM((batch, pair_pad), bf16),
        pltpu.VMEM((batch, pair_pad), f32),
    ]
    return vec_count, group, pad, scratch


def position():
    return lax.axis_index("rep") * lax.axis_size("shard") + lax.axis_index("shard")


def top(index, sizes, dense, labels, small, large, w_first, bias, wout):
    batch, width = dense.shape
    small_count, feats, bag_span = small.shape[0], large.shape[0], large.shape[1]
    vec_count, group, pad, scratch = top_plan(dense, small, large)
    return pl.pallas_call(
        functools.partial(top_kernel, vec_count, group, pad, None),
        out_shape=(
            jax.ShapeDtypeStruct((small_count, batch, width), bf16),
            jax.ShapeDtypeStruct((feats, bag_span, width), bf16),
        ),
        in_specs=[whole(pltpu.SMEM)] * 2 + [whole(pltpu.VMEM)] * 7,
        out_specs=(whole(pltpu.VMEM), whole(pltpu.VMEM)),
        scratch_shapes=scratch,
        compiler_params=pltpu.CompilerParams(
            vmem_limit_bytes=grant(dense, small, large, small, large, w_first, *scratch)
        ),
        name="top",
    )(
        index, sizes, dense, labels[None, :], small, large, w_first,
        bias[None, :], wout[None, :],
    )


def greet_all():
    copies, groups = lax.axis_size("rep"), lax.axis_size("shard")
    devices = copies * groups
    index = lax.axis_index("rep") * groups + lax.axis_index("shard")
    barrier = pltpu.get_barrier_semaphore()

    def greet(k, c):
        other = lax.rem(index + k, devices)
        pl.semaphore_signal(
            barrier, inc=1, device_id={"rep": other // groups, "shard": lax.rem(other, groups)},
            device_id_type=pl.DeviceIdType.MESH,
        )
        return c

    lax.fori_loop(1, devices, greet, 0)
    pl.semaphore_wait(barrier, devices - 1)


def remote(src, dst, send, recv, rep, shard):
    return pltpu.make_async_remote_copy(
        src_ref=src, dst_ref=dst, send_sem=send, recv_sem=recv,
        device_id={"rep": rep, "shard": shard}, device_id_type=pl.DeviceIdType.MESH,
    )


def head_kernel(
    rows_hbm, ends_hbm, ids_hbm, table_hbm, tables_hbm, large_out, small_out,
    rows, ends, ids, narrow, wide, tables, by_sample, outbox, send, recv, local,
):
    groups = lax.axis_size("shard")
    rep, me = lax.axis_index("rep"), lax.axis_index("shard")
    slots = rows.shape[1]
    arrays = ((rows_hbm, rows), (ends_hbm, ends), (ids_hbm, ids), (table_hbm, narrow), (tables_hbm, tables))
    fetch = [pltpu.make_async_copy(src, dst, local.at[n]) for n, (src, dst) in enumerate(arrays)]
    for copy in fetch:
        copy.start()
    greet_all()
    for copy in fetch[:4]:
        copy.wait()
    wide[...] = narrow[...].astype(f32)

    def block(off):
        to = lax.rem(me + off, groups)
        return remote(outbox.at[to], large_out.at[me], send.at[off], recv.at[off], rep, to)

    def block_in(off):
        at = lax.rem(me + groups - off, groups)
        return remote(outbox.at[at], large_out.at[at], send.at[off], recv.at[off], rep, at)

    def loop(low, high, act):
        def body(k, c):
            act(k)
            return c

        lax.fori_loop(low, high, body, 0)

    def give(i):
        off = lax.rem(groups // 2 + i, groups)
        to = lax.rem(me + off, groups)
        d = rep * groups + to
        picked = [
            jnp.concatenate([wide[pl.ds(rows[d, s + u], 1), :] for u in range(8)], axis=0)
            for s in range(0, slots, 8)
        ]
        pooled = lax.dot_general(
            members_of(ends[pl.ds(d, 1), :], slots), jnp.concatenate(picked, axis=0).astype(bf16),
            (((0,), (0,)), ((), ())), preferred_element_type=f32,
        )
        outbox[to] = pooled.astype(bf16)

        @pl.when(off != 0)
        def _():
            block(off).start()

    loop(0, groups, give)
    by_sample[...] = jnp.transpose(ids[...])
    large_out[me] = outbox[me]
    fetch[4].wait()
    at_row = iota((by_sample.shape[0], tables.shape[1]), 1)
    for t in range(tables.shape[0]):
        hot = (by_sample[:, t : t + 1] == at_row).astype(f32).astype(bf16)
        small_out[t] = jnp.dot(hot, tables[t], preferred_element_type=f32).astype(bf16)
    loop(1, groups, lambda off: block_in(off).wait_recv())
    loop(1, groups, lambda off: block(off).wait_send())


def head(groups, rows, ends, ids, table, tables, w_first):
    large = jax.ShapeDtypeStruct((groups, ends.shape[1], table.shape[1]), bf16)
    small = jax.ShapeDtypeStruct((tables.shape[0], ids.shape[1], tables.shape[2]), tables.dtype)
    scratch = [
        pltpu.VMEM(ends.shape, ends.dtype),
        pltpu.VMEM(ids.shape, ids.dtype),
        pltpu.VMEM(table.shape, table.dtype),
        pltpu.VMEM(table.shape, f32),
        pltpu.VMEM(tables.shape, tables.dtype),
        pltpu.VMEM((ids.shape[1], ids.shape[0]), ids.dtype),
        pltpu.VMEM(large.shape, bf16),
    ]
    dma = pltpu.SemaphoreType.DMA
    return pl.pallas_call(
        head_kernel,
        out_shape=(large, small),
        in_specs=[whole(pltpu.HBM)] * 5,
        out_specs=(whole(pltpu.VMEM),) * 2,
        scratch_shapes=[pltpu.SMEM(rows.shape, rows.dtype)] + scratch
        + [dma((groups,)), dma((groups,)), dma((5,))],
        compiler_params=pltpu.CompilerParams(
            collective_id=0, has_side_effects=True,
            vmem_limit_bytes=max(grant(large, small, *scratch), all_but(large, small, w_first)),
        ),
        name="head",
    )(rows, ends, ids, table, tables)


def swap_copies(ids_ref, grads_ref, peer_ids, peer_grads, sends, recvs):
    rep, me = lax.axis_index("rep"), lax.axis_index("shard")
    core = lax.rem(me, 2)
    peer = me + 1 - 2 * core
    count = ids_ref.shape[0] // 2
    away = (1 - core) * count
    return [
        remote(
            ids_ref.at[pl.ds(pl.multiple_of(away, 8), count)], peer_ids, sends.at[0], recvs.at[0], rep, peer
        ),
        remote(grads_ref.at[pl.ds(away, count)], peer_grads, sends.at[1], recvs.at[1], rep, peer),
    ]


def tail_kernel(
    outs, ids_ref, grads_ref, fold_ref, rows_ref, ends_ref, table_ref, tables_ref, small_out, large_out,
    peer_ids, peer_grads, folds, acc, lhs_0, lhs_1, rhs_0, rhs_1, keep, sent, came, sent_2, came_2, sent_3, came_3,
    prior, local, peer_s, peer_r, fold_s, fold_r, far_s, far_r, rs1_s, rs1_r, rs2_s, rs2_r,
    rs3_s, rs3_r, ag_z, ag_1, ag_2, ag_core, ag_r,
):
    groups = lax.axis_size("shard")
    ring = groups // 4
    rep, me = lax.axis_index("rep"), lax.axis_index("shard")
    z, y, core = me // 4, lax.rem(me, 4) // 2, lax.rem(me, 2)
    other = 1 - rep
    small_count, batch = ids_ref.shape
    half_count = small_count // 2
    per_unit = small_count // 16
    small_rows = keep.shape[2] // per_unit
    part = small_out.shape[5]
    slots = rows_ref.shape[1]
    spots = acc.shape[0]
    width = table_ref.shape[1]
    blocks = acc.shape[1] // width

    def shard_of(z_at, y_at, core_at):
        return z_at * 4 + y_at * 2 + core_at

    def loop(low, high, act):
        def body(k, c):
            act(k)
            return c

        lax.fori_loop(low, high, body, 0)

    peer = shard_of(z, y, 1 - core)
    swap = swap_copies(ids_ref, grads_ref, peer_ids, peer_grads, peer_s, peer_r)

    def out_block(k):
        to = lax.rem(me + k, groups)
        return remote(fold_ref.at[to], folds.at[rep * groups + me], fold_s.at[k], fold_r.at[k], rep, to)

    def in_block(k):
        at = lax.rem(me + groups - k, groups)
        return remote(fold_ref.at[at], folds.at[rep * groups + at], fold_s.at[k], fold_r.at[k], rep, at)

    def far_out(k):
        slot = folds.at[rep * groups + lax.rem(me + groups - k, groups)]
        return remote(slot, slot, far_s.at[k], far_r.at[k], other, me)

    def far_in(k):
        slot = folds.at[other * groups + lax.rem(me + groups - k, groups)]
        return remote(slot, slot, far_s.at[k], far_r.at[k], other, me)

    own_far = remote(fold_ref.at[me], folds.at[rep * groups + me], far_s.at[0], far_r.at[0], other, me)

    if outs is None:
        greet_all()
        for copy in swap:
            copy.start()
    loop(1, groups, lambda k: out_block(k).start())
    own_far.start()
    fetch = [
        pltpu.make_async_copy(tables_ref.at[core, h, rep, y, z], prior.at[h], local.at[h])
        for h in range(2)
    ]
    for copy in fetch:
        copy.start()
    folds[rep * groups + me] = fold_ref[me]
    acc[...] = jnp.zeros_like(acc)
    for copy in swap:
        copy.wait_recv()

    row = iota((small_rows, batch), 0)

    def dense(t):
        own = (row == ids_ref[pl.ds(core * half_count + t, 1), :]).astype(f32).astype(bf16)
        far = (row == peer_ids[pl.ds(t, 1), :]).astype(f32).astype(bf16)
        return jnp.dot(
            own, grads_ref[core * half_count + t], preferred_element_type=f32
        ) + jnp.dot(far, peer_grads[t], preferred_element_type=f32)

    def first_hop(h, s):
        to_rep = rep + (1 - h) * (1 - 2 * rep)
        to_y = y + h * (1 - 2 * y)
        return remote(
            sent.at[h, s], came.at[h, s], rs1_s.at[h, s], rs1_r.at[h, s], to_rep, shard_of(z, to_y, core)
        )

    def second_hop(h):
        to_rep = rep + h * (1 - 2 * rep)
        to_y = y + (1 - h) * (1 - 2 * y)
        return remote(
            sent_2.at[h], came_2.at[h], rs2_s.at[h], rs2_r.at[h], to_rep, shard_of(z, to_y, core)
        )

    def third_hop(h, k):
        to = lax.rem(z + k, ring)
        return remote(
            sent_3.at[h, to], came_3.at[h, z], rs3_s.at[h, k], rs3_r.at[h, k], rep, shard_of(to, y, core)
        )

    def third_in(h, k):
        at = lax.rem(z + ring - k, ring)
        return remote(
            sent_3.at[h, at], came_3.at[h, at], rs3_s.at[h, k], rs3_r.at[h, k], rep, shard_of(at, y, core)
        )

    def give(i):
        s, h = i // 2, lax.rem(i, 2)
        r_at = other + h * s * (2 * rep - 1)
        y_at = (1 - y) + (1 - h) * s * (2 * y - 1)
        first = ((h * 2 + r_at) * 2 + y_at) * per_unit
        for j in range(per_unit):
            sent[h, s, j * small_rows : (j + 1) * small_rows, :] = dense(first + j).astype(bf16)
        first_hop(h, s).start()

    def hold(i):
        s, h = i // 2, lax.rem(i, 2)
        r_at = rep + h * (1 - s) * (1 - 2 * rep)
        y_at = y + (1 - h) * (1 - s) * (1 - 2 * y)
        first = ((h * 2 + r_at) * 2 + y_at) * per_unit
        for j in range(per_unit):
            keep[h, s, j * small_rows : (j + 1) * small_rows, :] = dense(first + j)

    loop(0, 4, give)
    loop(0, 4, hold)

    spot = iota((spots, slots), 0)

    def place_rows(d, v, lhs, rhs):
        members = members_of(ends_ref[pl.ds(d, 1), :], slots)
        moved = jnp.dot(members, folds[d], preferred_element_type=f32)
        at = rows_ref[pl.ds(d, 1), :]
        block = at // spots
        wide = jnp.transpose(jnp.broadcast_to(block.astype(f32), (width, slots)))
        for q in range(blocks):
            rhs[v * slots : (v + 1) * slots, q * width : (q + 1) * width] = jnp.where(
                wide == q, moved, 0.0
            ).astype(bf16)
        lhs[:, v * slots : (v + 1) * slots] = (spot == at - block * spots).astype(f32).astype(bf16)

    turns = groups // 2
    cut_1, cut_2, cut_3 = turns // 4, turns // 2, turns * 7 // 8

    def take(k):
        in_block(k).wait_recv()

        @pl.when(k > 4 * cut_1 + 1)
        def _():
            far_out(k).start()

    def get(p):
        @pl.when((p > 0) & (p < groups // 2))
        def _():
            take(2 * p)

        @pl.when(p < groups // 2)
        def _():
            take(2 * p + 1)

        @pl.when((p >= groups // 2) & (p < groups))
        def _():
            far_in(2 * p - groups).wait_recv()
            far_in(2 * p + 1 - groups).wait_recv()

    def owner(k):
        side = k // groups
        at = lax.rem(me + groups - (k - side * groups), groups)
        return (rep + side * (1 - 2 * rep)) * groups + at

    step = 2 * width

    def make(p, lhs, rhs):
        place_rows(owner(2 * p), 0, lhs, rhs)
        place_rows(owner(2 * p + 1), 1, lhs, rhs)

    def multiply(lhs, rhs):
        for n in range(0, acc.shape[1], step):
            acc[:, n : n + step] += jnp.dot(lhs[...], rhs[:, n : n + step], preferred_element_type=f32)

    def pairs(i):
        get(2 * i + 1)
        make(2 * i + 1, lhs_1, rhs_1)
        multiply(lhs_0, rhs_0)
        get(2 * i + 2)
        make(jnp.minimum(2 * i + 2, groups - 1), lhs_0, rhs_0)
        multiply(lhs_1, rhs_1)

    loop(0, 1, get)
    make(0, lhs_0, rhs_0)
    loop(0, cut_1, pairs)

    def turn(h):
        first_hop(h, 0).wait_recv()
        sent_2[h] = (keep[h, 0] + came[h, 0].astype(f32)).astype(bf16)
        second_hop(h).start()

    loop(0, 2, turn)
    loop(1, 4 * cut_1 + 2, lambda k: far_out(k).start())
    loop(cut_1, cut_2, pairs)

    def along(h):
        first_hop(h, 1).wait_recv()
        second_hop(h).wait_recv()
        total = keep[h, 1] + came[h, 1].astype(f32) + came_2[h].astype(f32)
        keep[h, 1] = total
        sent_3[h] = total.astype(bf16).reshape(ring, part, width)
        loop(1, ring, lambda k: third_hop(h, k).start())

    loop(0, 2, along)
    loop(cut_2, cut_3, pairs)

    for copy in fetch:
        copy.wait()

    def own_part(h):
        total = keep[h, 1, pl.ds(pl.multiple_of(z * part, part), part), :]
        for k in range(1, ring):
            third_in(h, k).wait_recv()
            total = total + came_3[h, lax.rem(z + ring - k, ring)].astype(f32)
        small_out[core, h, rep, y, z] = (prior[h].astype(f32) - step_size * total).astype(bf16)

    loop(0, 2, own_part)

    pending = []

    def place(h, rep_at, z_at, y_at, core_at):
        return small_out.at[core_at, h, rep_at, y_at, z_at]

    def slot_of(rep_at, z_at, y_at, core_at):
        return rep_at * groups + shard_of(z_at, y_at, core_at)

    def send(h, rep_at, z_at, y_at, sem, to_rep, to_z, to_y, to_core):
        block = place(h, rep_at, z_at, y_at, core)
        copy = remote(
            block, block, sem, ag_r.at[h, slot_of(rep_at, z_at, y_at, core)],
            to_rep, shard_of(to_z, to_y, to_core),
        )
        copy.start()
        pending.append(copy)

    def arrived(h, rep_at, z_at, y_at, core_at):
        block = place(h, rep_at, z_at, y_at, core_at)
        remote(
            block, block, local.at[2], ag_r.at[h, slot_of(rep_at, z_at, y_at, core_at)], rep, peer
        ).wait_recv()

    def second(h, k, rep_at, z_at, y_at):
        hop = (rep, z, 1 - y, core) if h == 0 else (other, z, y, core)
        send(h, rep_at, z_at, y_at, ag_1.at[h, k], *hop)

    def third(h, k, rep_at, z_at, y_at):
        hop = (other, z, y, core) if h == 0 else (rep, z, 1 - y, core)
        send(h, rep_at, z_at, y_at, ag_2.at[h, k], *hop)

    def last(h, k, rep_at, z_at, y_at):
        send(h, rep_at, z_at, y_at, ag_core.at[h, k], rep, z, y, 1 - core)

    for k in range(1, ring):
        for h in range(2):
            send(h, rep, z, y, ag_z.at[h, k], rep, lax.rem(z + k, ring), y, core)
    for h in range(2):
        second(h, 0, rep, z, y)
        third(h, 0, rep, z, y)
        last(h, 0, rep, z, y)

    loop(cut_3, turns, pairs)
    for q in range(blocks):
        at = slice(q * spots, (q + 1) * spots)
        large_out[at, :] = (
            table_ref[at, :].astype(f32) - step_size * acc[:, q * width : (q + 1) * width]
        ).astype(bf16)

    for k in range(1, ring):
        z_at = lax.rem(z + ring - k, ring)
        for h in range(2):
            arrived(h, rep, z_at, y, core)
            second(h, k, rep, z_at, y)
            third(h, k, rep, z_at, y)
            last(h, k, rep, z_at, y)
    put = []

    def leave(src, dst):
        if outs is not None:
            copy = pltpu.make_async_copy(src, dst, outs[2].at[len(put)])
            copy.start()
            put.append(copy)

    small_hbm, large_hbm = (None, None) if outs is None else outs[:2]
    if outs is not None:
        leave(large_out, large_hbm)
    for k in range(ring):
        z_at = lax.rem(z + ring - k, ring)
        for h in range(2):
            where = (rep, z_at, 1 - y) if h == 0 else (other, z_at, y)
            arrived(h, *where, core)
            third(h, ring + k, *where)
            last(h, ring + k, *where)
    for k in range(2 * ring):
        z_at = lax.rem(z + ring - k % ring, ring)
        for h in range(2):
            if h == 0:
                where = (other, z_at, y if k < ring else 1 - y)
            else:
                where = (rep if k < ring else other, z_at, 1 - y)
            arrived(h, *where, core)
            last(h, 2 * ring + k, *where)
    if outs is not None:
        leave(small_out.at[core], small_hbm.at[core])
    for r in range(2):
        for k in range(ring):
            for y_at in range(2):
                for h in range(2):
                    arrived(h, r, k, y_at, 1 - core)
        if outs is not None:
            for h in range(2):
                leave(small_out.at[1 - core, h, r], small_hbm.at[1 - core, h, r])

    for copy in pending + swap:
        copy.wait_send()
    for copy in put:
        copy.wait()
    own_far.wait_send()
    loop(1, groups, lambda k: out_block(k).wait_send())
    loop(1, groups, lambda k: far_out(k).wait_send())
    loop(0, 4, lambda i: first_hop(lax.rem(i, 2), i // 2).wait_send())
    loop(0, 2, lambda h: second_hop(h).wait_send())
    for h in range(2):
        loop(1, ring, lambda k: third_hop(h, k).wait_send())


def tail_plan(ids, grads, fold, rows, table, tables):
    groups = fold.shape[0]
    devices, slots = rows.shape
    ring = groups // 4
    small_count, small_rows, width = tables.shape
    part = small_count * small_rows // devices // 2
    unit = small_count * small_rows // 16
    blocks = 8
    split = (2, 2, 2, 2, ring, part, width)
    scratch = [
        pltpu.VMEM((small_count // 2, ids.shape[1]), ids.dtype),
        pltpu.VMEM((small_count // 2,) + grads.shape[1:], bf16),
        pltpu.VMEM((devices,) + fold.shape[1:], bf16),
        pltpu.VMEM((table.shape[0] // blocks, blocks * width), f32),
        pltpu.VMEM((table.shape[0] // blocks, 2 * slots), bf16),
        pltpu.VMEM((table.shape[0] // blocks, 2 * slots), bf16),
        pltpu.VMEM((2 * slots, blocks * width), bf16),
        pltpu.VMEM((2 * slots, blocks * width), bf16),
        pltpu.VMEM((2, 2, unit, width), f32),
        pltpu.VMEM((2, 2, unit, width), bf16),
        pltpu.VMEM((2, 2, unit, width), bf16),
        pltpu.VMEM((2, unit, width), bf16),
        pltpu.VMEM((2, unit, width), bf16),
        pltpu.VMEM((2, ring, part, width), bf16),
        pltpu.VMEM((2, ring, part, width), bf16),
        pltpu.VMEM((2, part, width), bf16),
    ]
    dma = pltpu.SemaphoreType.DMA
    sems = [
        dma((3,)), dma((2,)), dma((2,)),
        dma((groups,)), dma((groups,)), dma((groups,)), dma((groups,)),
        dma((2, 2)), dma((2, 2)), dma((2,)), dma((2,)), dma((2, ring)), dma((2, ring)),
        dma((2, ring)), dma((2, ring)), dma((2, 2 * ring)), dma((2, 4 * ring)), dma((2, devices)),
    ]
    return split, scratch, sems


def tail(ids, grads, fold, rows, ends, table, tables):
    split, scratch, sems = tail_plan(ids, grads, fold, rows, table, tables)
    small, large = pl.pallas_call(
        functools.partial(tail_kernel, None),
        out_shape=(
            jax.ShapeDtypeStruct(split, bf16),
            jax.ShapeDtypeStruct(table.shape, bf16),
        ),
        in_specs=[whole(pltpu.VMEM)] * 6 + [whole(pl.ANY)],
        out_specs=(whole(pltpu.VMEM),) * 2,
        scratch_shapes=scratch + sems,
        compiler_params=pltpu.CompilerParams(
            collective_id=1, has_side_effects=True,
            vmem_limit_bytes=grant(ids, grads, fold, rows, ends, table, table, tables, *scratch),
        ),
        name="tail",
    )(ids, grads, fold, rows, ends, table, tables.reshape(split))
    return small.reshape(tables.shape), large


def store_kernel(small_ref, large_ref, small_out, large_out, small, large, sems):
    pieces = sems.shape[2]
    copies = []
    for n, (src, mid, dst) in enumerate(
        ((small_ref, small, small_out), (large_ref, large, large_out))
    ):
        size = src.shape[0] // pieces
        for p in range(pieces):
            at = pl.ds(p * size, size)
            copies.append((
                pltpu.make_async_copy(src.at[at], mid.at[at], sems.at[0, n, p]),
                pltpu.make_async_copy(mid.at[at], dst.at[at], sems.at[1, n, p]),
            ))
    for come, _ in copies:
        come.start()
    for come, go in copies:
        come.wait()
        go.start()
    for _, go in copies:
        go.wait()


def store(small, large):
    return pl.pallas_call(
        store_kernel,
        out_shape=(
            jax.ShapeDtypeStruct(small.shape, small.dtype),
            jax.ShapeDtypeStruct(large.shape, large.dtype),
        ),
        in_specs=[whole(pltpu.HBM)] * 2,
        out_specs=(whole(pltpu.HBM),) * 2,
        scratch_shapes=[
            pltpu.VMEM(small.shape, small.dtype), pltpu.VMEM(large.shape, large.dtype),
            pltpu.SemaphoreType.DMA((2, 2, 8)),
        ],
        compiler_params=pltpu.CompilerParams(vmem_limit_bytes=63 * MIB),
        name="store",
    )(small, large)


def whole_kernel(plan, counts, *refs):
    vec_count, group, pad = plan
    inputs, refs = refs[:12], refs[12:]
    rows_hbm, ends_hbm, ids_hbm, table_hbm, tables_hbm, split_hbm = inputs[:6]
    small_hbm, large_hbm, refs = refs[0], refs[1], refs[2:]
    rows, sizes, refs = refs[0], refs[1], refs[2:]
    own, refs = refs[: counts[0]], refs[counts[0] :]
    (rows_v, ends, ids, narrow, tables, by_sample, outbox, large, small, dense, labels, w, bias, wout,
     grads, fold) = own
    tops, refs = refs[: counts[1]], refs[counts[1] :]
    send, recv, local, more, done, small_new, large_new = refs[:7]
    refs = refs[7:]
    wide = tops[1].at[pl.ds(0, table_hbm.shape[0])]
    arrays = tuple(zip(inputs[6:], (sizes, dense, labels, w, bias, wout))) + ((rows_hbm, rows_v),)
    fetch = [pltpu.make_async_copy(src, dst, more.at[n]) for n, (src, dst) in enumerate(arrays)]
    for copy in fetch:
        copy.start()
    head_kernel(
        rows_hbm, ends_hbm, ids_hbm, table_hbm, tables_hbm, large, small,
        rows, ends, ids, narrow, wide, tables, by_sample, outbox, send, recv, local,
    )
    for copy in fetch:
        copy.wait()
    scratch, sems = refs[: counts[2]], refs[counts[2] :]

    def hook():
        for copy in swap_copies(ids, grads, scratch[0], scratch[1], sems[1], sems[2]):
            copy.start()

    top_kernel(
        vec_count, group, pad, hook, None, sizes, dense, labels, small, large, w, bias, wout,
        grads, fold, *tops,
    )
    tail_kernel(
        (small_hbm, large_hbm, done), ids, grads, fold, rows_v, ends, narrow, split_hbm,
        small_new, large_new, *scratch, *sems
    )


def together(rows, ends, ids, table, tables, sizes, dense, labels, w_first, bias, wout, groups):
    labels, bias, wout = labels[None, :], bias[None, :], wout[None, :]
    batch, width = dense.shape
    large = jax.ShapeDtypeStruct((groups, ends.shape[1], width), bf16)
    small = jax.ShapeDtypeStruct((tables.shape[0], batch, width), bf16)
    vec_count, group, pad, tops = top_plan(dense, small, large)
    split, scratch, sems = tail_plan(ids, small, large, rows, table, tables)
    shaped = (rows, ends, ids, table, tables)
    own = [pltpu.VMEM(a.shape, a.dtype) for a in shaped]
    own.append(pltpu.VMEM((batch, tables.shape[0]), ids.dtype))
    own += [
        pltpu.VMEM(a.shape, a.dtype)
        for a in (large, large, small, dense, labels, w_first, bias, wout, small, large)
    ]
    need = size_of(*own, *tops, *scratch) + 5 * MIB
    if need + size_of(table, tables) > 62 * MIB or tops[1].shape[0] < table.shape[0]:
        return None
    dma = pltpu.SemaphoreType.DMA
    small_new, large_new = pl.pallas_call(
        functools.partial(whole_kernel, (vec_count, group, pad), (len(own), len(tops), len(scratch))),
        out_shape=(
            jax.ShapeDtypeStruct(split, bf16),
            jax.ShapeDtypeStruct(table.shape, bf16),
        ),
        in_specs=[whole(pltpu.HBM)] * 12,
        out_specs=(whole(pltpu.HBM),) * 2,
        scratch_shapes=[pltpu.SMEM(rows.shape, rows.dtype), pltpu.SMEM(sizes.shape, sizes.dtype)]
        + own + tops + [dma((groups,)), dma((groups,)), dma((5,)), dma((7,)), dma((6,))]
        + [pltpu.VMEM(split, bf16), pltpu.VMEM(table.shape, bf16)] + scratch + sems,
        compiler_params=pltpu.CompilerParams(
            collective_id=3, has_side_effects=True,
            vmem_limit_bytes=VMEM_LIMIT,
        ),
        name="together",
    )(
        rows, ends, ids, table, tables, tables.reshape(split), sizes, dense, labels, w_first, bias, wout
    )
    return small_new.reshape(tables.shape), large_new


def shards(
    dense, small_ids, labels, small_tables, large_tables, batch_sizes, bag_ends,
    owner_row_index, w_first, b_first, w_out,
):
    groups = lax.axis_size("shard")
    index = lax.axis_index("rep") * groups + lax.axis_index("shard")
    ends, rows, table = bag_ends[0], owner_row_index[0], large_tables[0]
    ids = jnp.transpose(small_ids)

    both = together(
        rows, ends, ids, table, small_tables, batch_sizes, dense, labels, w_first, b_first, w_out, groups
    )
    if both is not None:
        small_new, large_new = store(*both)
        return small_new, large_new[None]
    large, small = head(groups, rows, ends, ids, table, small_tables, w_first)
    small_grads, fold = top(
        index[None], batch_sizes, dense, labels, small, large, w_first, b_first, w_out
    )
    small_new, large_new = tail(ids, small_grads, fold, rows, ends, table, small_tables)
    small_new, large_new = store(small_new, large_new)
    return small_new, large_new[None]


def solution(mesh):
    both = ("rep", "shard")
    placed = (
        P(both, None), P(both, None), P(both), P(), P("shard", None, None), P(),
        P("shard", None, None), P("shard", None, None), P(), P(), P(),
    )
    return jax.shard_map(
        shards, mesh=mesh, in_specs=placed, out_specs=(P(), P("shard", None, None)), check_vma=False
    )
```

```python
import functools
import math

import jax
import jax.numpy as jnp
from jax import lax
from jax.experimental import pallas as pl
from jax.experimental.pallas import tpu as pltpu
from jax.sharding import PartitionSpec as P

step_size = 32.0
LANES = 128
VMEM_LIMIT = 60 * 1024 * 1024
MIB = 1024 * 1024
f32 = jnp.float32
bf16 = jnp.bfloat16


def whole(space):
    return pl.BlockSpec(memory_space=space)


def size_of(*arrays):
    return sum(math.prod(a.shape) * jnp.dtype(a.dtype).itemsize for a in arrays)


def grant(*arrays):
    return min(VMEM_LIMIT, size_of(*arrays) + 6 * MIB)


def all_but(*arrays):
    return min(VMEM_LIMIT, 63 * MIB - size_of(*arrays))


def iota(shape, axis):
    return lax.broadcasted_iota(jnp.int32, shape, axis)


def members_of(ends, slots):
    span = ends.shape[-1]
    starts = jnp.where(iota((1, span), 1) == 0, 0, pltpu.roll(ends, 1, 1))
    places = iota((slots, span), 0)
    return ((places >= starts) & (places < ends)).astype(f32).astype(bf16)


def spans_of(vec_count):
    return [(i, i * (i - 1) // 2) for i in range(1, vec_count)]


def top_kernel(
    vec_count, group, pad, hook, index_ref, sizes_ref, dense_ref, labels_ref, small_ref, large_ref,
    w_ref, bias_ref, wout_ref, small_out, fold_out, vecs, gram, pairs, spread,
):
    batch, width = dense_ref.shape
    small_count = small_ref.shape[0]
    feats, bag_span = large_ref.shape[0], large_ref.shape[1]
    pair_pad = pairs.shape[1]
    pair_count = vec_count * (vec_count - 1) // 2
    scale = width ** (-0.5)
    index = index_ref[0] if hook is None else position()
    spans = spans_of(vec_count)

    def rows_of(i):
        return pl.ds(i, batch, stride=pad)

    vecs[rows_of(0), :] = dense_ref[...].astype(f32)
    for t in range(small_count):
        vecs[rows_of(1 + t), :] = small_ref[t].astype(f32)
    sample = iota((batch, bag_span), 0)
    bag = iota((batch, bag_span), 1) * batch
    for f in range(feats):
        reach = sample * sizes_ref[f, index]
        hot = ((reach >= bag) & (reach < bag + batch)).astype(f32).astype(bf16)
        vecs[rows_of(1 + small_count + f), :] = jnp.dot(
            hot, large_ref[f], preferred_element_type=f32
        )
    for i in range(vec_count, pad):
        vecs[rows_of(i), :] = jnp.zeros((batch, width), f32)

    unroll = 8

    many = batch // group
    tall = group * pad

    def gram_step(g, c):
        for u in range(unroll):
            at = pl.ds(pl.multiple_of((g * unroll + u) * tall, 8), tall)
            own = vecs[at, :].astype(bf16)
            gram[at, 0:tall] = lax.dot_general(
                own, own, (((1,), (1,)), ((), ())), preferred_element_type=f32
            )
        return c

    lax.fori_loop(0, many // unroll, gram_step, 0)

    lane = iota((1, LANES), 1)
    chunk = 64
    places = [(v, start) for v in range(group) for start in range(0, many, chunk)]

    def strided(v, start, i, size):
        return pl.ds((start * group + v) * pad + i, size, stride=tall)

    for v, start in places:
        tile = jnp.zeros((chunk, LANES), f32)
        at_tile = 0
        row = v * many + start
        for i, off in spans:
            piece = gram[strided(v, start, i, chunk), :]
            turn = (off - v * pad) % LANES
            if turn:
                piece = pltpu.roll(piece, turn, 1)
            low = off - at_tile * LANES
            tile = jnp.where((lane >= low) & (lane < low + i), piece, tile)
            if low + i >= LANES:
                pairs[row : row + chunk, at_tile * LANES : (at_tile + 1) * LANES] = (
                    tile * scale
                ).astype(bf16)
                at_tile += 1
                rest = low + i - LANES
                tile = jnp.where(lane < rest, piece, jnp.zeros_like(piece))
        if at_tile * LANES < pair_pad:
            pairs[row : row + chunk, at_tile * LANES : pair_pad] = (tile * scale).astype(bf16)

    block = min(128, many)
    gram[0:batch, :] = jnp.transpose(
        jnp.broadcast_to(labels_ref[...].astype(f32), (LANES, batch))
    )
    labels_of = [gram[pl.ds(v, many, stride=group), :][:, 0:1] for v in range(group)]
    for v, start in [(v, start) for v in range(group) for start in range(0, many, block)]:
        at = slice(v * many + start, v * many + start + block)
        own_dense = vecs[strided(v, start, 0, block), :].astype(bf16)
        preact = (
            jnp.dot(pairs[at, :], w_ref[0:pair_pad, :], preferred_element_type=f32)
            + jnp.dot(own_dense, w_ref[pair_count : pair_count + width, :], preferred_element_type=f32)
            + bias_ref[...]
        )
        squash = jax.nn.sigmoid(preact)
        logits = jnp.sum(preact * squash * wout_ref[...], axis=1, keepdims=True)
        grad = jax.nn.sigmoid(logits) - labels_of[v][start : start + block, :]
        pre_grad = (
            grad * wout_ref[...] * (squash * (1.0 + preact * (1.0 - squash)))
        ).astype(bf16)
        for q in range(0, pair_pad, LANES):
            spread[at, q : q + LANES] = lax.dot_general(
                pre_grad, w_ref[q : q + LANES, :], (((1,), (1,)), ((), ())),
                preferred_element_type=f32,
            ) * scale

    gram[rows_of(0), :] = jnp.zeros((batch, LANES), f32)
    for i in range(vec_count, pad):
        gram[rows_of(i), :] = jnp.zeros((batch, LANES), f32)
    for v, start in places:
        row = v * many + start
        for i, off in spans:
            first = off // LANES
            low = off - first * LANES
            here = spread[row : row + chunk, first * LANES : (first + 1) * LANES]
            if low + i > LANES:
                after = spread[row : row + chunk, (first + 1) * LANES : (first + 2) * LANES]
                here = jnp.where(lane >= low, here, after)
            turn = (v * pad - low) % LANES
            if turn:
                here = pltpu.roll(here, turn, 1)
            gram[strided(v, start, i, chunk), :] = jnp.where(
                (lane >= v * pad) & (lane < v * pad + i), here, 0.0
            )

    def back_step(g, c):
        for u in range(unroll):
            at = pl.ds(pl.multiple_of((g * unroll + u) * tall, 8), tall)
            lower = gram[at, :]
            both = lower[:, 0:tall] + jnp.transpose(lower)[0:tall, :]
            vecs[at, :] = jnp.dot(
                both.astype(bf16), vecs[at, :].astype(bf16), preferred_element_type=f32
            )
        return c

    lax.fori_loop(0, many // unroll, back_step, 0)

    for t in range(small_count):
        small_out[t] = vecs[rows_of(1 + t), :].astype(bf16)
    sample_lane = iota((bag_span, batch), 1)
    bag_row = iota((bag_span, batch), 0) * batch
    for f in range(feats):
        if hook is not None and f == feats // 4:
            hook()
        reach = sample_lane * sizes_ref[f, index]
        hot = ((reach >= bag_row) & (reach < bag_row + batch)).astype(f32).astype(bf16)
        fold_out[f] = jnp.dot(
            hot, vecs[rows_of(1 + small_count + f), :].astype(bf16), preferred_element_type=f32
        ).astype(bf16)


def top_plan(dense, small, large):
    batch, width = dense.shape
    small_count, feats, bag_span = small.shape[0], large.shape[0], large.shape[1]
    vec_count = 1 + small_count + feats
    group = max(1, LANES // (-(-vec_count // 8) * 8))
    tiles = -(-group * vec_count // 8)
    if tiles % 2 == 0 and (tiles + 1) * 8 <= LANES:
        tiles += 1
    pad = tiles * 8 // group
    pair_count = vec_count * (vec_count - 1) // 2
    pair_pad = -(-pair_count // LANES) * LANES
    scratch = [
        pltpu.VMEM((batch * pad, width), f32),
        pltpu.VMEM((batch * pad, LANES), f32),
        pltpu.VMEM((batch, pair_pad), bf16),
        pltpu.VMEM((batch, pair_pad), f32),
    ]
    return vec_count, group, pad, scratch


def position():
    return lax.axis_index("rep") * lax.axis_size("shard") + lax.axis_index("shard")


def top(index, sizes, dense, labels, small, large, w_first, bias, wout):
    batch, width = dense.shape
    small_count, feats, bag_span = small.shape[0], large.shape[0], large.shape[1]
    vec_count, group, pad, scratch = top_plan(dense, small, large)
    return pl.pallas_call(
        functools.partial(top_kernel, vec_count, group, pad, None),
        out_shape=(
            jax.ShapeDtypeStruct((small_count, batch, width), bf16),
            jax.ShapeDtypeStruct((feats, bag_span, width), bf16),
        ),
        in_specs=[whole(pltpu.SMEM)] * 2 + [whole(pltpu.VMEM)] * 7,
        out_specs=(whole(pltpu.VMEM), whole(pltpu.VMEM)),
        scratch_shapes=scratch,
        compiler_params=pltpu.CompilerParams(
            vmem_limit_bytes=grant(dense, small, large, small, large, w_first, *scratch)
        ),
        name="top",
    )(
        index, sizes, dense, labels[None, :], small, large, w_first,
        bias[None, :], wout[None, :],
    )


def greet_all():
    copies, groups = lax.axis_size("rep"), lax.axis_size("shard")
    devices = copies * groups
    index = lax.axis_index("rep") * groups + lax.axis_index("shard")
    barrier = pltpu.get_barrier_semaphore()

    def greet(k, c):
        other = lax.rem(index + k, devices)
        pl.semaphore_signal(
            barrier, inc=1, device_id={"rep": other // groups, "shard": lax.rem(other, groups)},
            device_id_type=pl.DeviceIdType.MESH,
        )
        return c

    lax.fori_loop(1, devices, greet, 0)
    pl.semaphore_wait(barrier, devices - 1)


def remote(src, dst, send, recv, rep, shard):
    return pltpu.make_async_remote_copy(
        src_ref=src, dst_ref=dst, send_sem=send, recv_sem=recv,
        device_id={"rep": rep, "shard": shard}, device_id_type=pl.DeviceIdType.MESH,
    )


def head_kernel(
    rows_hbm, ends_hbm, ids_hbm, table_hbm, tables_hbm, large_out, small_out,
    rows, ends, ids, narrow, wide, tables, by_sample, outbox, send, recv, local,
):
    groups = lax.axis_size("shard")
    rep, me = lax.axis_index("rep"), lax.axis_index("shard")
    slots = rows.shape[1]
    arrays = ((rows_hbm, rows), (ends_hbm, ends), (ids_hbm, ids), (table_hbm, narrow), (tables_hbm, tables))
    fetch = [pltpu.make_async_copy(src, dst, local.at[n]) for n, (src, dst) in enumerate(arrays)]
    for copy in fetch:
        copy.start()
    greet_all()
    for copy in fetch[:4]:
        copy.wait()
    wide[...] = narrow[...].astype(f32)

    def block(off):
        to = lax.rem(me + off, groups)
        return remote(outbox.at[to], large_out.at[me], send.at[off], recv.at[off], rep, to)

    def block_in(off):
        at = lax.rem(me + groups - off, groups)
        return remote(outbox.at[at], large_out.at[at], send.at[off], recv.at[off], rep, at)

    def loop(low, high, act):
        def body(k, c):
            act(k)
            return c

        lax.fori_loop(low, high, body, 0)

    def give(i):
        off = lax.rem(groups // 2 + i, groups)
        to = lax.rem(me + off, groups)
        d = rep * groups + to
        picked = [
            jnp.concatenate([wide[pl.ds(rows[d, s + u], 1), :] for u in range(8)], axis=0)
            for s in range(0, slots, 8)
        ]
        pooled = lax.dot_general(
            members_of(ends[pl.ds(d, 1), :], slots), jnp.concatenate(picked, axis=0).astype(bf16),
            (((0,), (0,)), ((), ())), preferred_element_type=f32,
        )
        outbox[to] = pooled.astype(bf16)

        @pl.when(off != 0)
        def _():
            block(off).start()

    loop(0, groups, give)
    by_sample[...] = jnp.transpose(ids[...])
    large_out[me] = outbox[me]
    fetch[4].wait()
    at_row = iota((by_sample.shape[0], tables.shape[1]), 1)
    for t in range(tables.shape[0]):
        hot = (by_sample[:, t : t + 1] == at_row).astype(f32).astype(bf16)
        small_out[t] = jnp.dot(hot, tables[t], preferred_element_type=f32).astype(bf16)
    loop(1, groups, lambda off: block_in(off).wait_recv())
    loop(1, groups, lambda off: block(off).wait_send())


def head(groups, rows, ends, ids, table, tables, w_first):
    large = jax.ShapeDtypeStruct((groups, ends.shape[1], table.shape[1]), bf16)
    small = jax.ShapeDtypeStruct((tables.shape[0], ids.shape[1], tables.shape[2]), tables.dtype)
    scratch = [
        pltpu.VMEM(ends.shape, ends.dtype),
        pltpu.VMEM(ids.shape, ids.dtype),
        pltpu.VMEM(table.shape, table.dtype),
        pltpu.VMEM(table.shape, f32),
        pltpu.VMEM(tables.shape, tables.dtype),
        pltpu.VMEM((ids.shape[1], ids.shape[0]), ids.dtype),
        pltpu.VMEM(large.shape, bf16),
    ]
    dma = pltpu.SemaphoreType.DMA
    return pl.pallas_call(
        head_kernel,
        out_shape=(large, small),
        in_specs=[whole(pltpu.HBM)] * 5,
        out_specs=(whole(pltpu.VMEM),) * 2,
        scratch_shapes=[pltpu.SMEM(rows.shape, rows.dtype)] + scratch
        + [dma((groups,)), dma((groups,)), dma((5,))],
        compiler_params=pltpu.CompilerParams(
            collective_id=0, has_side_effects=True,
            vmem_limit_bytes=max(grant(large, small, *scratch), all_but(large, small, w_first)),
        ),
        name="head",
    )(rows, ends, ids, table, tables)


def swap_copies(ids_ref, grads_ref, peer_ids, peer_grads, sends, recvs):
    rep, me = lax.axis_index("rep"), lax.axis_index("shard")
    core = lax.rem(me, 2)
    peer = me + 1 - 2 * core
    count = ids_ref.shape[0] // 2
    away = (1 - core) * count
    return [
        remote(
            ids_ref.at[pl.ds(pl.multiple_of(away, 8), count)], peer_ids, sends.at[0], recvs.at[0], rep, peer
        ),
        remote(grads_ref.at[pl.ds(away, count)], peer_grads, sends.at[1], recvs.at[1], rep, peer),
    ]


def tail_kernel(
    outs, ids_ref, grads_ref, fold_ref, rows_ref, ends_ref, table_ref, tables_ref, small_out, large_out,
    peer_ids, peer_grads, folds, acc, lhs_0, lhs_1, rhs_0, rhs_1, keep, sent, came, sent_2, came_2, sent_3, came_3,
    prior, local, peer_s, peer_r, fold_s, fold_r, far_s, far_r, rs1_s, rs1_r, rs2_s, rs2_r,
    rs3_s, rs3_r, ag_z, ag_1, ag_2, ag_core, ag_r,
):
    groups = lax.axis_size("shard")
    ring = groups // 4
    rep, me = lax.axis_index("rep"), lax.axis_index("shard")
    z, y, core = me // 4, lax.rem(me, 4) // 2, lax.rem(me, 2)
    other = 1 - rep
    small_count, batch = ids_ref.shape
    half_count = small_count // 2
    per_unit = small_count // 16
    small_rows = keep.shape[2] // per_unit
    part = small_out.shape[5]
    slots = rows_ref.shape[1]
    spots = acc.shape[0]
    width = table_ref.shape[1]
    blocks = acc.shape[1] // width

    def shard_of(z_at, y_at, core_at):
        return z_at * 4 + y_at * 2 + core_at

    def loop(low, high, act):
        def body(k, c):
            act(k)
            return c

        lax.fori_loop(low, high, body, 0)

    peer = shard_of(z, y, 1 - core)
    swap = swap_copies(ids_ref, grads_ref, peer_ids, peer_grads, peer_s, peer_r)

    def out_block(k):
        to = lax.rem(me + k, groups)
        return remote(fold_ref.at[to], folds.at[rep * groups + me], fold_s.at[k], fold_r.at[k], rep, to)

    def in_block(k):
        at = lax.rem(me + groups - k, groups)
        return remote(fold_ref.at[at], folds.at[rep * groups + at], fold_s.at[k], fold_r.at[k], rep, at)

    def far_out(k):
        slot = folds.at[rep * groups + lax.rem(me + groups - k, groups)]
        return remote(slot, slot, far_s.at[k], far_r.at[k], other, me)

    def far_in(k):
        slot = folds.at[other * groups + lax.rem(me + groups - k, groups)]
        return remote(slot, slot, far_s.at[k], far_r.at[k], other, me)

    own_far = remote(fold_ref.at[me], folds.at[rep * groups + me], far_s.at[0], far_r.at[0], other, me)

    if outs is None:
        greet_all()
        for copy in swap:
            copy.start()
    loop(1, groups, lambda k: out_block(k).start())
    own_far.start()
    fetch = [
        pltpu.make_async_copy(tables_ref.at[core, h, rep, y, z], prior.at[h], local.at[h])
        for h in range(2)
    ]
    for copy in fetch:
        copy.start()
    folds[rep * groups + me] = fold_ref[me]
    acc[...] = jnp.zeros_like(acc)
    for copy in swap:
        copy.wait_recv()

    row = iota((small_rows, batch), 0)

    def dense(t):
        own = (row == ids_ref[pl.ds(core * half_count + t, 1), :]).astype(f32).astype(bf16)
        far = (row == peer_ids[pl.ds(t, 1), :]).astype(f32).astype(bf16)
        return jnp.dot(
            own, grads_ref[core * half_count + t], preferred_element_type=f32
        ) + jnp.dot(far, peer_grads[t], preferred_element_type=f32)

    def first_hop(h, s):
        to_rep = rep + (1 - h) * (1 - 2 * rep)
        to_y = y + h * (1 - 2 * y)
        return remote(
            sent.at[h, s], came.at[h, s], rs1_s.at[h, s], rs1_r.at[h, s], to_rep, shard_of(z, to_y, core)
        )

    def second_hop(h):
        to_rep = rep + h * (1 - 2 * rep)
        to_y = y + (1 - h) * (1 - 2 * y)
        return remote(
            sent_2.at[h], came_2.at[h], rs2_s.at[h], rs2_r.at[h], to_rep, shard_of(z, to_y, core)
        )

    def third_hop(h, k):
        to = lax.rem(z + k, ring)
        return remote(
            sent_3.at[h, to], came_3.at[h, z], rs3_s.at[h, k], rs3_r.at[h, k], rep, shard_of(to, y, core)
        )

    def third_in(h, k):
        at = lax.rem(z + ring - k, ring)
        return remote(
            sent_3.at[h, at], came_3.at[h, at], rs3_s.at[h, k], rs3_r.at[h, k], rep, shard_of(at, y, core)
        )

    def give(i):
        s, h = i // 2, lax.rem(i, 2)
        r_at = other + h * s * (2 * rep - 1)
        y_at = (1 - y) + (1 - h) * s * (2 * y - 1)
        first = ((h * 2 + r_at) * 2 + y_at) * per_unit
        for j in range(per_unit):
            sent[h, s, j * small_rows : (j + 1) * small_rows, :] = dense(first + j).astype(bf16)
        first_hop(h, s).start()

    def hold(i):
        s, h = i // 2, lax.rem(i, 2)
        r_at = rep + h * (1 - s) * (1 - 2 * rep)
        y_at = y + (1 - h) * (1 - s) * (1 - 2 * y)
        first = ((h * 2 + r_at) * 2 + y_at) * per_unit
        for j in range(per_unit):
            keep[h, s, j * small_rows : (j + 1) * small_rows, :] = dense(first + j)

    loop(0, 4, give)
    loop(0, 4, hold)

    spot = iota((spots, slots), 0)

    def place_rows(d, v, lhs, rhs):
        members = members_of(ends_ref[pl.ds(d, 1), :], slots)
        moved = jnp.dot(members, folds[d], preferred_element_type=f32)
        at = rows_ref[pl.ds(d, 1), :]
        block = at // spots
        wide = jnp.transpose(jnp.broadcast_to(block.astype(f32), (width, slots)))
        for q in range(blocks):
            rhs[v * slots : (v + 1) * slots, q * width : (q + 1) * width] = jnp.where(
                wide == q, moved, 0.0
            ).astype(bf16)
        lhs[:, v * slots : (v + 1) * slots] = (spot == at - block * spots).astype(f32).astype(bf16)

    turns = groups // 2
    cut_1, cut_2, cut_3 = turns // 4, turns // 2, turns * 7 // 8

    def take(k):
        in_block(k).wait_recv()

        @pl.when(k > 4 * cut_1 + 1)
        def _():
            far_out(k).start()

    def get(p):
        @pl.when((p > 0) & (p < groups // 2))
        def _():
            take(2 * p)

        @pl.when(p < groups // 2)
        def _():
            take(2 * p + 1)

        @pl.when((p >= groups // 2) & (p < groups))
        def _():
            far_in(2 * p - groups).wait_recv()
            far_in(2 * p + 1 - groups).wait_recv()

    def owner(k):
        side = k // groups
        at = lax.rem(me + groups - (k - side * groups), groups)
        return (rep + side * (1 - 2 * rep)) * groups + at

    step = 2 * width

    def make(p, lhs, rhs):
        place_rows(owner(2 * p), 0, lhs, rhs)
        place_rows(owner(2 * p + 1), 1, lhs, rhs)

    def multiply(lhs, rhs):
        for n in range(0, acc.shape[1], step):
            acc[:, n : n + step] += jnp.dot(lhs[...], rhs[:, n : n + step], preferred_element_type=f32)

    def pairs(i):
        get(2 * i + 1)
        make(2 * i + 1, lhs_1, rhs_1)
        multiply(lhs_0, rhs_0)
        get(2 * i + 2)
        make(jnp.minimum(2 * i + 2, groups - 1), lhs_0, rhs_0)
        multiply(lhs_1, rhs_1)

    loop(0, 1, get)
    make(0, lhs_0, rhs_0)
    loop(0, cut_1, pairs)

    def turn(h):
        first_hop(h, 0).wait_recv()
        sent_2[h] = (keep[h, 0] + came[h, 0].astype(f32)).astype(bf16)
        second_hop(h).start()

    loop(0, 2, turn)
    loop(1, 4 * cut_1 + 2, lambda k: far_out(k).start())
    loop(cut_1, cut_2, pairs)

    def along(h):
        first_hop(h, 1).wait_recv()
        second_hop(h).wait_recv()
        total = keep[h, 1] + came[h, 1].astype(f32) + came_2[h].astype(f32)
        keep[h, 1] = total
        sent_3[h] = total.astype(bf16).reshape(ring, part, width)
        loop(1, ring, lambda k: third_hop(h, k).start())

    loop(0, 2, along)
    loop(cut_2, cut_3, pairs)

    for copy in fetch:
        copy.wait()

    def own_part(h):
        total = keep[h, 1, pl.ds(pl.multiple_of(z * part, part), part), :]
        for k in range(1, ring):
            third_in(h, k).wait_recv()
            total = total + came_3[h, lax.rem(z + ring - k, ring)].astype(f32)
        small_out[core, h, rep, y, z] = (prior[h].astype(f32) - step_size * total).astype(bf16)

    loop(0, 2, own_part)

    pending = []

    def place(h, rep_at, z_at, y_at, core_at):
        return small_out.at[core_at, h, rep_at, y_at, z_at]

    def slot_of(rep_at, z_at, y_at, core_at):
        return rep_at * groups + shard_of(z_at, y_at, core_at)

    def send(h, rep_at, z_at, y_at, sem, to_rep, to_z, to_y, to_core):
        block = place(h, rep_at, z_at, y_at, core)
        copy = remote(
            block, block, sem, ag_r.at[h, slot_of(rep_at, z_at, y_at, core)],
            to_rep, shard_of(to_z, to_y, to_core),
        )
        copy.start()
        pending.append(copy)

    def arrived(h, rep_at, z_at, y_at, core_at):
        block = place(h, rep_at, z_at, y_at, core_at)
        remote(
            block, block, local.at[2], ag_r.at[h, slot_of(rep_at, z_at, y_at, core_at)], rep, peer
        ).wait_recv()

    def second(h, k, rep_at, z_at, y_at):
        hop = (rep, z, 1 - y, core) if h == 0 else (other, z, y, core)
        send(h, rep_at, z_at, y_at, ag_1.at[h, k], *hop)

    def third(h, k, rep_at, z_at, y_at):
        hop = (other, z, y, core) if h == 0 else (rep, z, 1 - y, core)
        send(h, rep_at, z_at, y_at, ag_2.at[h, k], *hop)

    def last(h, k, rep_at, z_at, y_at):
        send(h, rep_at, z_at, y_at, ag_core.at[h, k], rep, z, y, 1 - core)

    for k in range(1, ring):
        for h in range(2):
            send(h, rep, z, y, ag_z.at[h, k], rep, lax.rem(z + k, ring), y, core)
    for h in range(2):
        second(h, 0, rep, z, y)
        third(h, 0, rep, z, y)
        last(h, 0, rep, z, y)

    loop(cut_3, turns, pairs)
    for q in range(blocks):
        at = slice(q * spots, (q + 1) * spots)
        large_out[at, :] = (
            table_ref[at, :].astype(f32) - step_size * acc[:, q * width : (q + 1) * width]
        ).astype(bf16)

    line = [lax.rem(z + ring - k, ring) for k in range(ring)]
    if ring == 4:
        side = z // 2
        line = [z, z + 1 - 2 * lax.rem(z, 2), 2 - side, 3 * (1 - side)]
    for k in range(1, ring):
        z_at = line[k]
        for h in range(2):
            arrived(h, rep, z_at, y, core)
            second(h, k, rep, z_at, y)
            third(h, k, rep, z_at, y)
            last(h, k, rep, z_at, y)
    put = []

    def leave(src, dst):
        if outs is not None:
            copy = pltpu.make_async_copy(src, dst, outs[2].at[len(put)])
            copy.start()
            put.append(copy)

    small_hbm, large_hbm = (None, None) if outs is None else outs[:2]
    if outs is not None:
        leave(large_out, large_hbm)
    for k in range(ring):
        z_at = line[k]
        for h in range(2):
            where = (rep, z_at, 1 - y) if h == 0 else (other, z_at, y)
            arrived(h, *where, core)
            third(h, ring + k, *where)
            last(h, ring + k, *where)
    for k in range(2 * ring):
        z_at = line[k % ring]
        for h in range(2):
            if h == 0:
                where = (other, z_at, y if k < ring else 1 - y)
            else:
                where = (rep if k < ring else other, z_at, 1 - y)
            arrived(h, *where, core)
            last(h, 2 * ring + k, *where)
    if outs is not None:
        leave(small_out.at[core], small_hbm.at[core])
    for r in range(2):
        for k in range(ring):
            for y_at in range(2):
                for h in range(2):
                    arrived(h, r, k, y_at, 1 - core)
        if outs is not None:
            for h in range(2):
                leave(small_out.at[1 - core, h, r], small_hbm.at[1 - core, h, r])

    for copy in pending + swap:
        copy.wait_send()
    for copy in put:
        copy.wait()
    own_far.wait_send()
    loop(1, groups, lambda k: out_block(k).wait_send())
    loop(1, groups, lambda k: far_out(k).wait_send())
    loop(0, 4, lambda i: first_hop(lax.rem(i, 2), i // 2).wait_send())
    loop(0, 2, lambda h: second_hop(h).wait_send())
    for h in range(2):
        loop(1, ring, lambda k: third_hop(h, k).wait_send())


def tail_plan(ids, grads, fold, rows, table, tables):
    groups = fold.shape[0]
    devices, slots = rows.shape
    ring = groups // 4
    small_count, small_rows, width = tables.shape
    part = small_count * small_rows // devices // 2
    unit = small_count * small_rows // 16
    blocks = 8
    split = (2, 2, 2, 2, ring, part, width)
    scratch = [
        pltpu.VMEM((small_count // 2, ids.shape[1]), ids.dtype),
        pltpu.VMEM((small_count // 2,) + grads.shape[1:], bf16),
        pltpu.VMEM((devices,) + fold.shape[1:], bf16),
        pltpu.VMEM((table.shape[0] // blocks, blocks * width), f32),
        pltpu.VMEM((table.shape[0] // blocks, 2 * slots), bf16),
        pltpu.VMEM((table.shape[0] // blocks, 2 * slots), bf16),
        pltpu.VMEM((2 * slots, blocks * width), bf16),
        pltpu.VMEM((2 * slots, blocks * width), bf16),
        pltpu.VMEM((2, 2, unit, width), f32),
        pltpu.VMEM((2, 2, unit, width), bf16),
        pltpu.VMEM((2, 2, unit, width), bf16),
        pltpu.VMEM((2, unit, width), bf16),
        pltpu.VMEM((2, unit, width), bf16),
        pltpu.VMEM((2, ring, part, width), bf16),
        pltpu.VMEM((2, ring, part, width), bf16),
        pltpu.VMEM((2, part, width), bf16),
    ]
    dma = pltpu.SemaphoreType.DMA
    sems = [
        dma((3,)), dma((2,)), dma((2,)),
        dma((groups,)), dma((groups,)), dma((groups,)), dma((groups,)),
        dma((2, 2)), dma((2, 2)), dma((2,)), dma((2,)), dma((2, ring)), dma((2, ring)),
        dma((2, ring)), dma((2, ring)), dma((2, 2 * ring)), dma((2, 4 * ring)), dma((2, devices)),
    ]
    return split, scratch, sems


def tail(ids, grads, fold, rows, ends, table, tables):
    split, scratch, sems = tail_plan(ids, grads, fold, rows, table, tables)
    small, large = pl.pallas_call(
        functools.partial(tail_kernel, None),
        out_shape=(
            jax.ShapeDtypeStruct(split, bf16),
            jax.ShapeDtypeStruct(table.shape, bf16),
        ),
        in_specs=[whole(pltpu.VMEM)] * 6 + [whole(pl.ANY)],
        out_specs=(whole(pltpu.VMEM),) * 2,
        scratch_shapes=scratch + sems,
        compiler_params=pltpu.CompilerParams(
            collective_id=1, has_side_effects=True,
            vmem_limit_bytes=grant(ids, grads, fold, rows, ends, table, table, tables, *scratch),
        ),
        name="tail",
    )(ids, grads, fold, rows, ends, table, tables.reshape(split))
    return small.reshape(tables.shape), large


def store_kernel(small_ref, large_ref, small_out, large_out, small, large, sems):
    pieces = sems.shape[2]
    copies = []
    for n, (src, mid, dst) in enumerate(
        ((small_ref, small, small_out), (large_ref, large, large_out))
    ):
        size = src.shape[0] // pieces
        for p in range(pieces):
            at = pl.ds(p * size, size)
            copies.append((
                pltpu.make_async_copy(src.at[at], mid.at[at], sems.at[0, n, p]),
                pltpu.make_async_copy(mid.at[at], dst.at[at], sems.at[1, n, p]),
            ))
    for come, _ in copies:
        come.start()
    for come, go in copies:
        come.wait()
        go.start()
    for _, go in copies:
        go.wait()


def store(small, large):
    return pl.pallas_call(
        store_kernel,
        out_shape=(
            jax.ShapeDtypeStruct(small.shape, small.dtype),
            jax.ShapeDtypeStruct(large.shape, large.dtype),
        ),
        in_specs=[whole(pltpu.HBM)] * 2,
        out_specs=(whole(pltpu.HBM),) * 2,
        scratch_shapes=[
            pltpu.VMEM(small.shape, small.dtype), pltpu.VMEM(large.shape, large.dtype),
            pltpu.SemaphoreType.DMA((2, 2, 8)),
        ],
        compiler_params=pltpu.CompilerParams(vmem_limit_bytes=63 * MIB),
        name="store",
    )(small, large)


def whole_kernel(plan, counts, *refs):
    vec_count, group, pad = plan
    inputs, refs = refs[:12], refs[12:]
    rows_hbm, ends_hbm, ids_hbm, table_hbm, tables_hbm, split_hbm = inputs[:6]
    small_hbm, large_hbm, refs = refs[0], refs[1], refs[2:]
    rows, sizes, refs = refs[0], refs[1], refs[2:]
    own, refs = refs[: counts[0]], refs[counts[0] :]
    (rows_v, ends, ids, narrow, tables, by_sample, outbox, large, small, dense, labels, w, bias, wout,
     grads, fold) = own
    tops, refs = refs[: counts[1]], refs[counts[1] :]
    send, recv, local, more, done, small_new, large_new = refs[:7]
    refs = refs[7:]
    wide = tops[1].at[pl.ds(0, table_hbm.shape[0])]
    arrays = tuple(zip(inputs[6:], (sizes, dense, labels, w, bias, wout))) + ((rows_hbm, rows_v),)
    fetch = [pltpu.make_async_copy(src, dst, more.at[n]) for n, (src, dst) in enumerate(arrays)]
    for copy in fetch:
        copy.start()
    head_kernel(
        rows_hbm, ends_hbm, ids_hbm, table_hbm, tables_hbm, large, small,
        rows, ends, ids, narrow, wide, tables, by_sample, outbox, send, recv, local,
    )
    for copy in fetch:
        copy.wait()
    scratch, sems = refs[: counts[2]], refs[counts[2] :]

    def hook():
        for copy in swap_copies(ids, grads, scratch[0], scratch[1], sems[1], sems[2]):
            copy.start()

    top_kernel(
        vec_count, group, pad, hook, None, sizes, dense, labels, small, large, w, bias, wout,
        grads, fold, *tops,
    )
    tail_kernel(
        (small_hbm, large_hbm, done), ids, grads, fold, rows_v, ends, narrow, split_hbm,
        small_new, large_new, *scratch, *sems
    )


def together(rows, ends, ids, table, tables, sizes, dense, labels, w_first, bias, wout, groups):
    labels, bias, wout = labels[None, :], bias[None, :], wout[None, :]
    batch, width = dense.shape
    large = jax.ShapeDtypeStruct((groups, ends.shape[1], width), bf16)
    small = jax.ShapeDtypeStruct((tables.shape[0], batch, width), bf16)
    vec_count, group, pad, tops = top_plan(dense, small, large)
    split, scratch, sems = tail_plan(ids, small, large, rows, table, tables)
    shaped = (rows, ends, ids, table, tables)
    own = [pltpu.VMEM(a.shape, a.dtype) for a in shaped]
    own.append(pltpu.VMEM((batch, tables.shape[0]), ids.dtype))
    own += [
        pltpu.VMEM(a.shape, a.dtype)
        for a in (large, large, small, dense, labels, w_first, bias, wout, small, large)
    ]
    need = size_of(*own, *tops, *scratch) + 5 * MIB
    if need + size_of(table, tables) > 62 * MIB or tops[1].shape[0] < table.shape[0]:
        return None
    dma = pltpu.SemaphoreType.DMA
    small_new, large_new = pl.pallas_call(
        functools.partial(whole_kernel, (vec_count, group, pad), (len(own), len(tops), len(scratch))),
        out_shape=(
            jax.ShapeDtypeStruct(split, bf16),
            jax.ShapeDtypeStruct(table.shape, bf16),
        ),
        in_specs=[whole(pltpu.HBM)] * 12,
        out_specs=(whole(pltpu.HBM),) * 2,
        scratch_shapes=[pltpu.SMEM(rows.shape, rows.dtype), pltpu.SMEM(sizes.shape, sizes.dtype)]
        + own + tops + [dma((groups,)), dma((groups,)), dma((5,)), dma((7,)), dma((6,))]
        + [pltpu.VMEM(split, bf16), pltpu.VMEM(table.shape, bf16)] + scratch + sems,
        compiler_params=pltpu.CompilerParams(
            collective_id=3, has_side_effects=True,
            vmem_limit_bytes=VMEM_LIMIT,
        ),
        name="together",
    )(
        rows, ends, ids, table, tables, tables.reshape(split), sizes, dense, labels, w_first, bias, wout
    )
    return small_new.reshape(tables.shape), large_new


def shards(
    dense, small_ids, labels, small_tables, large_tables, batch_sizes, bag_ends,
    owner_row_index, w_first, b_first, w_out,
):
    groups = lax.axis_size("shard")
    index = lax.axis_index("rep") * groups + lax.axis_index("shard")
    ends, rows, table = bag_ends[0], owner_row_index[0], large_tables[0]
    ids = jnp.transpose(small_ids)

    both = together(
        rows, ends, ids, table, small_tables, batch_sizes, dense, labels, w_first, b_first, w_out, groups
    )
    if both is not None:
        small_new, large_new = store(*both)
        return small_new, large_new[None]
    large, small = head(groups, rows, ends, ids, table, small_tables, w_first)
    small_grads, fold = top(
        index[None], batch_sizes, dense, labels, small, large, w_first, b_first, w_out
    )
    small_new, large_new = tail(ids, small_grads, fold, rows, ends, table, small_tables)
    small_new, large_new = store(small_new, large_new)
    return small_new, large_new[None]


def solution(mesh):
    both = ("rep", "shard")
    placed = (
        P(both, None), P(both, None), P(both), P(), P("shard", None, None), P(),
        P("shard", None, None), P("shard", None, None), P(), P(), P(),
    )
    return jax.shard_map(
        shards, mesh=mesh, in_specs=placed, out_specs=(P(), P("shard", None, None)), check_vma=False
    )
```
